256 devices in a mesh: vpair: 16 (over x, y), rank: 16 (over z, core).
Axes of the slice: x: 4, y: 4, z: 8, core: 2. Of those that a mesh axis runs over, the one named last changes fastest.
Arguments:
- amplitudes: bfloat16 [8, 1200, 1200], P(None, 'vpair', 'rank'), may hold values from -6 to 6
- factors: bfloat16 [1200, 8192], P('vpair', 'rank'), may hold values from -0.1875 to 0.1875
- kernel: bfloat16 [8192, 8192], P('vpair', 'rank'), may hold values from -0.875 to 0.875
- other_terms: float32 [8, 1200, 1200], P(None, 'vpair'), may hold values from -6 to 6
- virt_energy: float32 [1200], replicated, may hold values from 0.2 to 4
- pair_energy: float32 [8], replicated, may hold values from -3 to -0.5
Outputs:
- residual: float32 [8, 1200, 1200], P(None, 'vpair')
- update_rms: float32 [], replicated
The draws below stay inside these ranges and needn't reach their ends.
All inputs are finite; a program needn't handle non-finite values.
Results may differ from the reference program's by a relative error of at most 0.0035.
Values may be sent and summed in bfloat16 or wider, within the bound.
A program may use at most 192 MiB of HBM per device.

```python
import jax
import jax.numpy as jnp
from jax import lax

NVIR = 1200
NTHC = 8192
PAIRS = 8


def draw_virt_energy(key, part):
    jitter = jax.random.uniform(key, (NVIR,), jnp.float32)
    spread = (jnp.arange(NVIR, dtype=jnp.float32) + jitter) / NVIR
    return 0.2 + 3.8 * spread


def block_levels(rng, dims, split, smallest, largest):
    gain = 1.0
    for axis_at, parts in split:
        heights = jax.random.uniform(jax.random.fold_in(jax.random.fold_in(rng, 6), axis_at), (parts,), jnp.float32, smallest / len(split), largest / len(split))
        gain = gain * jnp.repeat(jnp.exp(heights), dims[axis_at] // parts).reshape((-1,) + (1,) * (len(dims) - 1 - axis_at))
    return gain


def centred(rng, shape, scale, limit, cuts=(), held_as=jnp.bfloat16):
    drawn = scale * jax.random.normal(rng, shape, jnp.float32)
    if cuts:
        drawn = drawn * block_levels(rng, shape, cuts, -0.22, 0.18)
    return jnp.clip(drawn, -limit, limit).astype(held_as)


def setup_inputs(seed: int = 0) -> dict:
    keys = jax.random.split(jax.random.key(seed), 7)
    amplitudes = centred(keys[0], (PAIRS, NVIR, NVIR), 1.0, 6.0, ((1, 16), (2, 16)))
    factors = centred(keys[1], (NVIR, NTHC), NVIR ** -0.5, 0.1875, ((0, 16), (1, 16)))
    kernel = centred(keys[2], (NTHC, NTHC), (NTHC * NTHC // (NVIR * NVIR)) ** -0.5, 0.875, ((0, 16), (1, 16)))
    other_terms = centred(keys[3], (PAIRS, NVIR, NVIR), 1.0, 6.0, ((1, 16),), jnp.float32)
    virt_energy = draw_virt_energy(jax.random.fold_in(keys[6], 71), 0)
    pair_energy = jnp.clip(jax.random.uniform(keys[5], (PAIRS,), jnp.float32, -3.0, -0.5), -3.0, -0.5)
    return dict(amplitudes=amplitudes, factors=factors, kernel=kernel, other_terms=other_terms, virt_energy=virt_energy, pair_energy=pair_energy)


epsilon = 1e-06

def reference(amplitudes, factors, kernel, other_terms, virt_energy, pair_energy):
    kernel_wide = kernel.astype(jnp.float32)

    def one_pair(operands):
        amplitude, other_block, pair_value = operands
        first_half = jnp.dot(amplitude, factors, preferred_element_type=jnp.float32).astype(jnp.bfloat16)
        coupled = jnp.dot(factors.T, first_half, preferred_element_type=jnp.float32)
        weighted = (kernel_wide * coupled).astype(jnp.bfloat16)
        back_half = jnp.dot(factors, weighted, preferred_element_type=jnp.float32).astype(jnp.bfloat16)
        ladder = jnp.dot(back_half, factors.T, preferred_element_type=jnp.float32)
        residual = other_block + ladder
        denominator = virt_energy[:, None] + virt_energy[None, :] - pair_value
        update = residual / denominator
        return (residual, jnp.sum(update * update))
    residual, squares = lax.map(one_pair, (amplitudes, other_terms, pair_energy))
    update_rms = jnp.sqrt(jnp.sum(squares) / (PAIRS * NVIR * NVIR) + epsilon)
    return (residual, update_rms)
```

```python
import functools

import jax
import jax.numpy as jnp
from jax import lax
from jax.experimental import pallas as pl
from jax.experimental.pallas import tpu as pltpu
from jax.sharding import Mesh
from jax.sharding import PartitionSpec as P

MESH = pl.DeviceIdType.MESH
BF = jnp.bfloat16
F32 = jnp.float32
EPS = 1e-06
NT = (((1,), (1,)), ((), ()))
TN = (((0,), (0,)), ((), ()))
TICKS = 12
READY = 6


def roll(a, shift):
    shift %= 128
    return a if shift == 0 else pltpu.roll(a, shift, 1)


def ladder_kernel(
    f_ref, t_ref, zt_ref, other_ref, ea_ref, eb_ref, ep_ref, out_ref, rms_ref,
    xb, tt, ttp, half, hs, hb, ht, zb_ref, wt, acc, rb, bs, br, ls, lb, lt, ltr, lc, la, sc, sp, sz,
    x_ss, x_rs, c_ss, c_rs, r_ss, r_rs, t_ss, t_rs, u_ss, u_rs, g_ss, g_rs, m_ss, m_rs, loc,
):
    x, y, z, c = (lax.axis_index(n) for n in ("x", "y", "z", "core"))
    v = 4 * x + y
    xp, xm = (x + 1) % 4, (x + 3) % 4
    yp, ym = (y + 1) % 4, (y + 3) % 4
    zp, zm = (z + 1) % 8, (z + 7) % 8
    sib = {"core": 1 - c}

    def rows(i, off, n, ref=None):
        return (xb if ref is None else ref).at[i, pl.ds(pl.multiple_of(off, 16), n)]

    def send(src, dst, ss, rs, dev):
        pltpu.make_async_remote_copy(
            src_ref=src, dst_ref=dst, send_sem=ss, recv_sem=rs, device_id=dev, device_id_type=MESH
        ).start()

    def got(dst, rs):
        pltpu.make_async_remote_copy(
            src_ref=dst, dst_ref=dst, send_sem=rs, recv_sem=rs, device_id=sib, device_id_type=MESH
        ).wait_recv()

    def left(src, ss):
        pltpu.make_async_remote_copy(
            src_ref=src, dst_ref=src, send_sem=ss, recv_sem=ss, device_id=sib, device_id_type=MESH
        ).wait_send()

    def a_off(i, j):
        return i * 128 + j * 32

    def b_off(i, j):
        return 512 + j * 128 + i * 32

    def c_off(i, j):
        return 1024 + i * 64 + j * 16

    own = [
        pltpu.make_async_copy(f_ref.at[pl.ds(0, 32)], rows(z, a_off(x, y), 32), loc.at[0]),
        pltpu.make_async_copy(f_ref.at[pl.ds(32, 32)], rows(z, b_off(x, y), 32), loc.at[1]),
        pltpu.make_async_copy(f_ref.at[pl.ds(64, 16)], rows(z, c_off(x, y), 16), loc.at[2]),
        pltpu.make_async_copy(t_ref, tt.at[2 * z + c], loc.at[3]),
    ]
    for o in own:
        o.start()

    bar = pltpu.get_barrier_semaphore()

    def plane_dev(j, core):
        w = (v + j) % 16
        return {"x": w // 4, "y": w % 4, "core": core}

    def greet(j, _):
        pl.semaphore_signal(bar, inc=1, device_id=plane_dev(j, c), device_id_type=MESH)
        pl.semaphore_signal(bar, inc=1, device_id=plane_dev(j, 1 - c), device_id_type=MESH)
        return 0

    lax.fori_loop(1, 16, greet, 0)
    pl.semaphore_signal(bar, inc=1, device_id=sib, device_id_type=MESH)

    def greet_z(j, _):
        pl.semaphore_signal(bar, inc=1, device_id={"z": (z + j) % 8}, device_id_type=MESH)
        return 0

    lax.fori_loop(1, 8, greet_z, 0)
    for o in own:
        o.wait()
    pl.semaphore_wait(bar, 38)

    def zblk(k):
        return (z + ((k + 1) // 2) * (2 * (k % 2) - 1) + 8) % 8

    def ring_step(s, zl, zr):
        for d, (blk, dev) in enumerate(((zl, zp), (zr, zm))):
            i = 2 * s + d
            dev = {"z": dev}
            r = 2 * blk + c
            if s < 3:
                for o in (a_off(x, y), b_off(x, y)):
                    w = 0 if o is None else o
                send(rows(blk, a_off(x, y), 32), rows(blk, a_off(x, y), 32), r_ss.at[i], r_rs.at[i], dev)
                send(rows(blk, b_off(x, y), 32), rows(blk, b_off(x, y), 32), r_ss.at[8 + i], r_rs.at[8 + i], dev)
                send(tt.at[r], tt.at[r], t_ss.at[i], t_rs.at[i], dev)
            elif d == 0:
                send(rows(blk, a_off(x, y), 32), rows(blk, a_off(x, y), 32), r_ss.at[i], r_rs.at[i], dev)
                send(tt.at[r, pl.ds(0, 48)], tt.at[r, pl.ds(0, 48)], t_ss.at[i], t_rs.at[i], dev)
            else:
                send(rows(blk, b_off(x, y), 32), rows(blk, b_off(x, y), 32), r_ss.at[i], r_rs.at[i], dev)
                send(tt.at[r, pl.ds(48, 32)], tt.at[r, pl.ds(48, 32)], t_ss.at[i], t_rs.at[i], dev)

    def push_t(n, blk):
        r = 2 * blk + c
        send(tt.at[r], tt.at[r], u_ss.at[n], u_rs.at[n], sib)

    def ring_got(s):
        lo, hi = (z + 7 - s) % 8, (z + 1 + s) % 8
        for d, blk in enumerate((lo, hi)):
            i = 2 * s + d
            r = 2 * blk + c
            if s < 3:
                got(rows(blk, a_off(x, y), 32), r_rs.at[i])
                got(rows(blk, b_off(x, y), 32), r_rs.at[8 + i])
                got(tt.at[r], t_rs.at[i])
            elif d == 0:
                got(rows(blk, a_off(x, y), 32), r_rs.at[i])
                got(tt.at[r, pl.ds(0, 48)], t_rs.at[i])
            else:
                got(rows(blk, b_off(x, y), 32), r_rs.at[i])
                got(tt.at[r, pl.ds(48, 32)], t_rs.at[i])
        return lo, hi

    ring_step(0, z, z)
    push_t(0, z)

    def c_piece(i, j, h):
        return xb.at[z, pl.ds(pl.multiple_of(c_off(i, j), 16), 16), pl.ds(256 * h, 256)]

    def c_step(s):
        if s == 0:
            p = rows(z, c_off(x, y), 16)
            send(p, p, c_ss.at[0], c_rs.at[0], {"y": yp})
            send(p, p, c_ss.at[1], c_rs.at[1], {"y": ym})
        elif s == 1:
            got(rows(z, c_off(x, ym), 16), c_rs.at[0])
            got(rows(z, c_off(x, yp), 16), c_rs.at[1])
            p, q = c_piece(x, ym, 0), c_piece(x, yp, 1)
            send(p, p, c_ss.at[2], c_rs.at[2], {"y": yp})
            send(q, q, c_ss.at[3], c_rs.at[3], {"y": ym})
        elif s == 2:
            got(c_piece(x, (y + 2) % 4, 0), c_rs.at[2])
            got(c_piece(x, (y + 2) % 4, 1), c_rs.at[3])
            p = rows(z, c_off(x, 0), 64)
            send(p, p, c_ss.at[4], c_rs.at[4], {"x": xp})
            send(p, p, c_ss.at[5], c_rs.at[5], {"x": xm})
        elif s == 3:
            got(rows(z, c_off(xm, 0), 64), c_rs.at[4])
            got(rows(z, c_off(xp, 0), 64), c_rs.at[5])
            p, q = rows(z, c_off(xm, 0), 32), rows(z, c_off(xp, 2), 32)
            send(p, p, c_ss.at[6], c_rs.at[6], {"x": xp})
            send(q, q, c_ss.at[7], c_rs.at[7], {"x": xm})
        else:
            if s == 4:
                got(rows(z, c_off((x + 2) % 4, 0), 32), c_rs.at[6])
                got(rows(z, c_off((x + 2) % 4, 2), 32), c_rs.at[7])
            else:
                g = s - 5
                lo, hi = (z + 7 - g) % 8, (z + 1 + g) % 8
                i = 8 + 2 * g
                if g < 3:
                    got(rows(lo, 1024, 256), c_rs.at[i])
                    got(rows(hi, 1024, 256), c_rs.at[i + 1])
                else:
                    got(rows(lo, 1024, 128), c_rs.at[i])
                    got(rows(hi, 1152, 128), c_rs.at[i + 1])
            if s < 8:
                h = s - 4
                i = 8 + 2 * h
                lo, hi = (z + 8 - h) % 8, (z + h) % 8
                n = 256 if h < 3 else 128
                o = 1024 if h < 3 else 1152
                send(rows(lo, 1024, n), rows(lo, 1024, n), c_ss.at[i], c_rs.at[i], {"z": zp})
                send(rows(hi, o, n), rows(hi, o, n), c_ss.at[i + 1], c_rs.at[i + 1], {"z": zm})

    def s1(k):
        b = zblk(k)
        p, q = rows(b, a_off(x, y), 32), rows(b, b_off(x, y), 32)
        send(p, p, x_ss.at[k, 0], x_rs.at[k, 0], {"y": yp})
        send(p, p, x_ss.at[k, 1], x_rs.at[k, 1], {"y": ym})
        send(q, q, x_ss.at[k, 8], x_rs.at[k, 8], {"x": xp})
        send(q, q, x_ss.at[k, 9], x_rs.at[k, 9], {"x": xm})

    def s2(k):
        b = zblk(k)
        got(rows(b, a_off(x, ym), 32), x_rs.at[k, 0])
        got(rows(b, a_off(x, yp), 32), x_rs.at[k, 1])
        p, q = rows(b, a_off(x, ym), 16), rows(b, a_off(x, yp) + 16, 16)
        send(p, p, x_ss.at[k, 2], x_rs.at[k, 2], {"y": yp})
        send(q, q, x_ss.at[k, 3], x_rs.at[k, 3], {"y": ym})
        got(rows(b, b_off(xm, y), 32), x_rs.at[k, 8])
        got(rows(b, b_off(xp, y), 32), x_rs.at[k, 9])
        p, q = rows(b, b_off(xm, y), 16), rows(b, b_off(xp, y) + 16, 16)
        send(p, p, x_ss.at[k, 10], x_rs.at[k, 10], {"x": xp})
        send(q, q, x_ss.at[k, 11], x_rs.at[k, 11], {"x": xm})

    def s3(k):
        b = zblk(k)
        y2, x2 = (y + 2) % 4, (x + 2) % 4
        got(rows(b, a_off(x, y2), 16), x_rs.at[k, 2])
        got(rows(b, a_off(x, y2) + 16, 16), x_rs.at[k, 3])
        p = rows(b, a_off(x, 0), 128)
        send(p, p, x_ss.at[k, 4], x_rs.at[k, 4], {"x": xp})
        send(p, p, x_ss.at[k, 5], x_rs.at[k, 5], {"x": xm})
        got(rows(b, b_off(x2, y), 16), x_rs.at[k, 10])
        got(rows(b, b_off(x2, y) + 16, 16), x_rs.at[k, 11])
        p = rows(b, b_off(0, y), 128)
        send(p, p, x_ss.at[k, 12], x_rs.at[k, 12], {"y": yp})
        send(p, p, x_ss.at[k, 13], x_rs.at[k, 13], {"y": ym})

    def s4(k):
        b = zblk(k)
        got(rows(b, a_off(xm, 0), 128), x_rs.at[k, 4])
        got(rows(b, a_off(xp, 0), 128), x_rs.at[k, 5])
        p, q = rows(b, a_off(xm, 0), 64), rows(b, a_off(xp, 2), 64)
        send(p, p, x_ss.at[k, 6], x_rs.at[k, 6], {"x": xp})
        send(q, q, x_ss.at[k, 7], x_rs.at[k, 7], {"x": xm})
        got(rows(b, b_off(0, ym), 128), x_rs.at[k, 12])
        got(rows(b, b_off(0, yp), 128), x_rs.at[k, 13])
        p, q = rows(b, b_off(0, ym), 64), rows(b, b_off(2, yp), 64)
        send(p, p, x_ss.at[k, 14], x_rs.at[k, 14], {"y": yp})
        send(q, q, x_ss.at[k, 15], x_rs.at[k, 15], {"y": ym})

    def s5(k):
        b = zblk(k)
        y2, x2 = (y + 2) % 4, (x + 2) % 4
        got(rows(b, a_off(x2, 0), 64), x_rs.at[k, 6])
        got(rows(b, a_off(x2, 2), 64), x_rs.at[k, 7])
        got(rows(b, b_off(0, y2), 64), x_rs.at[k, 14])
        got(rows(b, b_off(2, y2), 64), x_rs.at[k, 15])

    def send_kernel():
        kc = y % 2

        def one(j, _):
            w = (v + j) % 16
            src = zt_ref.at[pl.ds(pl.multiple_of(32 * w, 32), 32)]
            send(src, zb_ref.at[v // 2, c], m_ss.at[0], m_rs.at[0], plane_dev(j, kc))
            return 0

        lax.fori_loop(1, 16, one, 0)
        src = zt_ref.at[pl.ds(pl.multiple_of(32 * v, 32), 32)]

        @pl.when(c == kc)
        def _():
            pltpu.make_async_copy(src, zb_ref.at[v // 2, c], m_rs.at[0]).start()

        @pl.when(c != kc)
        def _():
            send(src, zb_ref.at[v // 2, c], m_ss.at[0], m_rs.at[0], sib)

    def make_half():
        for n in range(1, 8):
            b = zblk(n)
            got(tt.at[2 * b + 1 - c], u_rs.at[n])
        got(tt.at[2 * z + 1 - c], u_rs.at[0])
        for i in range(4):
            for j in range(4):
                w = 4 * i + j
                ttp[pl.ds(a_off(i, j), 32), :] = tt[w, pl.ds(0, 32), :]
                ttp[pl.ds(b_off(i, j), 32), :] = tt[w, pl.ds(32, 32), :]
                ttp[pl.ds(c_off(i, j), 16), :] = tt[w, pl.ds(64, 16), :]
        lanes = lax.broadcasted_iota(jnp.int32, (80, 128), 1) // 32

        def chunk(a, _):
            q = pl.ds(pl.multiple_of(256 * a, 256), 256)
            half[...] = lax.dot_general(ttp[...], xb[z, :, q], TN, preferred_element_type=F32)
            for h in range(2):
                for g in range(2):
                    part = [half[pl.ds(80 * (4 * g + k), 80), pl.ds(128 * h, 128)] for k in range(4)]
                    for s in range(4):
                        m = roll(part[0], (0 - s) * 32)
                        for k in range(1, 4):
                            m = jnp.where(lanes == k, roll(part[k], (k - s) * 32), m)
                        hs[8 * a + 4 * h + s, :, pl.ds(128 * g, 128)] = m.astype(BF)
            return 0

        lax.fori_loop(0, 2, chunk, 0)

        def one(j, _):
            send(hs.at[(v + j) % 16], hb.at[c, v], m_ss.at[1], m_rs.at[1], plane_dev(j, c))
            return 0

        lax.fori_loop(1, 16, one, 0)
        pltpu.make_async_copy(hs.at[v], hb.at[c, v], m_rs.at[1]).start()

    def take_half():
        got(hb.at[c], m_rs.at[1])
        send(hb.at[c], hb.at[c], m_ss.at[2], m_rs.at[2], sib)
        acc[...] = jnp.zeros_like(acc)
        got(hb.at[1 - c], m_rs.at[2])
        for s in range(2):
            to = pl.ds(256 * s, 256)
            for i in range(4):
                m = jnp.concatenate([hb[s, 4 * i + j, pl.ds(0, 32), :] for j in range(4)], 0)
                ht[to, pl.ds(128 * i, 128)] = m.astype(F32).T.astype(BF)
                m = jnp.concatenate([hb[s, 4 * j + i, pl.ds(32, 32), :] for j in range(4)], 0)
                ht[to, pl.ds(512 + 128 * i, 128)] = m.astype(F32).T.astype(BF)
            for i in range(2):
                m = jnp.concatenate([hb[s, 8 * i + j, pl.ds(64, 16), :] for j in range(8)], 0)
                ht[to, pl.ds(1024 + 128 * i, 128)] = m.astype(F32).T.astype(BF)
        got(zb_ref, m_rs.at[0])

    def compute(k, _):
        b = zblk(k)
        for q in range(2):
            q = pl.ds(256 * q, 256)
            cp = jnp.dot(ht[...], xb[b, :, q], preferred_element_type=F32)
            zz = zb_ref[b, :, :, q].astype(F32)
            for s in range(2):
                for i in range(8):
                    o = 256 * s + 32 * i
                    wt[pl.ds(o, 32), q] = (cp[o : o + 32] * zz[s]).astype(BF)
        for a in range(5):
            a = pl.ds(256 * a, 256)
            acc[:, a] += lax.dot_general(wt[...], xb[b, a, :], NT, preferred_element_type=F32)
        return 0

    def tick(t, _):
        for s in range(1, 9):
            if s <= 4:

                @pl.when(t == s)
                def _(s=s):
                    lo, hi = ring_got(s - 1)
                    if s < 4:
                        ring_step(s, lo, hi)
                        push_t(2 * s - 1, hi)
                        push_t(2 * s, lo)
                    else:
                        push_t(7, lo)

        @pl.when(t >= 4)
        def _():
            s5(t - 4)

        for s in range(9):

            @pl.when(t == s)
            def _(s=s):
                c_step(s)

        @pl.when((t >= 3) & (t < 11))
        def _():
            s4(t - 3)

        @pl.when((t >= 2) & (t < 10))
        def _():
            s3(t - 2)

        @pl.when((t >= 1) & (t < 9))
        def _():
            s2(t - 1)

        @pl.when(t < 8)
        def _():
            s1(t)

        @pl.when(t == 0)
        def _():
            send_kernel()

        @pl.when(t == 4)
        def _():
            make_half()

        @pl.when(t == READY)
        def _():
            take_half()

        lo = jnp.minimum(jnp.maximum(t - 4, 0), jnp.maximum(2 * (t - READY), 0))
        hi = jnp.minimum(jnp.maximum(t - 3, 0), jnp.maximum(2 * (t - READY + 1), 0))
        lax.fori_loop(lo, hi, compute, 0)
        return 0

    lax.fori_loop(0, TICKS, tick, 0)

    mine = pl.ds(pl.multiple_of(256 * c, 256), 256)
    give = acc.at[pl.ds(pl.multiple_of(256 * (1 - c), 256), 256)]
    send(give, rb, m_ss.at[3], m_rs.at[3], sib)
    got(rb, m_rs.at[3])
    for n in range(10):
        a = pl.ds(128 * n, 128)
        m = (acc[mine, a] + rb[:, a]).T.astype(BF)
        if n < 4:
            for j in range(4):
                bs[4 * n + j, pl.ds(0, 32), :] = m[32 * j : 32 * j + 32]
        elif n < 8:
            for j in range(4):
                bs[4 * j + n - 4, pl.ds(32, 32), :] = m[32 * j : 32 * j + 32]
        else:
            for j in range(8):
                bs[8 * (n - 8) + j, pl.ds(64, 16), :] = m[16 * j : 16 * j + 16]

    def give_back(j, _):
        send(bs.at[(v + j) % 16], br.at[v], m_ss.at[4], m_rs.at[4], plane_dev(j, c))
        return 0

    lax.fori_loop(1, 16, give_back, 0)
    pltpu.make_async_copy(bs.at[v], br.at[v], m_rs.at[4]).start()
    got(br, m_rs.at[4])

    lanes = lax.broadcasted_iota(jnp.int32, (80, 128), 1) // 32
    for g in range(2):
        for a in range(4):
            part = [br[4 * a + s, :, pl.ds(128 * g, 128)].astype(F32) for s in range(4)]
            for k in range(4):
                m = roll(part[0], (0 - k) * 32)
                for s in range(1, 4):
                    m = jnp.where(lanes == s, roll(part[s], (s - k) * 32), m)
                ls[4 * g + k, :, pl.ds(128 * a, 128)] = m.astype(BF)

    def give_z(j, _):
        w = (z + j) % 8
        send(ls.at[w], lb.at[z], m_ss.at[5], m_rs.at[5], {"z": w})
        return 0

    lax.fori_loop(1, 8, give_z, 0)
    pltpu.make_async_copy(ls.at[z], lb.at[z], m_rs.at[5]).start()
    got(lb, m_rs.at[5])

    lt[...] = jnp.zeros_like(lt)

    def lad(b, _):
        for a in range(5):
            a = pl.ds(256 * a, 256)
            lt[a, pl.ds(0, 80)] += lax.dot_general(xb[b, a, :], lb[b], NT, preferred_element_type=F32)
        return 0

    lax.fori_loop(0, 8, lad, 0)
    send(lt, ltr, m_ss.at[6], m_rs.at[6], sib)
    got(ltr, m_rs.at[6])
    lc[pl.ds(1200, 80), :] = jnp.zeros((80, 128), F32)
    for i in range(4):
        for j in range(4):
            o = 75 * (4 * i + j)
            for n, off, cnt in ((0, a_off(i, j), 32), (32, b_off(i, j), 32), (64, c_off(i, j), 11)):
                lc[pl.ds(o + n, cnt), :] = lt[pl.ds(off, cnt), :] + ltr[pl.ds(off, cnt), :]
    total = jnp.zeros((75, 128), F32)
    ep = ep_ref[z]
    for n in range(10):
        b = pl.ds(128 * n, 128)
        m = lc[b, :].T[:80]
        la[z, :, b] = m.astype(BF)
        w = 128 if n < 9 else 48
        b = pl.ds(128 * n, w)
        den = ea_ref[...] + eb_ref[:, b] - ep
        u = (other_ref[z, :, b] + m[:75, :w]) / den
        u = u * u
        if w < 128:
            u = jnp.concatenate([u, jnp.zeros((75, 128 - w), F32)], 1)
        total = total + u
    sc[...] = jnp.full((8, 128), jnp.sum(total), F32)

    def la_part(i, h, lo=0, n=80):
        return la.at[i, pl.ds(lo, n), pl.ds(pl.multiple_of(640 * h, 128), 640)]

    def la_step(s, lo, hi):
        for d, (blk, dev) in enumerate(((lo, zp), (hi, zm))):
            p = la_part(blk, c) if s < 3 else la_part(blk, c, 48 * d, 48 - 16 * d)
            send(p, p, g_ss.at[2 * s + d], g_rs.at[2 * s + d], {"z": dev})

    def la_push(n, blk):
        send(la_part(blk, c), la_part(blk, c), g_ss.at[8 + n], g_rs.at[8 + n], sib)

    la_step(0, z, z)

    def give_sum(j, _):
        send(sc, sp.at[v], m_ss.at[7], m_rs.at[7], plane_dev(j, c))
        return 0

    lax.fori_loop(1, 16, give_sum, 0)
    pltpu.make_async_copy(sc, sp.at[v], m_rs.at[7]).start()
    for s in range(4):
        lo, hi = (z + 7 - s) % 8, (z + 1 + s) % 8
        if s < 3:
            got(la_part(lo, c), g_rs.at[2 * s])
            got(la_part(hi, c), g_rs.at[2 * s + 1])
            la_step(s + 1, lo, hi)
            la_push(2 * s, hi)
            la_push(2 * s + 1, lo)
        else:
            got(la_part(lo, c, 0, 48), g_rs.at[6])
            got(la_part(lo, c, 48, 32), g_rs.at[7])
            la_push(6, lo)
        if s == 0:
            got(sp, m_rs.at[7])
            s_all = sp[0]
            for n in range(1, 16):
                s_all = s_all + sp[n]
            sz[z] = s_all

            def give_sz(j, _):
                send(sz.at[z], sz.at[z], m_ss.at[8], m_rs.at[8], {"z": (z + j) % 8})
                return 0

            lax.fori_loop(1, 8, give_sz, 0)
    for n in range(7):
        b = zblk(n + 1)
        got(la_part(b, 1 - c), g_rs.at[8 + n])

    def finish(i, _):
        out_ref[i] = other_ref[i] + la[i, pl.ds(0, 75), pl.ds(0, 1200)].astype(F32)
        return 0

    lax.fori_loop(0, 8, finish, 0)
    got(sz.at[pl.ds(0, 7)], m_rs.at[8])
    s_all = sz[0]
    for n in range(1, 8):
        s_all = s_all + sz[n]
    rms_ref[...] = jnp.sqrt(s_all / (8 * 1200 * 1200) + EPS)

    for s in range(4):
        for d in range(2):
            i = 2 * s + d
            if s < 3:
                left(rows(0, 0, 32), r_ss.at[i])
                left(rows(0, 0, 32), r_ss.at[8 + i])
                left(tt.at[0], t_ss.at[i])
                left(la_part(0, 0), g_ss.at[i])
            else:
                left(rows(0, 0, 32), r_ss.at[i])
                left(tt.at[0, pl.ds(0, 48 - 16 * d)], t_ss.at[i])
                left(la_part(0, 0, 0, 48 - 16 * d), g_ss.at[i])
    for n in range(8):
        left(tt.at[0], u_ss.at[n])
    for n in range(7):
        left(la_part(0, 0), g_ss.at[8 + n])
    for n in (0, 1):
        left(rows(0, 0, 16), c_ss.at[n])
        left(xb.at[0, pl.ds(0, 16), pl.ds(0, 256)], c_ss.at[2 + n])
        left(rows(0, 0, 64), c_ss.at[4 + n])
        left(rows(0, 0, 32), c_ss.at[6 + n])
        left(rows(0, 0, 256), c_ss.at[8 + n])
        left(rows(0, 0, 256), c_ss.at[10 + n])
        left(rows(0, 0, 256), c_ss.at[12 + n])
        left(rows(0, 0, 128), c_ss.at[14 + n])

    def drain(k, _):
        for o in (0, 8):
            for n, cnt in ((0, 32), (2, 16), (4, 128), (6, 64)):
                left(rows(0, 0, cnt), x_ss.at[k, o + n])
                left(rows(0, 0, cnt), x_ss.at[k, o + n + 1])
        return 0

    lax.fori_loop(0, 8, drain, 0)

    @pl.when(c == y % 2)
    def _():
        left(zt_ref.at[pl.ds(0, 480)], m_ss.at[0])

    @pl.when(c != y % 2)
    def _():
        left(zt_ref, m_ss.at[0])

    left(hs.at[pl.ds(0, 15)], m_ss.at[1])
    left(hb.at[0], m_ss.at[2])
    left(rb, m_ss.at[3])
    left(bs.at[pl.ds(0, 15)], m_ss.at[4])
    left(ls.at[pl.ds(0, 7)], m_ss.at[5])
    left(lt, m_ss.at[6])
    left(sp.at[pl.ds(0, 15)], m_ss.at[7])
    left(sz.at[pl.ds(0, 7)], m_ss.at[8])


def shards(amplitudes, factors, kernel, other_terms, virt_energy, pair_energy):
    pairs, block, _ = amplitudes.shape
    v = lax.axis_index("x") * 4 + lax.axis_index("y")
    f = jnp.pad(factors, ((0, 5), (0, 0)))
    t = jnp.pad(jnp.transpose(amplitudes, (2, 0, 1)), ((0, 5), (0, 0), (0, 5))).reshape(80, 640)
    zt = kernel.T
    ea = lax.dynamic_slice_in_dim(virt_energy, v * block, block, 0)[:, None]
    eb = virt_energy[None, :]
    vm = pl.BlockSpec(memory_space=pltpu.VMEM)
    V = pltpu.VMEM
    dma = pltpu.SemaphoreType.DMA
    out, rms = pl.pallas_call(
        ladder_kernel,
        out_shape=(
            jax.ShapeDtypeStruct(other_terms.shape, F32),
            jax.ShapeDtypeStruct((8, 128), F32),
        ),
        in_specs=[vm] * 6 + [pl.BlockSpec(memory_space=pltpu.SMEM)],
        out_specs=(vm, vm),
        scratch_shapes=[
            V((8, 1280, 512), BF),
            V((16, 80, 640), BF),
            V((1280, 640), BF),
            V((640, 256), F32),
            V((16, 80, 256), BF),
            V((2, 16, 80, 256), BF),
            V((512, 1280), BF),
            V((8, 2, 32, 512), BF),
            V((512, 512), BF),
            V((512, 1280), F32),
            V((256, 1280), F32),
            V((16, 80, 256), BF),
            V((16, 80, 256), BF),
            V((8, 80, 512), BF),
            V((8, 80, 512), BF),
            V((1280, 128), F32),
            V((1280, 128), F32),
            V((1280, 128), F32),
            V((8, 80, 1280), BF),
            V((8, 128), F32),
            V((16, 8, 128), F32),
            V((8, 8, 128), F32),
            dma((8, 16)), dma((8, 16)),
            dma((16,)), dma((16,)),
            dma((16,)), dma((16,)),
            dma((8,)), dma((8,)),
            dma((8,)), dma((8,)),
            dma((16,)), dma((16,)),
            dma((16,)), dma((16,)),
            dma((4,)),
        ],
        compiler_params=pltpu.CompilerParams(
            collective_id=0, has_side_effects=True, vmem_limit_bytes=60 * 1024 * 1024
        ),
        name="ladder",
    )(f, t, zt, other_terms, ea, eb, pair_energy)
    return out, rms[0, 0]


def solution(mesh):
    torus = Mesh(mesh.devices.reshape(4, 4, 8, 2), ("x", "y", "z", "core"))
    plane, rank = ("x", "y"), ("z", "core")
    return jax.shard_map(
        shards,
        mesh=torus,
        in_specs=(P(None, plane, rank), P(plane, rank), P(plane, rank), P(None, plane, None), P(), P()),
        out_specs=(P(None, plane, None), P()),
        check_vma=False,
    )
```

```python
import functools

import jax
import jax.numpy as jnp
from jax import lax
from jax.experimental import pallas as pl
from jax.experimental.pallas import tpu as pltpu
from jax.sharding import Mesh
from jax.sharding import PartitionSpec as P

MESH = pl.DeviceIdType.MESH
BF = jnp.bfloat16
F32 = jnp.float32
EPS = 1e-06
NT = (((1,), (1,)), ((), ()))
TN = (((0,), (0,)), ((), ()))
TICKS = 12
READY = 6


def roll(a, shift):
    shift %= 128
    return a if shift == 0 else pltpu.roll(a, shift, 1)


def ladder_kernel(
    f_ref, t_ref, k_ref, other_hbm, e_ref, ep_ref, out_ref, rms_ref,
    stage, res, zt_ref, er,
    xb, tt, ttp, half, hs, hb, ht, zb_ref, wt, acc, rb, bs, br, ls, lb, lt, ltr, lc, la, sc, sp, sz,
    x_ss, x_rs, c_ss, c_rs, r_ss, r_rs, t_ss, t_rs, u_ss, u_rs, g_ss, g_rs, m_ss, m_rs, p_ss, p_rs, q_ss, q_rs, loc,
):
    x, y, z, c = (lax.axis_index(n) for n in ("x", "y", "z", "core"))
    v = 4 * x + y
    xp, xm = (x + 1) % 4, (x + 3) % 4
    yp, ym = (y + 1) % 4, (y + 3) % 4
    zp, zm = (z + 1) % 8, (z + 7) % 8
    sib = {"core": 1 - c}

    def rows(i, off, n, ref=None):
        return (xb if ref is None else ref).at[i, pl.ds(pl.multiple_of(off, 16), n)]

    def send(src, dst, ss, rs, dev):
        pltpu.make_async_remote_copy(
            src_ref=src, dst_ref=dst, send_sem=ss, recv_sem=rs, device_id=dev, device_id_type=MESH
        ).start()

    def got(dst, rs):
        pltpu.make_async_remote_copy(
            src_ref=dst, dst_ref=dst, send_sem=rs, recv_sem=rs, device_id=sib, device_id_type=MESH
        ).wait_recv()

    def left(src, ss):
        pltpu.make_async_remote_copy(
            src_ref=src, dst_ref=src, send_sem=ss, recv_sem=ss, device_id=sib, device_id_type=MESH
        ).wait_send()

    def a_off(i, j):
        return i * 128 + j * 32

    def b_off(i, j):
        return 512 + j * 128 + i * 32

    def c_off(i, j):
        return 1024 + i * 64 + j * 16

    own = [
        pltpu.make_async_copy(f_ref.at[pl.ds(0, 32)], rows(z, a_off(x, y), 32), loc.at[0]),
        pltpu.make_async_copy(f_ref.at[pl.ds(32, 32)], rows(z, b_off(x, y), 32), loc.at[1]),
    ]
    for o in own:
        o.start()

    others = pltpu.make_async_copy(other_hbm, stage, loc.at[2])
    others.start()

    bar = pltpu.get_barrier_semaphore()

    def plane_dev(j, core):
        w = (v + j) % 16
        return {"x": w // 4, "y": w % 4, "core": core}

    def greet(j, _):
        pl.semaphore_signal(bar, inc=1, device_id=plane_dev(j, c), device_id_type=MESH)
        pl.semaphore_signal(bar, inc=1, device_id=plane_dev(j, 1 - c), device_id_type=MESH)
        return 0

    lax.fori_loop(1, 16, greet, 0)
    pl.semaphore_signal(bar, inc=1, device_id=sib, device_id_type=MESH)

    def greet_z(j, _):
        pl.semaphore_signal(bar, inc=1, device_id={"z": (z + j) % 8}, device_id_type=MESH)
        return 0

    lax.fori_loop(1, 8, greet_z, 0)
    with jax.named_scope("local"):
        last = jnp.concatenate([f_ref[pl.ds(64, 11), :].astype(F32), jnp.zeros((5, 512), F32)], 0)
        xb[z, pl.ds(pl.multiple_of(c_off(x, y), 16), 16), :] = last.astype(BF)
        for n in range(5):
            cnt = 128 if n < 4 else 88
            m = t_ref[pl.ds(128 * n, cnt), :].astype(F32)
            if cnt < 128:
                m = jnp.concatenate([m, jnp.zeros((128 - cnt, 75), F32)], 0)
            m = jnp.concatenate([m.T, jnp.zeros((5, 128), F32)], 0)
            tt[2 * z + c, :, pl.ds(128 * n, 128)] = m.astype(BF)
        for n in range(4):
            zt_ref[:, pl.ds(128 * n, 128)] = k_ref[pl.ds(128 * n, 128), :].astype(F32).T.astype(BF)
        er[:, pl.ds(0, 1200)] = jnp.broadcast_to(e_ref[...], (8, 1200))
        er[:, pl.ds(1200, 80)] = jnp.zeros((8, 80), F32)
        others.wait()
        for n in range(10):
            w = 128 if n < 9 else 48
            res[n, :, pl.ds(0, w)] = stage[:, pl.ds(128 * n, w)]
    for o in own:
        o.wait()
    with jax.named_scope('barrier'):
        pl.semaphore_wait(bar, 38)

    def zblk(k):
        return (z + ((k + 1) // 2) * (2 * (k % 2) - 1) + 8) % 8

    def ring_step(s, zl, zr):
        for d, (blk, dev) in enumerate(((zl, zp), (zr, zm))):
            i = 2 * s + d
            dev = {"z": dev}
            r = 2 * blk + c
            if s < 3:
                for o in (a_off(x, y), b_off(x, y)):
                    w = 0 if o is None else o
                send(rows(blk, a_off(x, y), 32), rows(blk, a_off(x, y), 32), r_ss.at[i], r_rs.at[i], dev)
                send(rows(blk, b_off(x, y), 32), rows(blk, b_off(x, y), 32), r_ss.at[8 + i], r_rs.at[8 + i], dev)
                send(tt.at[r], tt.at[r], t_ss.at[i], t_rs.at[i], dev)
            elif d == 0:
                send(rows(blk, a_off(x, y), 32), rows(blk, a_off(x, y), 32), r_ss.at[i], r_rs.at[i], dev)
                send(tt.at[r, pl.ds(0, 48)], tt.at[r, pl.ds(0, 48)], t_ss.at[i], t_rs.at[i], dev)
            else:
                send(rows(blk, b_off(x, y), 32), rows(blk, b_off(x, y), 32), r_ss.at[i], r_rs.at[i], dev)
                send(tt.at[r, pl.ds(48, 32)], tt.at[r, pl.ds(48, 32)], t_ss.at[i], t_rs.at[i], dev)

    def push_t(n, blk):
        r = 2 * blk + c
        send(tt.at[r], tt.at[r], u_ss.at[n], u_rs.at[n], sib)

    def ring_got(s):
        lo, hi = (z + 7 - s) % 8, (z + 1 + s) % 8
        for d, blk in enumerate((lo, hi)):
            i = 2 * s + d
            r = 2 * blk + c
            if s < 3:
                got(rows(blk, a_off(x, y), 32), r_rs.at[i])
                got(rows(blk, b_off(x, y), 32), r_rs.at[8 + i])
                got(tt.at[r], t_rs.at[i])
            elif d == 0:
                got(rows(blk, a_off(x, y), 32), r_rs.at[i])
                got(tt.at[r, pl.ds(0, 48)], t_rs.at[i])
            else:
                got(rows(blk, b_off(x, y), 32), r_rs.at[i])
                got(tt.at[r, pl.ds(48, 32)], t_rs.at[i])
        return lo, hi

    ring_step(0, z, z)
    push_t(0, z)

    def c_piece(i, j, h):
        return xb.at[z, pl.ds(pl.multiple_of(c_off(i, j), 16), 16), pl.ds(256 * h, 256)]

    def c_step(s):
        if s == 0:
            p = rows(z, c_off(x, y), 16)
            send(p, p, c_ss.at[0], c_rs.at[0], {"y": yp})
            send(p, p, c_ss.at[1], c_rs.at[1], {"y": ym})
        elif s == 1:
            got(rows(z, c_off(x, ym), 16), c_rs.at[0])
            got(rows(z, c_off(x, yp), 16), c_rs.at[1])
            p, q = c_piece(x, ym, 0), c_piece(x, yp, 1)
            send(p, p, c_ss.at[2], c_rs.at[2], {"y": yp})
            send(q, q, c_ss.at[3], c_rs.at[3], {"y": ym})
        elif s == 2:
            got(c_piece(x, (y + 2) % 4, 0), c_rs.at[2])
            got(c_piece(x, (y + 2) % 4, 1), c_rs.at[3])
            p = rows(z, c_off(x, 0), 64)
            send(p, p, c_ss.at[4], c_rs.at[4], {"x": xp})
            send(p, p, c_ss.at[5], c_rs.at[5], {"x": xm})
        elif s == 3:
            got(rows(z, c_off(xm, 0), 64), c_rs.at[4])
            got(rows(z, c_off(xp, 0), 64), c_rs.at[5])
            p, q = rows(z, c_off(xm, 0), 32), rows(z, c_off(xp, 2), 32)
            send(p, p, c_ss.at[6], c_rs.at[6], {"x": xp})
            send(q, q, c_ss.at[7], c_rs.at[7], {"x": xm})
        else:
            if s == 4:
                got(rows(z, c_off((x + 2) % 4, 0), 32), c_rs.at[6])
                got(rows(z, c_off((x + 2) % 4, 2), 32), c_rs.at[7])
            else:
                g = s - 5
                lo, hi = (z + 7 - g) % 8, (z + 1 + g) % 8
                i = 8 + 2 * g
                if g < 3:
                    got(rows(lo, 1024, 256), c_rs.at[i])
                    got(rows(hi, 1024, 256), c_rs.at[i + 1])
                else:
                    got(rows(lo, 1024, 128), c_rs.at[i])
                    got(rows(hi, 1152, 128), c_rs.at[i + 1])
            if s < 8:
                h = s - 4
                i = 8 + 2 * h
                lo, hi = (z + 8 - h) % 8, (z + h) % 8
                n = 256 if h < 3 else 128
                o = 1024 if h < 3 else 1152
                send(rows(lo, 1024, n), rows(lo, 1024, n), c_ss.at[i], c_rs.at[i], {"z": zp})
                send(rows(hi, o, n), rows(hi, o, n), c_ss.at[i + 1], c_rs.at[i + 1], {"z": zm})

    def s1(k):
        b = zblk(k)
        p, q = rows(b, a_off(x, y), 32), rows(b, b_off(x, y), 32)
        send(p, p, x_ss.at[k, 0], x_rs.at[k, 0], {"y": yp})
        send(p, p, x_ss.at[k, 1], x_rs.at[k, 1], {"y": ym})
        send(q, q, x_ss.at[k, 8], x_rs.at[k, 8], {"x": xp})
        send(q, q, x_ss.at[k, 9], x_rs.at[k, 9], {"x": xm})

    def s2(k):
        b = zblk(k)
        got(rows(b, a_off(x, ym), 32), x_rs.at[k, 0])
        got(rows(b, a_off(x, yp), 32), x_rs.at[k, 1])
        p, q = rows(b, a_off(x, ym), 16), rows(b, a_off(x, yp) + 16, 16)
        send(p, p, x_ss.at[k, 2], x_rs.at[k, 2], {"y": yp})
        send(q, q, x_ss.at[k, 3], x_rs.at[k, 3], {"y": ym})
        got(rows(b, b_off(xm, y), 32), x_rs.at[k, 8])
        got(rows(b, b_off(xp, y), 32), x_rs.at[k, 9])
        p, q = rows(b, b_off(xm, y), 16), rows(b, b_off(xp, y) + 16, 16)
        send(p, p, x_ss.at[k, 10], x_rs.at[k, 10], {"x": xp})
        send(q, q, x_ss.at[k, 11], x_rs.at[k, 11], {"x": xm})

    def s3(k):
        b = zblk(k)
        y2, x2 = (y + 2) % 4, (x + 2) % 4
        got(rows(b, a_off(x, y2), 16), x_rs.at[k, 2])
        got(rows(b, a_off(x, y2) + 16, 16), x_rs.at[k, 3])
        p = rows(b, a_off(x, 0), 128)
        send(p, p, x_ss.at[k, 4], x_rs.at[k, 4], {"x": xp})
        send(p, p, x_ss.at[k, 5], x_rs.at[k, 5], {"x": xm})
        got(rows(b, b_off(x2, y), 16), x_rs.at[k, 10])
        got(rows(b, b_off(x2, y) + 16, 16), x_rs.at[k, 11])
        p = rows(b, b_off(0, y), 128)
        send(p, p, x_ss.at[k, 12], x_rs.at[k, 12], {"y": yp})
        send(p, p, x_ss.at[k, 13], x_rs.at[k, 13], {"y": ym})

    def s4(k):
        b = zblk(k)
        got(rows(b, a_off(xm, 0), 128), x_rs.at[k, 4])
        got(rows(b, a_off(xp, 0), 128), x_rs.at[k, 5])
        p, q = rows(b, a_off(xm, 0), 64), rows(b, a_off(xp, 2), 64)
        send(p, p, x_ss.at[k, 6], x_rs.at[k, 6], {"x": xp})
        send(q, q, x_ss.at[k, 7], x_rs.at[k, 7], {"x": xm})
        got(rows(b, b_off(0, ym), 128), x_rs.at[k, 12])
        got(rows(b, b_off(0, yp), 128), x_rs.at[k, 13])
        p, q = rows(b, b_off(0, ym), 64), rows(b, b_off(2, yp), 64)
        send(p, p, x_ss.at[k, 14], x_rs.at[k, 14], {"y": yp})
        send(q, q, x_ss.at[k, 15], x_rs.at[k, 15], {"y": ym})

    def s5(k):
        b = zblk(k)
        y2, x2 = (y + 2) % 4, (x + 2) % 4
        got(rows(b, a_off(x2, 0), 64), x_rs.at[k, 6])
        got(rows(b, a_off(x2, 2), 64), x_rs.at[k, 7])
        got(rows(b, b_off(0, y2), 64), x_rs.at[k, 14])
        got(rows(b, b_off(2, y2), 64), x_rs.at[k, 15])

    def send_kernel():
        kc = y % 2

        def one(j, _):
            w = (v + j) % 16
            src = zt_ref.at[pl.ds(pl.multiple_of(32 * w, 32), 32)]
            send(src, zb_ref.at[v // 2, c], m_ss.at[0], m_rs.at[0], plane_dev(j, kc))
            return 0

        lax.fori_loop(1, 16, one, 0)
        src = zt_ref.at[pl.ds(pl.multiple_of(32 * v, 32), 32)]

        @pl.when(c == kc)
        def _():
            pltpu.make_async_copy(src, zb_ref.at[v // 2, c], m_rs.at[0]).start()

        @pl.when(c != kc)
        def _():
            send(src, zb_ref.at[v // 2, c], m_ss.at[0], m_rs.at[0], sib)

    def make_half():
        for n in range(1, 8):
            b = zblk(n)
            got(tt.at[2 * b + 1 - c], u_rs.at[n])
        got(tt.at[2 * z + 1 - c], u_rs.at[0])
        for i in range(4):
            for j in range(4):
                w = 4 * i + j
                ttp[pl.ds(a_off(i, j), 32), :] = tt[w, pl.ds(0, 32), :]
                ttp[pl.ds(b_off(i, j), 32), :] = tt[w, pl.ds(32, 32), :]
                ttp[pl.ds(c_off(i, j), 16), :] = tt[w, pl.ds(64, 16), :]
        lanes = lax.broadcasted_iota(jnp.int32, (80, 128), 1) // 32

        def chunk(a, _):
            q = pl.ds(pl.multiple_of(256 * a, 256), 256)
            m = lax.dot_general(ttp[...], xb[z, :, q], TN, preferred_element_type=F32)
            half[0] = m[:, :128]
            half[1] = m[:, 128:]
            for h in range(2):
                for g in range(2):
                    part = [half[h, pl.ds(4 * g + k, 80, stride=8), :] for k in range(4)]
                    for s in range(4):
                        m = roll(part[0], (0 - s) * 32)
                        for k in range(1, 4):
                            m = jnp.where(lanes == k, roll(part[k], (k - s) * 32), m)
                        hs[8 * a + 4 * h + s, :, pl.ds(128 * g, 128)] = m.astype(BF)
            return 0

        lax.fori_loop(0, 2, chunk, 0)

        def one(j, _):
            send(hs.at[(v + j) % 16], hb.at[c, v], m_ss.at[1], m_rs.at[1], plane_dev(j, c))
            return 0

        lax.fori_loop(1, 16, one, 0)
        pltpu.make_async_copy(hs.at[v], hb.at[c, v], m_rs.at[1]).start()

    def take_half():
        with jax.named_scope('w_hb'):
            got(hb.at[c], m_rs.at[1])
        send(hb.at[c], hb.at[c], m_ss.at[2], m_rs.at[2], sib)
        acc[...] = jnp.zeros_like(acc)
        with jax.named_scope('w_hbs'):
            got(hb.at[1 - c], m_rs.at[2])
        for s in range(2):
            to = pl.ds(256 * s, 256)
            for i in range(4):
                m = jnp.concatenate([hb[s, 4 * i + j, pl.ds(0, 32), :] for j in range(4)], 0)
                ht[to, pl.ds(128 * i, 128)] = m.astype(F32).T.astype(BF)
                m = jnp.concatenate([hb[s, 4 * j + i, pl.ds(32, 32), :] for j in range(4)], 0)
                ht[to, pl.ds(512 + 128 * i, 128)] = m.astype(F32).T.astype(BF)
            for i in range(2):
                m = jnp.concatenate([hb[s, 8 * i + j, pl.ds(64, 16), :] for j in range(8)], 0)
                ht[to, pl.ds(1024 + 128 * i, 128)] = m.astype(F32).T.astype(BF)
        with jax.named_scope('w_zb'):
            got(zb_ref, m_rs.at[0])

    def compute(k, _):
        b = zblk(k)
        for q in range(2):
            q = pl.ds(256 * q, 256)
            cp = jnp.dot(ht[...], xb[b, :, q], preferred_element_type=F32)
            zz = zb_ref[b, :, :, q].astype(F32)
            for s in range(2):
                for i in range(8):
                    o = 256 * s + 32 * i
                    wt[pl.ds(o, 32), q] = (cp[o : o + 32] * zz[s]).astype(BF)
        for a in range(5):
            a = pl.ds(256 * a, 256)
            acc[:, a] += lax.dot_general(wt[...], xb[b, a, :], NT, preferred_element_type=F32)
        return 0

    def tick(t, _):
        for s in range(1, 9):
            if s <= 4:

                @pl.when(t == s)
                def _(s=s):
                    with jax.named_scope('ring_got'):
                        lo, hi = ring_got(s - 1)
                    if s < 4:
                        ring_step(s, lo, hi)
                        push_t(2 * s - 1, hi)
                        push_t(2 * s, lo)
                    else:
                        push_t(7, lo)

        @pl.when(t >= 4)
        def _():
            with jax.named_scope('s5'):
                s5(t - 4)

        for s in range(9):

            @pl.when(t == s)
            def _(s=s):
                with jax.named_scope('c_step'):
                    c_step(s)

        @pl.when((t >= 3) & (t < 11))
        def _():
            with jax.named_scope('s4'):
                s4(t - 3)

        @pl.when((t >= 2) & (t < 10))
        def _():
            with jax.named_scope('s3'):
                s3(t - 2)

        @pl.when((t >= 1) & (t < 9))
        def _():
            with jax.named_scope('s2'):
                s2(t - 1)

        @pl.when(t < 8)
        def _():
            with jax.named_scope('s1'):
                s1(t)

        @pl.when(t == 0)
        def _():
            with jax.named_scope('send_kernel'):
                send_kernel()

        @pl.when(t == 4)
        def _():
            with jax.named_scope('make_half'):
                make_half()

        @pl.when(t == READY)
        def _():
            with jax.named_scope('take_half'):
                take_half()

        lo = jnp.minimum(jnp.maximum(t - 4, 0), jnp.maximum(2 * (t - READY), 0))
        hi = jnp.minimum(jnp.maximum(t - 3, 0), jnp.maximum(2 * (t - READY + 1), 0))
        with jax.named_scope('compute'):
            lax.fori_loop(lo, hi, compute, 0)
        return 0

    lax.fori_loop(0, TICKS, tick, 0)

    mine = pl.ds(pl.multiple_of(256 * c, 256), 256)
    give = acc.at[pl.ds(pl.multiple_of(256 * (1 - c), 256), 256)]
    send(give, rb, m_ss.at[3], m_rs.at[3], sib)
    with jax.named_scope('w_rb'):
        got(rb, m_rs.at[3])
    for n in range(10):
        a = pl.ds(128 * n, 128)
        m = (acc[mine, a] + rb[:, a]).T.astype(BF)
        if n < 4:
            for j in range(4):
                bs[4 * n + j, pl.ds(0, 32), :] = m[32 * j : 32 * j + 32]
        elif n < 8:
            for j in range(4):
                bs[4 * j + n - 4, pl.ds(32, 32), :] = m[32 * j : 32 * j + 32]
        else:
            for j in range(8):
                bs[8 * (n - 8) + j, pl.ds(64, 16), :] = m[16 * j : 16 * j + 16]

    pieces = ((0, 32), (32, 48))
    for h, (lo, n) in enumerate(pieces):

        def give_back(j, _):
            w = (v + j) % 16
            send(bs.at[w, pl.ds(lo, n)], br.at[v, pl.ds(lo, n)], p_ss.at[h], p_rs.at[h], plane_dev(j, c))
            return 0

        lax.fori_loop(1, 16, give_back, 0)
        pltpu.make_async_copy(bs.at[v, pl.ds(lo, n)], br.at[v, pl.ds(lo, n)], p_rs.at[h]).start()

    def z_of(j):
        return (j // 2 + 1) if j % 2 == 0 else 7 - j // 2

    for h, (lo, n) in enumerate(pieces):
        with jax.named_scope("w_br"):
            got(br.at[:, pl.ds(lo, n)], p_rs.at[h])
        with jax.named_scope("unpack"):
            lanes = lax.broadcasted_iota(jnp.int32, (n, 128), 1) // 32
            for g in range(2):
                for a in range(4):
                    part = [br[4 * a + s, pl.ds(lo, n), pl.ds(128 * g, 128)].astype(F32) for s in range(4)]
                    for k in range(4):
                        m = roll(part[0], (0 - k) * 32)
                        for s in range(1, 4):
                            m = jnp.where(lanes == s, roll(part[s], (s - k) * 32), m)
                        ls[4 * g + k, pl.ds(lo, n), pl.ds(128 * a, 128)] = m.astype(BF)
        for j in range(7):
            d = z_of(j)
            w = (z + d) % 8
            send(ls.at[w, pl.ds(lo, n)], lb.at[z, pl.ds(lo, n)], q_ss.at[h, d], q_rs.at[h, d], {"z": w})
        if h == 0:
            lt[...] = jnp.zeros_like(lt)

    def lad(b, src):
        for a in range(5):
            a = pl.ds(256 * a, 256)
            lt[a, pl.ds(0, 80)] += lax.dot_general(xb[b, a, :], src[b], NT, preferred_element_type=F32)

    lad(z, ls)

    def lad_step(j, _):
        d = jnp.where(j % 2 == 0, j // 2 + 1, 7 - j // 2)
        b = (z + 8 - d) % 8
        with jax.named_scope("w_lb"):
            for h, (lo, n) in enumerate(pieces):
                got(lb.at[b, pl.ds(lo, n)], q_rs.at[h, d])
        with jax.named_scope("w_lad"):
            lad(b, lb)
        return 0

    lax.fori_loop(0, 7, lad_step, 0)
    send(lt, ltr, m_ss.at[6], m_rs.at[6], sib)
    ea = pltpu.roll(er[...], (1280 - 75 * v) % 1280, 1)[:, :128].T[:75, 0:1]
    with jax.named_scope("w_ltr"):
        got(ltr, m_rs.at[6])
    lc[pl.ds(1200, 80), :] = jnp.zeros((80, 128), F32)
    for i in range(4):
        for j in range(4):
            o = 75 * (4 * i + j)
            for n, off, cnt in ((0, a_off(i, j), 32), (32, b_off(i, j), 32), (64, c_off(i, j), 11)):
                lc[pl.ds(o + n, cnt), :] = lt[pl.ds(off, cnt), :] + ltr[pl.ds(off, cnt), :]
    for n in range(10):
        b = pl.ds(128 * n, 128)
        la[z, :, b] = lc[b, :].T[:80].astype(BF)

    chunks = ((0, 48), (48, 32))

    def la_part(i, h, ch):
        lo, n = chunks[ch]
        return la.at[i, pl.ds(lo, n), pl.ds(pl.multiple_of(640 * h, 128), 640)]

    def la_send(s, blk, d, ch):
        p = la_part(blk, c, ch)
        send(p, p, g_ss.at[2 * s + d, ch], g_rs.at[2 * s + d, ch], {"z": (zp, zm)[d]})

    def la_push(n, blk, ch):
        p = la_part(blk, c, ch)
        send(p, p, g_ss.at[8 + n, ch], g_rs.at[8 + n, ch], sib)

    for ch in range(2):
        for d in range(2):
            la_send(0, z, d, ch)

    total = jnp.zeros((75, 128), F32)
    ep = ep_ref[z]
    for n in range(10):
        w = 128 if n < 9 else 48
        b = pl.ds(128 * n, w)
        den = ea + er[0:1, b] - ep
        u = (res[n, pl.ds(z, 75, stride=8), :] + lc[pl.ds(128 * n, 128), :].T[:75])[:, :w] / den
        u = u * u
        if w < 128:
            u = jnp.concatenate([u, jnp.zeros((75, 128 - w), F32)], 1)
        total = total + u
    sc[...] = jnp.full((8, 128), jnp.sum(total), F32)

    def give_sum(j, _):
        send(sc, sp.at[v], m_ss.at[7], m_rs.at[7], plane_dev(j, c))
        return 0

    lax.fori_loop(1, 16, give_sum, 0)
    pltpu.make_async_copy(sc, sp.at[v], m_rs.at[7]).start()

    def finish(i):
        o = pl.ds(i, 75, stride=8)
        for n in range(10):
            b = pl.ds(128 * n, 128)
            res[n, o, :] = res[n, o, :] + la[i, :, b].astype(F32)[:75]

    for s in range(4):
        lo, hi = (z + 7 - s) % 8, (z + 1 + s) % 8
        with jax.named_scope(f"w_la{s}"):
            if s < 3:
                for ch in range(2):
                    got(la_part(lo, c, ch), g_rs.at[2 * s, ch])
                    if s < 2 or ch == 0:
                        la_send(s + 1, lo, 0, ch)
                    la_push(2 * s + 1, lo, ch)
                    got(la_part(hi, c, ch), g_rs.at[2 * s + 1, ch])
                    if s < 2 or ch == 1:
                        la_send(s + 1, hi, 1, ch)
                    la_push(2 * s, hi, ch)
            else:
                for ch in range(2):
                    got(la_part(lo, c, ch), g_rs.at[6 + ch, ch])
                    la_push(6, lo, ch)
        if s == 0:
            finish(z)
        if s == 1:
            with jax.named_scope("w_sp"):
                got(sp, m_rs.at[7])
            s_all = sp[0]
            for n in range(1, 16):
                s_all = s_all + sp[n]
            sz[z] = s_all

            def give_sz(j, _):
                send(sz.at[z], sz.at[z], m_ss.at[8], m_rs.at[8], {"z": (z + j) % 8})
                return 0

            lax.fori_loop(1, 8, give_sz, 0)
        if s >= 1:
            for n in (2 * s - 2, 2 * s - 1):
                with jax.named_scope("w_las"):
                    for ch in range(2):
                        got(la_part(zblk(n + 1), 1 - c, ch), g_rs.at[8 + n, ch])
                with jax.named_scope("finish"):
                    finish(zblk(n + 1))
    with jax.named_scope("w_las"):
        for ch in range(2):
            got(la_part(zblk(7), 1 - c, ch), g_rs.at[14, ch])
    with jax.named_scope("finish"):
        finish(zblk(7))
    outs = []
    for lo in range(0, 600, 200):
        for n in range(10):
            w = 128 if n < 9 else 48
            stage[pl.ds(lo, 200), pl.ds(128 * n, w)] = res[n, pl.ds(lo, 200), pl.ds(0, w)]
        p = pl.ds(lo, 200)
        outs.append(pltpu.make_async_copy(stage.at[p], out_ref.at[p], loc.at[3 + lo // 200]))
        outs[-1].start()
    with jax.named_scope("w_sz"):
        got(sz.at[pl.ds(0, 7)], m_rs.at[8])
    s_all = sz[0]
    for n in range(1, 8):
        s_all = s_all + sz[n]
    s_all = jnp.sqrt(s_all / (8 * 1200 * 1200) + EPS)
    rms_ref[0, 0] = s_all[0, 0]
    with jax.named_scope('w_out'):
        for o in outs:
            o.wait()

    for s in range(4):
        for d in range(2):
            i = 2 * s + d
            if s < 3:
                left(rows(0, 0, 32), r_ss.at[i])
                left(rows(0, 0, 32), r_ss.at[8 + i])
                left(tt.at[0], t_ss.at[i])
                for ch in range(2):
                    left(la_part(0, 0, ch), g_ss.at[i, ch])
            else:
                left(rows(0, 0, 32), r_ss.at[i])
                left(tt.at[0, pl.ds(0, 48 - 16 * d)], t_ss.at[i])
                left(la_part(0, 0, d), g_ss.at[i, d])
    for n in range(8):
        left(tt.at[0], u_ss.at[n])
    for n in range(7):
        for ch in range(2):
            left(la_part(0, 0, ch), g_ss.at[8 + n, ch])
    for n in (0, 1):
        left(rows(0, 0, 16), c_ss.at[n])
        left(xb.at[0, pl.ds(0, 16), pl.ds(0, 256)], c_ss.at[2 + n])
        left(rows(0, 0, 64), c_ss.at[4 + n])
        left(rows(0, 0, 32), c_ss.at[6 + n])
        left(rows(0, 0, 256), c_ss.at[8 + n])
        left(rows(0, 0, 256), c_ss.at[10 + n])
        left(rows(0, 0, 256), c_ss.at[12 + n])
        left(rows(0, 0, 128), c_ss.at[14 + n])

    def drain(k, _):
        for o in (0, 8):
            for n, cnt in ((0, 32), (2, 16), (4, 128), (6, 64)):
                left(rows(0, 0, cnt), x_ss.at[k, o + n])
                left(rows(0, 0, cnt), x_ss.at[k, o + n + 1])
        return 0

    lax.fori_loop(0, 8, drain, 0)

    @pl.when(c == y % 2)
    def _():
        left(zt_ref.at[pl.ds(0, 480)], m_ss.at[0])

    @pl.when(c != y % 2)
    def _():
        left(zt_ref, m_ss.at[0])

    left(hs.at[pl.ds(0, 15)], m_ss.at[1])
    left(hb.at[0], m_ss.at[2])
    left(rb, m_ss.at[3])
    for h, (lo, n) in enumerate(pieces):
        left(bs.at[pl.ds(0, 15), pl.ds(lo, n)], p_ss.at[h])
        for d in range(1, 8):
            left(ls.at[0, pl.ds(lo, n)], q_ss.at[h, d])
    left(lt, m_ss.at[6])
    left(sp.at[pl.ds(0, 15)], m_ss.at[7])
    left(sz.at[pl.ds(0, 7)], m_ss.at[8])


def shards(amplitudes, factors, kernel, other_terms, virt_energy, pair_energy):
    t = jnp.transpose(amplitudes, (1, 0, 2)).reshape(600, 75)
    other = jnp.transpose(other_terms, (1, 0, 2)).reshape(600, 1200)
    vm = pl.BlockSpec(memory_space=pltpu.VMEM)
    sm = pl.BlockSpec(memory_space=pltpu.SMEM)
    V = pltpu.VMEM
    dma = pltpu.SemaphoreType.DMA
    out, rms = pl.pallas_call(
        ladder_kernel,
        out_shape=(
            jax.ShapeDtypeStruct((600, 1200), F32),
            jax.ShapeDtypeStruct((1, 1), F32),
        ),
        in_specs=[vm, vm, vm, pl.BlockSpec(memory_space=pl.ANY), vm, sm],
        out_specs=(pl.BlockSpec(memory_space=pl.ANY), sm),
        scratch_shapes=[
            V((600, 1200), F32),
            V((10, 600, 128), F32),
            V((512, 512), BF),
            V((8, 1280), F32),
            V((8, 1280, 512), BF),
            V((16, 80, 640), BF),
            V((1280, 640), BF),
            V((2, 640, 128), F32),
            V((16, 80, 256), BF),
            V((2, 16, 80, 256), BF),
            V((512, 1280), BF),
            V((8, 2, 32, 512), BF),
            V((512, 512), BF),
            V((512, 1280), F32),
            V((256, 1280), F32),
            V((16, 80, 256), BF),
            V((16, 80, 256), BF),
            V((8, 80, 512), BF),
            V((8, 80, 512), BF),
            V((1280, 128), F32),
            V((1280, 128), F32),
            V((1280, 128), F32),
            V((8, 80, 1280), BF),
            V((8, 128), F32),
            V((16, 8, 128), F32),
            V((8, 8, 128), F32),
            dma((8, 16)), dma((8, 16)),
            dma((16,)), dma((16,)),
            dma((16,)), dma((16,)),
            dma((8,)), dma((8,)),
            dma((8,)), dma((8,)),
            dma((16, 2)), dma((16, 2)),
            dma((16,)), dma((16,)),
            dma((2,)), dma((2,)),
            dma((2, 8)), dma((2, 8)),
            dma((12,)),
        ],
        compiler_params=pltpu.CompilerParams(
            collective_id=0, has_side_effects=True, vmem_limit_bytes=60 * 1024 * 1024
        ),
        name="ladder",
    )(factors, t, kernel, other, virt_energy[None, :], pair_energy)
    return jnp.transpose(out.reshape(75, 8, 1200), (1, 0, 2)), rms.reshape(())


def solution(mesh):
    torus = Mesh(mesh.devices.reshape(4, 4, 8, 2), ("x", "y", "z", "core"))
    plane, rank = ("x", "y"), ("z", "core")
    return jax.shard_map(
        shards,
        mesh=torus,
        in_specs=(P(None, plane, rank), P(plane, rank), P(plane, rank), P(None, plane, None), P(), P()),
        out_specs=(P(None, plane, None), P()),
        check_vma=False,
    )
```

```python
import functools

import jax
import jax.numpy as jnp
from jax import lax
from jax.experimental import pallas as pl
from jax.experimental.pallas import tpu as pltpu
from jax.sharding import Mesh
from jax.sharding import PartitionSpec as P

MESH = pl.DeviceIdType.MESH
BF = jnp.bfloat16
F32 = jnp.float32
EPS = 1e-06
NT = (((1,), (1,)), ((), ()))
TN = (((0,), (0,)), ((), ()))
TICKS = 12
READY = 6
FAR = sorted(((i, j) for i in range(4) for j in range(4) if i or j), key=lambda p: -min(p[0], 4 - p[0]) - min(p[1], 4 - p[1]))


def roll(a, shift):
    shift %= 128
    return a if shift == 0 else pltpu.roll(a, shift, 1)


def ladder_kernel(
    f_ref, t_ref, k_ref, other_hbm, e_ref, ep_ref, out_ref, rms_ref,
    stage, res, zt_ref, er,
    xb, tt, ttp, half, hs, hb, ht, zb_ref, wt, acc, rb, bs, br, ls, lb, lt, ltr, lc, la, sc, sp, sz,
    x_ss, x_rs, c_ss, c_rs, r_ss, r_rs, t_ss, t_rs, u_ss, u_rs, g_ss, g_rs, m_ss, m_rs, p_ss, p_rs, q_ss, q_rs, loc,
):
    x, y, z, c = (lax.axis_index(n) for n in ("x", "y", "z", "core"))
    v = 4 * x + y
    xp, xm = (x + 1) % 4, (x + 3) % 4
    yp, ym = (y + 1) % 4, (y + 3) % 4
    zp, zm = (z + 1) % 8, (z + 7) % 8
    sib = {"core": 1 - c}

    def rows(i, off, n, w=512, lo=0):
        return xb.at[i, pl.ds(pl.multiple_of(off, 16), n), pl.ds(lo, w)]

    def send(src, dst, ss, rs, dev):
        pltpu.make_async_remote_copy(
            src_ref=src, dst_ref=dst, send_sem=ss, recv_sem=rs, device_id=dev, device_id_type=MESH
        ).start()

    def got(dst, rs):
        pltpu.make_async_remote_copy(
            src_ref=dst, dst_ref=dst, send_sem=rs, recv_sem=rs, device_id=sib, device_id_type=MESH
        ).wait_recv()

    def left(src, ss):
        pltpu.make_async_remote_copy(
            src_ref=src, dst_ref=src, send_sem=ss, recv_sem=ss, device_id=sib, device_id_type=MESH
        ).wait_send()

    def a_off(i, j):
        return i * 128 + j * 32

    def b_off(i, j):
        return 512 + j * 128 + i * 32

    def c_off(i, j):
        return 1024 + i * 64 + j * 16

    own = [
        pltpu.make_async_copy(f_ref.at[pl.ds(0, 32)], rows(z, a_off(x, y), 32), loc.at[0]),
        pltpu.make_async_copy(f_ref.at[pl.ds(32, 32)], rows(z, b_off(x, y), 32), loc.at[1]),
    ]
    for o in own:
        o.start()

    others = pltpu.make_async_copy(other_hbm, stage, loc.at[2])
    others.start()

    bar = pltpu.get_barrier_semaphore()

    def plane_dev(j, core):
        w = (v + j) % 16
        return {"x": w // 4, "y": w % 4, "core": core}

    def greet(j, _):
        pl.semaphore_signal(bar, inc=1, device_id=plane_dev(j, c), device_id_type=MESH)
        pl.semaphore_signal(bar, inc=1, device_id=plane_dev(j, 1 - c), device_id_type=MESH)
        return 0

    lax.fori_loop(1, 16, greet, 0)
    pl.semaphore_signal(bar, inc=1, device_id=sib, device_id_type=MESH)

    def greet_z(j, _):
        pl.semaphore_signal(bar, inc=1, device_id={"z": (z + j) % 8}, device_id_type=MESH)
        return 0

    lax.fori_loop(1, 8, greet_z, 0)
    with jax.named_scope("local"):
        last = jnp.concatenate([f_ref[pl.ds(64, 11), :].astype(F32), jnp.zeros((5, 512), F32)], 0)
        xb[z, pl.ds(pl.multiple_of(c_off(x, y), 16), 16), :] = last.astype(BF)
        for n in range(5):
            cnt = 128 if n < 4 else 88
            m = t_ref[pl.ds(128 * n, cnt), :].astype(F32)
            if cnt < 128:
                m = jnp.concatenate([m, jnp.zeros((128 - cnt, 75), F32)], 0)
            m = jnp.concatenate([m.T, jnp.zeros((5, 128), F32)], 0)
            tt[2 * z + c, :, pl.ds(128 * n, 128)] = m.astype(BF)
        for n in range(4):
            zt_ref[:, pl.ds(128 * n, 128)] = k_ref[pl.ds(128 * n, 128), :].astype(F32).T.astype(BF)
        er[:, pl.ds(0, 1200)] = jnp.broadcast_to(e_ref[...], (8, 1200))
        er[:, pl.ds(1200, 80)] = jnp.zeros((8, 80), F32)
        others.wait()
        for n in range(10):
            w = 128 if n < 9 else 48
            res[n, :, pl.ds(0, w)] = stage[:, pl.ds(128 * n, w)]
    for o in own:
        o.wait()
    with jax.named_scope('barrier'):
        pl.semaphore_wait(bar, 38)

    def zblk(k):
        return (z + ((k + 1) // 2) * (2 * (k % 2) - 1) + 8) % 8

    def ring_pieces(s, d, blk):
        a, b = rows(blk, a_off(x, y), 32, 384), rows(blk, b_off(x, y), 32, 384)
        return ((a, 2 * s + d), (b, 8 + 2 * s + d)) if s < 3 else (((a, b)[d], 6 + d),)

    def t_piece(s, d, blk):
        r = 2 * blk + c
        return tt.at[r] if s < 3 else tt.at[r, pl.ds(48 * d, 48 - 16 * d)]

    def ring_step(s, zl, zr):
        for d, blk in enumerate((zl, zr)):
            for p, i in ring_pieces(s, d, blk):
                send(p, p, r_ss.at[i], r_rs.at[i], {"z": (zp, zm)[d]})

    def t_step(s, zl, zr):
        for d, blk in enumerate((zl, zr)):
            p = t_piece(s, d, blk)
            send(p, p, t_ss.at[2 * s + d], t_rs.at[2 * s + d], {"z": (zp, zm)[d]})

    def push_t(n, blk):
        r = 2 * blk + c
        send(tt.at[r], tt.at[r], u_ss.at[n], u_rs.at[n], sib)

    def ring_got(s):
        lo, hi = (z + 7 - s) % 8, (z + 1 + s) % 8
        for d, blk in enumerate((lo, hi)):
            for p, i in ring_pieces(s, d, blk):
                got(p, r_rs.at[i])
        return lo, hi

    def t_got(s):
        lo, hi = (z + 7 - s) % 8, (z + 1 + s) % 8
        for d, blk in enumerate((lo, hi)):
            got(t_piece(s, d, blk), t_rs.at[2 * s + d])
        return lo, hi

    ring_step(0, z, z)
    t_step(0, z, z)
    push_t(0, z)

    def c_piece(i, j, h):
        return xb.at[z, pl.ds(pl.multiple_of(c_off(i, j), 16), 16), pl.ds(256 * h, 256)]

    def c_step(s):
        if s == 0:
            p = rows(z, c_off(x, y), 16)
            send(p, p, c_ss.at[0], c_rs.at[0], {"y": yp})
            send(p, p, c_ss.at[1], c_rs.at[1], {"y": ym})
        elif s == 1:
            got(rows(z, c_off(x, ym), 16), c_rs.at[0])
            got(rows(z, c_off(x, yp), 16), c_rs.at[1])
            p, q = c_piece(x, ym, 0), c_piece(x, yp, 1)
            send(p, p, c_ss.at[2], c_rs.at[2], {"y": yp})
            send(q, q, c_ss.at[3], c_rs.at[3], {"y": ym})
        elif s == 2:
            got(c_piece(x, (y + 2) % 4, 0), c_rs.at[2])
            got(c_piece(x, (y + 2) % 4, 1), c_rs.at[3])
            p = rows(z, c_off(x, 0), 64)
            send(p, p, c_ss.at[4], c_rs.at[4], {"x": xp})
            send(p, p, c_ss.at[5], c_rs.at[5], {"x": xm})
        elif s == 3:
            got(rows(z, c_off(xm, 0), 64), c_rs.at[4])
            got(rows(z, c_off(xp, 0), 64), c_rs.at[5])
            p, q = rows(z, c_off(xm, 0), 32), rows(z, c_off(xp, 2), 32)
            send(p, p, c_ss.at[6], c_rs.at[6], {"x": xp})
            send(q, q, c_ss.at[7], c_rs.at[7], {"x": xm})
        else:
            g = s - 5
            if s == 4:
                got(rows(z, c_off((x + 2) % 4, 0), 32), c_rs.at[6])
                got(rows(z, c_off((x + 2) % 4, 2), 32), c_rs.at[7])
            else:
                for d, blk in enumerate(((z + 7 - g) % 8, (z + 1 + g) % 8)):
                    for p, i in c_ring(g, d, blk):
                        got(p, c_rs.at[i])
            if s < 8:
                g += 1
                for d, blk in enumerate(((z + 8 - g) % 8, (z + g) % 8)):
                    for p, i in c_ring(g, d, blk):
                        send(p, p, c_ss.at[i], c_rs.at[i], {"z": (zp, zm)[d]})

    def c_ring(g, d, blk):
        n = 1 if g < 3 else 2
        return (
            (rows(blk, 1024 + (0 if n == 1 else 128 * d), 256 // n), 8 + 2 * g + d),
            (rows(blk, 0 if n == 1 else 512 * d, 1024 // n, 128, 384), 16 + 2 * g + d),
        )

    def s1(k, w=384):
        b = zblk(k)
        p, q = rows(b, a_off(x, y), 32, w), rows(b, b_off(x, y), 32, w)
        send(p, p, x_ss.at[k, 0], x_rs.at[k, 0], {"y": yp})
        send(p, p, x_ss.at[k, 1], x_rs.at[k, 1], {"y": ym})
        send(q, q, x_ss.at[k, 8], x_rs.at[k, 8], {"x": xp})
        send(q, q, x_ss.at[k, 9], x_rs.at[k, 9], {"x": xm})

    def s2(k, w=384):
        b = zblk(k)
        got(rows(b, a_off(x, ym), 32, w), x_rs.at[k, 0])
        got(rows(b, a_off(x, yp), 32, w), x_rs.at[k, 1])
        p, q = rows(b, a_off(x, ym), 16, w), rows(b, a_off(x, yp) + 16, 16, w)
        send(p, p, x_ss.at[k, 2], x_rs.at[k, 2], {"y": yp})
        send(q, q, x_ss.at[k, 3], x_rs.at[k, 3], {"y": ym})
        got(rows(b, b_off(xm, y), 32, w), x_rs.at[k, 8])
        got(rows(b, b_off(xp, y), 32, w), x_rs.at[k, 9])
        p, q = rows(b, b_off(xm, y), 16, w), rows(b, b_off(xp, y) + 16, 16, w)
        send(p, p, x_ss.at[k, 10], x_rs.at[k, 10], {"x": xp})
        send(q, q, x_ss.at[k, 11], x_rs.at[k, 11], {"x": xm})

    def s3(k, w=384):
        b = zblk(k)
        y2, x2 = (y + 2) % 4, (x + 2) % 4
        got(rows(b, a_off(x, y2), 16, w), x_rs.at[k, 2])
        got(rows(b, a_off(x, y2) + 16, 16, w), x_rs.at[k, 3])
        p = rows(b, a_off(x, 0), 128, w)
        send(p, p, x_ss.at[k, 4], x_rs.at[k, 4], {"x": xp})
        send(p, p, x_ss.at[k, 5], x_rs.at[k, 5], {"x": xm})
        got(rows(b, b_off(x2, y), 16, w), x_rs.at[k, 10])
        got(rows(b, b_off(x2, y) + 16, 16, w), x_rs.at[k, 11])
        p = rows(b, b_off(0, y), 128, w)
        send(p, p, x_ss.at[k, 12], x_rs.at[k, 12], {"y": yp})
        send(p, p, x_ss.at[k, 13], x_rs.at[k, 13], {"y": ym})

    def s4(k, w=384):
        b = zblk(k)
        got(rows(b, a_off(xm, 0), 128, w), x_rs.at[k, 4])
        got(rows(b, a_off(xp, 0), 128, w), x_rs.at[k, 5])
        p, q = rows(b, a_off(xm, 0), 64, w), rows(b, a_off(xp, 2), 64, w)
        send(p, p, x_ss.at[k, 6], x_rs.at[k, 6], {"x": xp})
        send(q, q, x_ss.at[k, 7], x_rs.at[k, 7], {"x": xm})
        got(rows(b, b_off(0, ym), 128, w), x_rs.at[k, 12])
        got(rows(b, b_off(0, yp), 128, w), x_rs.at[k, 13])
        p, q = rows(b, b_off(0, ym), 64, w), rows(b, b_off(2, yp), 64, w)
        send(p, p, x_ss.at[k, 14], x_rs.at[k, 14], {"y": yp})
        send(q, q, x_ss.at[k, 15], x_rs.at[k, 15], {"y": ym})

    def s5(k, w=384):
        b = zblk(k)
        y2, x2 = (y + 2) % 4, (x + 2) % 4
        got(rows(b, a_off(x2, 0), 64, w), x_rs.at[k, 6])
        got(rows(b, a_off(x2, 2), 64, w), x_rs.at[k, 7])
        got(rows(b, b_off(0, y2), 64, w), x_rs.at[k, 14])
        got(rows(b, b_off(2, y2), 64, w), x_rs.at[k, 15])

    def send_kernel():
        kc = y % 2

        def one(j, _):
            w = (v + j) % 16
            src = zt_ref.at[pl.ds(pl.multiple_of(32 * w, 32), 32)]
            send(src, zb_ref.at[v // 2, c], m_ss.at[0], m_rs.at[0], plane_dev(j, kc))
            return 0

        lax.fori_loop(1, 16, one, 0)
        src = zt_ref.at[pl.ds(pl.multiple_of(32 * v, 32), 32)]

        @pl.when(c == kc)
        def _():
            pltpu.make_async_copy(src, zb_ref.at[v // 2, c], m_rs.at[0]).start()

        @pl.when(c != kc)
        def _():
            send(src, zb_ref.at[v // 2, c], m_ss.at[0], m_rs.at[0], sib)

    def make_half():
        for n in range(1, 8):
            b = zblk(n)
            got(tt.at[2 * b + 1 - c], u_rs.at[n])
        got(tt.at[2 * z + 1 - c], u_rs.at[0])
        for i in range(4):
            for j in range(4):
                w = 4 * i + j
                ttp[pl.ds(a_off(i, j), 32), :] = tt[w, pl.ds(0, 32), :]
                ttp[pl.ds(b_off(i, j), 32), :] = tt[w, pl.ds(32, 32), :]
                ttp[pl.ds(c_off(i, j), 16), :] = tt[w, pl.ds(64, 16), :]
        lanes = lax.broadcasted_iota(jnp.int32, (80, 128), 1) // 32

        def chunk(a, _):
            q = pl.ds(pl.multiple_of(256 * a, 256), 256)
            m = lax.dot_general(ttp[...], xb[z, :, q], TN, preferred_element_type=F32)
            half[0] = m[:, :128]
            half[1] = m[:, 128:]
            for h in range(2):
                for g in range(2):
                    part = [half[h, pl.ds(4 * g + k, 80, stride=8), :] for k in range(4)]
                    for s in range(4):
                        m = roll(part[0], (0 - s) * 32)
                        for k in range(1, 4):
                            m = jnp.where(lanes == k, roll(part[k], (k - s) * 32), m)
                        hs[8 * a + 4 * h + s, :, pl.ds(128 * g, 128)] = m.astype(BF)
            return 0

        lax.fori_loop(0, 2, chunk, 0)

        def one(j, _):
            send(hs.at[(v + j) % 16], hb.at[c, v], m_ss.at[1], m_rs.at[1], plane_dev(j, c))
            return 0

        lax.fori_loop(1, 16, one, 0)
        pltpu.make_async_copy(hs.at[v], hb.at[c, v], m_rs.at[1]).start()

    def take_half():
        with jax.named_scope('w_hb'):
            got(hb.at[c], m_rs.at[1])
        send(hb.at[c], hb.at[c], m_ss.at[2], m_rs.at[2], sib)
        acc[...] = jnp.zeros_like(acc)
        with jax.named_scope('w_hbs'):
            got(hb.at[1 - c], m_rs.at[2])
        for s in range(2):
            to = pl.ds(256 * s, 256)
            for i in range(4):
                m = jnp.concatenate([hb[s, 4 * i + j, pl.ds(0, 32), :] for j in range(4)], 0)
                ht[to, pl.ds(128 * i, 128)] = m.astype(F32).T.astype(BF)
                m = jnp.concatenate([hb[s, 4 * j + i, pl.ds(32, 32), :] for j in range(4)], 0)
                ht[to, pl.ds(512 + 128 * i, 128)] = m.astype(F32).T.astype(BF)
            for i in range(2):
                m = jnp.concatenate([hb[s, 8 * i + j, pl.ds(64, 16), :] for j in range(8)], 0)
                ht[to, pl.ds(1024 + 128 * i, 128)] = m.astype(F32).T.astype(BF)
        with jax.named_scope('w_zb'):
            got(zb_ref, m_rs.at[0])

    def compute(k, _):
        b = zblk(k)
        for q in range(2):
            q = pl.ds(256 * q, 256)
            cp = jnp.dot(ht[...], xb[b, :, q], preferred_element_type=F32)
            zz = zb_ref[b, :, :, q].astype(F32)
            for s in range(2):
                for i in range(8):
                    o = 256 * s + 32 * i
                    wt[pl.ds(o, 32), q] = (cp[o : o + 32] * zz[s]).astype(BF)
        for a in range(5):
            a = pl.ds(256 * a, 256)
            acc[:, a] += lax.dot_general(wt[...], xb[b, a, :], NT, preferred_element_type=F32)
        return 0

    def on(cond, name, f, *args):
        @pl.when(cond)
        def _():
            with jax.named_scope(name):
                f(*args)

    def forward(s):
        lo, hi = ring_got(s - 1)
        if s < 4:
            ring_step(s, lo, hi)

    def forward_t(s):
        lo, hi = t_got(s - 1)
        if s < 4:
            t_step(s, lo, hi)
            push_t(2 * s - 1, hi)
            push_t(2 * s, lo)
        else:
            push_t(7, lo)

    def tick(t, _):
        for s in range(1, 5):
            on(t == s, "forward", forward, s)
        on(t == 4, "s5", s5, 0, 512)
        on(t > 4, "s5", s5, t - 4)
        for s in range(5):
            on(t == s, "c_step", c_step, s)
        on(t == 3, "s4", s4, 0, 512)
        on((t > 3) & (t < 11), "s4", s4, t - 3)
        on(t == 2, "s3", s3, 0, 512)
        on((t > 2) & (t < 10), "s3", s3, t - 2)
        on(t == 1, "s2", s2, 0, 512)
        on((t > 1) & (t < 9), "s2", s2, t - 1)
        on(t == 0, "s1", s1, 0, 512)
        on((t > 0) & (t < 8), "s1", s1, t)
        on(t == 0, "send_kernel", send_kernel)
        for s in range(1, 5):
            on(t == s, "forward_t", forward_t, s)
        on(t == 4, "make_half", make_half)
        for s in range(5, 8):
            on(t == 2 * s - 4, "c_step", c_step, s)
        on(t == READY, "take_half", take_half)
        with jax.named_scope("compute"):
            lo = jnp.maximum(t - READY, 0)
            hi = jnp.maximum(t - READY + 1, 0) + (t >= 11).astype(jnp.int32)
            lax.fori_loop(lo, hi, compute, 0)
        return 0

    lax.fori_loop(0, TICKS, tick, 0)
    with jax.named_scope('c_step'):
        c_step(8)
    with jax.named_scope('compute'):
        compute(7, 0)

    mine = pl.ds(pl.multiple_of(256 * c, 256), 256)
    give = acc.at[pl.ds(pl.multiple_of(256 * (1 - c), 256), 256)]
    send(give, rb, m_ss.at[3], m_rs.at[3], sib)
    with jax.named_scope('w_rb'):
        got(rb, m_rs.at[3])
    for n in range(10):
        a = pl.ds(128 * n, 128)
        m = (acc[mine, a] + rb[:, a]).T.astype(BF)
        if n < 4:
            for j in range(4):
                bs[4 * n + j, pl.ds(0, 32), :] = m[32 * j : 32 * j + 32]
        elif n < 8:
            for j in range(4):
                bs[4 * j + n - 4, pl.ds(32, 32), :] = m[32 * j : 32 * j + 32]
        else:
            for j in range(8):
                bs[8 * (n - 8) + j, pl.ds(64, 16), :] = m[16 * j : 16 * j + 16]

    pieces = ((0, 32), (32, 48))
    for h, (lo, n) in enumerate(pieces):

        for i, j in FAR:
            i, j = (x + i) % 4, (y + j) % 4
            w = 4 * i + j
            send(bs.at[w, pl.ds(lo, n)], br.at[v, pl.ds(lo, n)], p_ss.at[h], p_rs.at[h], {"x": i, "y": j})
        pltpu.make_async_copy(bs.at[v, pl.ds(lo, n)], br.at[v, pl.ds(lo, n)], p_rs.at[h]).start()

    for h, (lo, n) in enumerate(pieces):
        with jax.named_scope("w_br"):
            got(br.at[:, pl.ds(lo, n)], p_rs.at[h])
        with jax.named_scope("unpack"):
            lanes = lax.broadcasted_iota(jnp.int32, (n, 128), 1) // 32
            for g in range(2):
                for a in range(4):
                    part = [br[4 * a + s, pl.ds(lo, n), pl.ds(128 * g, 128)].astype(F32) for s in range(4)]
                    for k in range(4):
                        m = roll(part[0], (0 - k) * 32)
                        for s in range(1, 4):
                            m = jnp.where(lanes == s, roll(part[s], (s - k) * 32), m)
                        ls[4 * g + k, pl.ds(lo, n), pl.ds(128 * a, 128)] = m.astype(BF)
        for d in (4, 3, 5, 2, 6, 1, 7):
            w = (z + d) % 8
            send(ls.at[w, pl.ds(lo, n)], lb.at[z, pl.ds(lo, n)], q_ss.at[h, d], q_rs.at[h, d], {"z": w})
        if h == 0:
            lt[...] = jnp.zeros_like(lt)

    def lad(b, src):
        for a in range(5):
            a = pl.ds(256 * a, 256)
            lt[a, pl.ds(0, 80)] += lax.dot_general(xb[b, a, :], src[b], NT, preferred_element_type=F32)

    lad(z, ls)

    def lad_step(j, _):
        d = 4 + ((j + 1) // 2) * (1 - 2 * (j % 2))
        b = (z + 8 - d) % 8
        with jax.named_scope("w_lb"):
            for h, (lo, n) in enumerate(pieces):
                got(lb.at[b, pl.ds(lo, n)], q_rs.at[h, d])
        with jax.named_scope("w_lad"):
            lad(b, lb)
        return 0

    lax.fori_loop(0, 7, lad_step, 0)
    send(lt, ltr, m_ss.at[6], m_rs.at[6], sib)
    ea = pltpu.roll(er[...], (1280 - 75 * v) % 1280, 1)[:, :128].T[:75, 0:1]
    with jax.named_scope("w_ltr"):
        got(ltr, m_rs.at[6])
    lc[pl.ds(1200, 80), :] = jnp.zeros((80, 128), F32)
    for i in range(4):
        for j in range(4):
            o = 75 * (4 * i + j)
            for n, off, cnt in ((0, a_off(i, j), 32), (32, b_off(i, j), 32), (64, c_off(i, j), 11)):
                lc[pl.ds(o + n, cnt), :] = lt[pl.ds(off, cnt), :] + ltr[pl.ds(off, cnt), :]
    for n in range(10):
        b = pl.ds(128 * n, 128)
        la[z, :, b] = lc[b, :].T[:80].astype(BF)

    chunks = ((0, 48), (48, 32))

    def la_part(i, h, ch):
        lo, n = chunks[ch]
        return la.at[i, pl.ds(lo, n), pl.ds(pl.multiple_of(640 * h, 128), 640)]

    def la_send(s, blk, d, ch):
        p = la_part(blk, c, ch)
        send(p, p, g_ss.at[2 * s + d, ch], g_rs.at[2 * s + d, ch], {"z": (zp, zm)[d]})

    def la_push(n, blk, ch):
        p = la_part(blk, c, ch)
        send(p, p, g_ss.at[8 + n, ch], g_rs.at[8 + n, ch], sib)

    for ch in range(2):
        for d in range(2):
            la_send(0, z, d, ch)

    total = jnp.zeros((75, 128), F32)
    ep = ep_ref[z]
    for n in range(10):
        w = 128 if n < 9 else 48
        b = pl.ds(128 * n, w)
        den = ea + er[0:1, b] - ep
        u = (res[n, pl.ds(z, 75, stride=8), :] + lc[pl.ds(128 * n, 128), :].T[:75])[:, :w] / den
        u = u * u
        if w < 128:
            u = jnp.concatenate([u, jnp.zeros((75, 128 - w), F32)], 1)
        total = total + u
    sc[...] = jnp.full((8, 128), jnp.sum(total), F32)

    def give_sum(j, _):
        send(sc, sp.at[v], m_ss.at[7], m_rs.at[7], plane_dev(j, c))
        return 0

    lax.fori_loop(1, 16, give_sum, 0)
    pltpu.make_async_copy(sc, sp.at[v], m_rs.at[7]).start()

    def finish(i):
        o = pl.ds(i, 75, stride=8)
        for n in range(10):
            b = pl.ds(128 * n, 128)
            res[n, o, :] = res[n, o, :] + la[i, :, b].astype(F32)[:75]

    for s in range(4):
        lo, hi = (z + 7 - s) % 8, (z + 1 + s) % 8
        with jax.named_scope(f"w_la{s}"):
            if s < 3:
                for ch in range(2):
                    got(la_part(lo, c, ch), g_rs.at[2 * s, ch])
                    if s < 2 or ch == 0:
                        la_send(s + 1, lo, 0, ch)
                    la_push(2 * s + 1, lo, ch)
                    got(la_part(hi, c, ch), g_rs.at[2 * s + 1, ch])
                    if s < 2 or ch == 1:
                        la_send(s + 1, hi, 1, ch)
                    la_push(2 * s, hi, ch)
            else:
                for ch in range(2):
                    got(la_part(lo, c, ch), g_rs.at[6 + ch, ch])
                    la_push(6, lo, ch)
        if s == 0:
            finish(z)
        if s == 1:
            with jax.named_scope("w_sp"):
                got(sp, m_rs.at[7])
            s_all = sp[0]
            for n in range(1, 16):
                s_all = s_all + sp[n]
            sz[z] = s_all

            def give_sz(j, _):
                send(sz.at[z], sz.at[z], m_ss.at[8], m_rs.at[8], {"z": (z + j) % 8})
                return 0

            lax.fori_loop(1, 8, give_sz, 0)
        if s >= 1:
            for n in (2 * s - 2, 2 * s - 1):
                with jax.named_scope("w_las"):
                    for ch in range(2):
                        got(la_part(zblk(n + 1), 1 - c, ch), g_rs.at[8 + n, ch])
                with jax.named_scope("finish"):
                    finish(zblk(n + 1))
    with jax.named_scope("w_las"):
        for ch in range(2):
            got(la_part(zblk(7), 1 - c, ch), g_rs.at[14, ch])
    with jax.named_scope("finish"):
        finish(zblk(7))
    outs = []
    for lo in range(0, 600, 200):
        for n in range(10):
            w = 128 if n < 9 else 48
            stage[pl.ds(lo, 200), pl.ds(128 * n, w)] = res[n, pl.ds(lo, 200), pl.ds(0, w)]
        p = pl.ds(lo, 200)
        outs.append(pltpu.make_async_copy(stage.at[p], out_ref.at[p], loc.at[3 + lo // 200]))
        outs[-1].start()
    with jax.named_scope("w_sz"):
        got(sz.at[pl.ds(0, 7)], m_rs.at[8])
    s_all = sz[0]
    for n in range(1, 8):
        s_all = s_all + sz[n]
    s_all = jnp.sqrt(s_all / (8 * 1200 * 1200) + EPS)
    rms_ref[0, 0] = s_all[0, 0]
    with jax.named_scope('w_out'):
        for o in outs:
            o.wait()

    for s in range(4):
        for d in range(2):
            i = 2 * s + d
            if s < 3:
                left(rows(0, 0, 32, 384), r_ss.at[i])
                left(rows(0, 0, 32, 384), r_ss.at[8 + i])
                left(tt.at[0], t_ss.at[i])
                for ch in range(2):
                    left(la_part(0, 0, ch), g_ss.at[i, ch])
            else:
                left(rows(0, 0, 32, 384), r_ss.at[i])
                left(tt.at[0, pl.ds(0, 48 - 16 * d)], t_ss.at[i])
                left(la_part(0, 0, d), g_ss.at[i, d])
    for n in range(8):
        left(tt.at[0], u_ss.at[n])
    for n in range(7):
        for ch in range(2):
            left(la_part(0, 0, ch), g_ss.at[8 + n, ch])
    for n in (0, 1):
        left(rows(0, 0, 16), c_ss.at[n])
        left(xb.at[0, pl.ds(0, 16), pl.ds(0, 256)], c_ss.at[2 + n])
        left(rows(0, 0, 64), c_ss.at[4 + n])
        left(rows(0, 0, 32), c_ss.at[6 + n])
        for g in range(4):
            for p, i in c_ring(g, n, 0):
                left(p, c_ss.at[i])

    def drain(k, w):
        for o in (0, 8):
            for n, cnt in ((0, 32), (2, 16), (4, 128), (6, 64)):
                left(rows(0, 0, cnt, w), x_ss.at[k, o + n])
                left(rows(0, 0, cnt, w), x_ss.at[k, o + n + 1])
        return w

    drain(0, 512)
    lax.fori_loop(1, 8, lambda k, _: drain(k, 384) * 0, 0)

    @pl.when(c == y % 2)
    def _():
        left(zt_ref.at[pl.ds(0, 480)], m_ss.at[0])

    @pl.when(c != y % 2)
    def _():
        left(zt_ref, m_ss.at[0])

    left(hs.at[pl.ds(0, 15)], m_ss.at[1])
    left(hb.at[0], m_ss.at[2])
    left(rb, m_ss.at[3])
    for h, (lo, n) in enumerate(pieces):
        left(bs.at[pl.ds(0, 15), pl.ds(lo, n)], p_ss.at[h])
        for d in range(1, 8):
            left(ls.at[0, pl.ds(lo, n)], q_ss.at[h, d])
    left(lt, m_ss.at[6])
    left(sp.at[pl.ds(0, 15)], m_ss.at[7])
    left(sz.at[pl.ds(0, 7)], m_ss.at[8])


def shards(amplitudes, factors, kernel, other_terms, virt_energy, pair_energy):
    t = jnp.transpose(amplitudes, (1, 0, 2)).reshape(600, 75)
    other = jnp.transpose(other_terms, (1, 0, 2)).reshape(600, 1200)
    vm = pl.BlockSpec(memory_space=pltpu.VMEM)
    sm = pl.BlockSpec(memory_space=pltpu.SMEM)
    V = pltpu.VMEM
    dma = pltpu.SemaphoreType.DMA
    out, rms = pl.pallas_call(
        ladder_kernel,
        out_shape=(
            jax.ShapeDtypeStruct((600, 1200), F32),
            jax.ShapeDtypeStruct((1, 1), F32),
        ),
        in_specs=[vm, vm, vm, pl.BlockSpec(memory_space=pl.ANY), vm, sm],
        out_specs=(pl.BlockSpec(memory_space=pl.ANY), sm),
        scratch_shapes=[
            V((600, 1200), F32),
            V((10, 600, 128), F32),
            V((512, 512), BF),
            V((8, 1280), F32),
            V((8, 1280, 512), BF),
            V((16, 80, 640), BF),
            V((1280, 640), BF),
            V((2, 640, 128), F32),
            V((16, 80, 256), BF),
            V((2, 16, 80, 256), BF),
            V((512, 1280), BF),
            V((8, 2, 32, 512), BF),
            V((512, 512), BF),
            V((512, 1280), F32),
            V((256, 1280), F32),
            V((16, 80, 256), BF),
            V((16, 80, 256), BF),
            V((8, 80, 512), BF),
            V((8, 80, 512), BF),
            V((1280, 128), F32),
            V((1280, 128), F32),
            V((1280, 128), F32),
            V((8, 80, 1280), BF),
            V((8, 128), F32),
            V((16, 8, 128), F32),
            V((8, 8, 128), F32),
            dma((8, 16)), dma((8, 16)),
            dma((24,)), dma((24,)),
            dma((16,)), dma((16,)),
            dma((8,)), dma((8,)),
            dma((8,)), dma((8,)),
            dma((16, 2)), dma((16, 2)),
            dma((16,)), dma((16,)),
            dma((2,)), dma((2,)),
            dma((2, 8)), dma((2, 8)),
            dma((12,)),
        ],
        compiler_params=pltpu.CompilerParams(
            collective_id=0, has_side_effects=True, vmem_limit_bytes=60 * 1024 * 1024
        ),
        name="ladder",
    )(factors, t, kernel, other, virt_energy[None, :], pair_energy)
    return jnp.transpose(out.reshape(75, 8, 1200), (1, 0, 2)), rms.reshape(())


def solution(mesh):
    torus = Mesh(mesh.devices.reshape(4, 4, 8, 2), ("x", "y", "z", "core"))
    plane, rank = ("x", "y"), ("z", "core")
    return jax.shard_map(
        shards,
        mesh=torus,
        in_specs=(P(None, plane, rank), P(plane, rank), P(plane, rank), P(None, plane, None), P(), P()),
        out_specs=(P(None, plane, None), P()),
        check_vma=False,
    )
```

```python
import functools

import jax
import jax.numpy as jnp
from jax import lax
from jax.experimental import pallas as pl
from jax.experimental.pallas import tpu as pltpu
from jax.sharding import Mesh
from jax.sharding import PartitionSpec as P

MESH = pl.DeviceIdType.MESH
BF = jnp.bfloat16
F32 = jnp.float32
EPS = 1e-06
NT = (((1,), (1,)), ((), ()))
TN = (((0,), (0,)), ((), ()))
TICKS = 14
READY = 6
FAR = sorted(((i, j) for i in range(4) for j in range(4) if i or j), key=lambda p: -min(p[0], 4 - p[0]) - min(p[1], 4 - p[1]))


def roll(a, shift):
    shift %= 128
    return a if shift == 0 else pltpu.roll(a, shift, 1)


def ladder_kernel(
    f_ref, t_ref, k_ref, other_hbm, e_ref, ep_ref, out_ref, rms_ref,
    stage, res, zt_ref, er,
    xb, tt, ttp, half, hs, hb, ht, zb_ref, wt, acc, rb, bs, br, ls, lb, lt, ltr, lc, la, sc, sp, sz,
    x_ss, x_rs, e_ss, e_rs, c_ss, c_rs, r_ss, r_rs, t_ss, t_rs, u_ss, u_rs, g_ss, g_rs, m_ss, m_rs, p_ss, p_rs, q_ss, q_rs, loc,
):
    x, y, z, c = (lax.axis_index(n) for n in ("x", "y", "z", "core"))
    v = 4 * x + y
    xp, xm = (x + 1) % 4, (x + 3) % 4
    yp, ym = (y + 1) % 4, (y + 3) % 4
    zp, zm = (z + 1) % 8, (z + 7) % 8
    sib = {"core": 1 - c}

    def rows(i, off, n, w=512, lo=0):
        return xb.at[i, pl.ds(pl.multiple_of(off, 16), n), pl.ds(lo, w)]

    def send(src, dst, ss, rs, dev):
        pltpu.make_async_remote_copy(
            src_ref=src, dst_ref=dst, send_sem=ss, recv_sem=rs, device_id=dev, device_id_type=MESH
        ).start()

    def got(dst, rs):
        pltpu.make_async_remote_copy(
            src_ref=dst, dst_ref=dst, send_sem=rs, recv_sem=rs, device_id=sib, device_id_type=MESH
        ).wait_recv()

    def left(src, ss):
        pltpu.make_async_remote_copy(
            src_ref=src, dst_ref=src, send_sem=ss, recv_sem=ss, device_id=sib, device_id_type=MESH
        ).wait_send()

    def a_off(i, j):
        return i * 128 + j * 32

    def b_off(i, j):
        return 512 + j * 128 + i * 32

    def c_off(i, j):
        return 1024 + i * 64 + j * 16

    own = [
        pltpu.make_async_copy(f_ref.at[pl.ds(0, 32)], rows(z, a_off(x, y), 32), loc.at[0]),
        pltpu.make_async_copy(f_ref.at[pl.ds(32, 32)], rows(z, b_off(x, y), 32), loc.at[1]),
    ]
    for o in own:
        o.start()

    others = pltpu.make_async_copy(other_hbm, stage, loc.at[2])
    others.start()

    bar = pltpu.get_barrier_semaphore()

    def plane_dev(j, core):
        w = (v + j) % 16
        return {"x": w // 4, "y": w % 4, "core": core}

    def greet(j, _):
        pl.semaphore_signal(bar, inc=1, device_id=plane_dev(j, c), device_id_type=MESH)
        pl.semaphore_signal(bar, inc=1, device_id=plane_dev(j, 1 - c), device_id_type=MESH)
        return 0

    lax.fori_loop(1, 16, greet, 0)
    pl.semaphore_signal(bar, inc=1, device_id=sib, device_id_type=MESH)

    def greet_z(j, _):
        pl.semaphore_signal(bar, inc=1, device_id={"z": (z + j) % 8}, device_id_type=MESH)
        return 0

    lax.fori_loop(1, 8, greet_z, 0)
    with jax.named_scope("local"):
        last = jnp.concatenate([f_ref[pl.ds(64, 11), :].astype(F32), jnp.zeros((5, 512), F32)], 0)
        xb[z, pl.ds(pl.multiple_of(c_off(x, y), 16), 16), :] = last.astype(BF)
        for n in range(5):
            cnt = 128 if n < 4 else 88
            m = t_ref[pl.ds(128 * n, cnt), :].astype(F32)
            if cnt < 128:
                m = jnp.concatenate([m, jnp.zeros((128 - cnt, 75), F32)], 0)
            m = jnp.concatenate([m.T, jnp.zeros((5, 128), F32)], 0)
            tt[2 * z + c, :, pl.ds(128 * n, 128)] = m.astype(BF)
        for n in range(4):
            zt_ref[:, pl.ds(128 * n, 128)] = k_ref[pl.ds(128 * n, 128), :].astype(F32).T.astype(BF)
        er[:, pl.ds(0, 1200)] = jnp.broadcast_to(e_ref[...], (8, 1200))
        er[:, pl.ds(1200, 80)] = jnp.zeros((8, 80), F32)
        others.wait()
        for n in range(10):
            w = 128 if n < 9 else 48
            res[n, :, pl.ds(0, w)] = stage[:, pl.ds(128 * n, w)]
    for o in own:
        o.wait()
    with jax.named_scope('barrier'):
        pl.semaphore_wait(bar, 38)

    def zblk(k):
        return (z + ((k + 1) // 2) * (2 * (k % 2) - 1) + 8) % 8

    def ring_pieces(s, d, blk):
        a = rows(blk, a_off(x, y), 32, 512 if d or s == 3 else 384)
        b = rows(blk, b_off(x, y), 32, 384 if d and s < 3 else 512)
        return ((a, 2 * s + d), (b, 8 + 2 * s + d)) if s < 3 else (((b, a)[d], 6 + d),)

    def t_piece(s, d, blk):
        r = 2 * blk + c
        return tt.at[r] if s < 3 else tt.at[r, pl.ds(48 * d, 48 - 16 * d)]

    def ring_step(s, zl, zr):
        for d, blk in enumerate((zl, zr)):
            for p, i in ring_pieces(s, d, blk):
                send(p, p, r_ss.at[i], r_rs.at[i], {"z": (zp, zm)[d]})

    def t_step(s, zl, zr):
        for d, blk in enumerate((zl, zr)):
            p = t_piece(s, d, blk)
            send(p, p, t_ss.at[2 * s + d], t_rs.at[2 * s + d], {"z": (zp, zm)[d]})

    def push_t(n, blk):
        r = 2 * blk + c
        send(tt.at[r], tt.at[r], u_ss.at[n], u_rs.at[n], sib)

    def ring_got(s):
        lo, hi = (z + 7 - s) % 8, (z + 1 + s) % 8
        for d, blk in enumerate((lo, hi)):
            for p, i in ring_pieces(s, d, blk):
                got(p, r_rs.at[i])
        return lo, hi

    def t_got(s):
        lo, hi = (z + 7 - s) % 8, (z + 1 + s) % 8
        for d, blk in enumerate((lo, hi)):
            got(t_piece(s, d, blk), t_rs.at[2 * s + d])
        return lo, hi

    ring_step(0, z, z)
    t_step(0, z, z)
    push_t(0, z)

    def c_piece(i, j, h):
        return xb.at[z, pl.ds(pl.multiple_of(c_off(i, j), 16), 16), pl.ds(256 * h, 256)]

    def c_step(s):
        if s == 0:
            p = rows(z, c_off(x, y), 16)
            send(p, p, c_ss.at[0], c_rs.at[0], {"y": yp})
            send(p, p, c_ss.at[1], c_rs.at[1], {"y": ym})
        elif s == 1:
            got(rows(z, c_off(x, ym), 16), c_rs.at[0])
            got(rows(z, c_off(x, yp), 16), c_rs.at[1])
            p, q = c_piece(x, ym, 0), c_piece(x, yp, 1)
            send(p, p, c_ss.at[2], c_rs.at[2], {"y": yp})
            send(q, q, c_ss.at[3], c_rs.at[3], {"y": ym})
        elif s == 2:
            got(c_piece(x, (y + 2) % 4, 0), c_rs.at[2])
            got(c_piece(x, (y + 2) % 4, 1), c_rs.at[3])
            p = rows(z, c_off(x, 0), 64)
            send(p, p, c_ss.at[4], c_rs.at[4], {"x": xp})
            send(p, p, c_ss.at[5], c_rs.at[5], {"x": xm})
        elif s == 3:
            got(rows(z, c_off(xm, 0), 64), c_rs.at[4])
            got(rows(z, c_off(xp, 0), 64), c_rs.at[5])
            p, q = rows(z, c_off(xm, 0), 32), rows(z, c_off(xp, 2), 32)
            send(p, p, c_ss.at[6], c_rs.at[6], {"x": xp})
            send(q, q, c_ss.at[7], c_rs.at[7], {"x": xm})
        else:
            got(rows(z, c_off((x + 2) % 4, 0), 32), c_rs.at[6])
            got(rows(z, c_off((x + 2) % 4, 2), 32), c_rs.at[7])

    def quarter(blk, q, d, half_only):
        xq, yq = (x + q) % 4, (y + q) % 4
        a, b = rows(blk, xq * 128, 128, 128, 384), rows(blk, 512 + yq * 128, 128, 128, 384)
        if half_only:
            return (rows(blk, 1024 + xq * 64 + 32 * d, 32),)
        return (a, b)[d], rows(blk, 1024 + xq * 64, 64)

    def quarter_send(g, q, blks, half_only=False):
        for d, blk in enumerate(blks):
            for p in quarter(blk, q, d, half_only):
                send(p, p, e_ss.at[g, q, d], e_rs.at[g, q, d], {"z": (zp, zm)[d]})

    def pump(e, _):
        g, i = e // 4, e % 4
        q = i + (i == 2).astype(jnp.int32) - (i == 3).astype(jnp.int32)
        blks = (z + 7 - g) % 8, (z + 1 + g) % 8

        def take(n):
            for d in range(2):
                got(rows(blks[d], 0, n), e_rs.at[g, q, d])

        @pl.when(g < 3)
        def _():
            take(96)

        @pl.when(g == 3)
        def _():
            take(32)

        @pl.when(g < 2)
        def _():
            quarter_send(g + 1, q, blks)

        @pl.when(g == 2)
        def _():
            quarter_send(g + 1, q, blks, True)

        return 0

    def s1(k, wa, wb):
        b = zblk(k)
        p, q = rows(b, a_off(x, y), 32, wa), rows(b, b_off(x, y), 32, wb)
        send(p, p, x_ss.at[k, 0], x_rs.at[k, 0], {"y": yp})
        send(p, p, x_ss.at[k, 1], x_rs.at[k, 1], {"y": ym})
        send(q, q, x_ss.at[k, 8], x_rs.at[k, 8], {"x": xp})
        send(q, q, x_ss.at[k, 9], x_rs.at[k, 9], {"x": xm})

    def s2(k, wa, wb):
        b = zblk(k)
        got(rows(b, a_off(x, ym), 32, wa), x_rs.at[k, 0])
        got(rows(b, a_off(x, yp), 32, wa), x_rs.at[k, 1])
        p, q = rows(b, a_off(x, ym), 16, wa), rows(b, a_off(x, yp) + 16, 16, wa)
        send(p, p, x_ss.at[k, 2], x_rs.at[k, 2], {"y": yp})
        send(q, q, x_ss.at[k, 3], x_rs.at[k, 3], {"y": ym})
        got(rows(b, b_off(xm, y), 32, wb), x_rs.at[k, 8])
        got(rows(b, b_off(xp, y), 32, wb), x_rs.at[k, 9])
        p, q = rows(b, b_off(xm, y), 16, wb), rows(b, b_off(xp, y) + 16, 16, wb)
        send(p, p, x_ss.at[k, 10], x_rs.at[k, 10], {"x": xp})
        send(q, q, x_ss.at[k, 11], x_rs.at[k, 11], {"x": xm})

    def s3(k, wa, wb):
        b = zblk(k)
        y2, x2 = (y + 2) % 4, (x + 2) % 4
        got(rows(b, a_off(x, y2), 16, wa), x_rs.at[k, 2])
        got(rows(b, a_off(x, y2) + 16, 16, wa), x_rs.at[k, 3])
        p = rows(b, a_off(x, 0), 128, wa)
        send(p, p, x_ss.at[k, 4], x_rs.at[k, 4], {"x": xp})
        send(p, p, x_ss.at[k, 5], x_rs.at[k, 5], {"x": xm})
        got(rows(b, b_off(x2, y), 16, wb), x_rs.at[k, 10])
        got(rows(b, b_off(x2, y) + 16, 16, wb), x_rs.at[k, 11])
        p = rows(b, b_off(0, y), 128, wb)
        send(p, p, x_ss.at[k, 12], x_rs.at[k, 12], {"y": yp})
        send(p, p, x_ss.at[k, 13], x_rs.at[k, 13], {"y": ym})

    def s4(k, wa, wb):
        b = zblk(k)
        got(rows(b, a_off(xm, 0), 128, wa), x_rs.at[k, 4])
        got(rows(b, a_off(xp, 0), 128, wa), x_rs.at[k, 5])
        p, q = rows(b, a_off(xm, 0), 64, wa), rows(b, a_off(xp, 2), 64, wa)
        send(p, p, x_ss.at[k, 6], x_rs.at[k, 6], {"x": xp})
        send(q, q, x_ss.at[k, 7], x_rs.at[k, 7], {"x": xm})
        got(rows(b, b_off(0, ym), 128, wb), x_rs.at[k, 12])
        got(rows(b, b_off(0, yp), 128, wb), x_rs.at[k, 13])
        p, q = rows(b, b_off(0, ym), 64, wb), rows(b, b_off(2, yp), 64, wb)
        send(p, p, x_ss.at[k, 14], x_rs.at[k, 14], {"y": yp})
        send(q, q, x_ss.at[k, 15], x_rs.at[k, 15], {"y": ym})

    def s5(k, wa, wb):
        b = zblk(k)
        y2, x2 = (y + 2) % 4, (x + 2) % 4
        got(rows(b, a_off(x2, 0), 64, wa), x_rs.at[k, 6])
        got(rows(b, a_off(x2, 2), 64, wa), x_rs.at[k, 7])
        got(rows(b, b_off(0, y2), 64, wb), x_rs.at[k, 14])
        got(rows(b, b_off(2, y2), 64, wb), x_rs.at[k, 15])

    def send_kernel():
        kc = y % 2

        def one(j, _):
            w = (v + j) % 16
            src = zt_ref.at[pl.ds(pl.multiple_of(32 * w, 32), 32)]
            send(src, zb_ref.at[v // 2, c], m_ss.at[0], m_rs.at[0], plane_dev(j, kc))
            return 0

        lax.fori_loop(1, 16, one, 0)
        src = zt_ref.at[pl.ds(pl.multiple_of(32 * v, 32), 32)]

        @pl.when(c == kc)
        def _():
            pltpu.make_async_copy(src, zb_ref.at[v // 2, c], m_rs.at[0]).start()

        @pl.when(c != kc)
        def _():
            send(src, zb_ref.at[v // 2, c], m_ss.at[0], m_rs.at[0], sib)

    def make_half():
        for n in range(1, 8):
            b = zblk(n)
            got(tt.at[2 * b + 1 - c], u_rs.at[n])
        got(tt.at[2 * z + 1 - c], u_rs.at[0])
        for i in range(4):
            for j in range(4):
                w = 4 * i + j
                ttp[pl.ds(a_off(i, j), 32), :] = tt[w, pl.ds(0, 32), :]
                ttp[pl.ds(b_off(i, j), 32), :] = tt[w, pl.ds(32, 32), :]
                ttp[pl.ds(c_off(i, j), 16), :] = tt[w, pl.ds(64, 16), :]
        lanes = lax.broadcasted_iota(jnp.int32, (80, 128), 1) // 32

        def chunk(a, _):
            q = pl.ds(pl.multiple_of(256 * a, 256), 256)
            m = lax.dot_general(ttp[...], xb[z, :, q], TN, preferred_element_type=F32)
            half[0] = m[:, :128]
            half[1] = m[:, 128:]
            for h in range(2):
                for g in range(2):
                    part = [half[h, pl.ds(4 * g + k, 80, stride=8), :] for k in range(4)]
                    for s in range(4):
                        m = roll(part[0], (0 - s) * 32)
                        for k in range(1, 4):
                            m = jnp.where(lanes == k, roll(part[k], (k - s) * 32), m)
                        hs[8 * a + 4 * h + s, :, pl.ds(128 * g, 128)] = m.astype(BF)
            return 0

        lax.fori_loop(0, 2, chunk, 0)

        def one(j, _):
            send(hs.at[(v + j) % 16], hb.at[c, v], m_ss.at[1], m_rs.at[1], plane_dev(j, c))
            return 0

        lax.fori_loop(1, 16, one, 0)
        pltpu.make_async_copy(hs.at[v], hb.at[c, v], m_rs.at[1]).start()

    def take_half():
        with jax.named_scope('w_hb'):
            got(hb.at[c], m_rs.at[1])
        send(hb.at[c], hb.at[c], m_ss.at[2], m_rs.at[2], sib)
        acc[...] = jnp.zeros_like(acc)
        with jax.named_scope('w_hbs'):
            got(hb.at[1 - c], m_rs.at[2])
        for s in range(2):
            to = pl.ds(256 * s, 256)
            for i in range(4):
                m = jnp.concatenate([hb[s, 4 * i + j, pl.ds(0, 32), :] for j in range(4)], 0)
                ht[to, pl.ds(128 * i, 128)] = m.astype(F32).T.astype(BF)
                m = jnp.concatenate([hb[s, 4 * j + i, pl.ds(32, 32), :] for j in range(4)], 0)
                ht[to, pl.ds(512 + 128 * i, 128)] = m.astype(F32).T.astype(BF)
            for i in range(2):
                m = jnp.concatenate([hb[s, 8 * i + j, pl.ds(64, 16), :] for j in range(8)], 0)
                ht[to, pl.ds(1024 + 128 * i, 128)] = m.astype(F32).T.astype(BF)
        with jax.named_scope('w_zb'):
            got(zb_ref, m_rs.at[0])

    def compute(k, _):
        b = zblk(k)
        for q in range(2):
            q = pl.ds(256 * q, 256)
            cp = jnp.dot(ht[...], xb[b, :, q], preferred_element_type=F32)
            zz = zb_ref[b, :, :, q].astype(F32)
            for s in range(2):
                for i in range(8):
                    o = 256 * s + 32 * i
                    wt[pl.ds(o, 32), q] = (cp[o : o + 32] * zz[s]).astype(BF)
        for a in range(5):
            a = pl.ds(256 * a, 256)
            acc[:, a] += lax.dot_general(wt[...], xb[b, a, :], NT, preferred_element_type=F32)
        return 0

    def on(cond, name, f, *args):
        @pl.when(cond)
        def _():
            with jax.named_scope(name):
                f(*args)

    def forward(s):
        lo, hi = ring_got(s - 1)
        if s < 4:
            ring_step(s, lo, hi)

    def forward_t(s):
        lo, hi = t_got(s - 1)
        if s < 4:
            t_step(s, lo, hi)
            push_t(2 * s - 1, hi)
            push_t(2 * s, lo)
        else:
            push_t(7, lo)

    def pumped(t):
        return jnp.clip(2 * (t - 4), 0, 16)

    def pair(f, n):
        @pl.when(n < 4)
        def _():
            f(2 * n - 1, 512, 384)
            f(2 * n, 384, 512)

        @pl.when(n == 4)
        def _():
            f(7, 512, 512)

    def single(f, k):
        @pl.when((k % 2 == 1) & (k < 7))
        def _():
            f(k, 512, 384)

        @pl.when(k % 2 == 0)
        def _():
            f(k, 384, 512)

        @pl.when(k == 7)
        def _():
            f(k, 512, 512)

    def tick(t, _):
        for s in range(1, 5):
            on(t == s, "forward", forward, s)
        on(t == 4, "s5", s5, 0, 512, 512)
        on(t >= 7, "s5", single, s5, t - 6)
        for s in range(5):
            on(t == s, "c_step", c_step, s)
        on(t == 3, "s4", s4, 0, 512, 512)
        on((t >= 5) & (t < 12), "s4", single, s4, t - 4)
        on(t == 2, "s3", s3, 0, 512, 512)
        on((t >= 3) & (t < 10), "s3", single, s3, t - 2)
        on(t == 0, "s1", s1, 0, 512, 512)
        on((t >= 1) & (t < 5), "s1", pair, s1, t)
        on(t == 0, "send_kernel", send_kernel)
        for s in range(1, 5):
            on(t == s, "forward_t", forward_t, s)
        on(t == 3, "quarter", quarter_send, 0, 0, (z, z))
        on(t == 4, "quarter", quarter_send, 0, 1, (z, z))
        on(t == 4, "quarter", quarter_send, 0, 3, (z, z))
        on(t == 4, "quarter", quarter_send, 0, 2, (z, z))
        on(t == 4, "make_half", make_half)
        on(t == 1, "s2", s2, 0, 512, 512)
        on((t >= 2) & (t < 4), "s2", pair, s2, t - 1)
        on(t == 5, "s2", pair, s2, t - 2)
        on(t == 5, "s2", pair, s2, t - 1)
        with jax.named_scope("pump"):
            lax.fori_loop(pumped(t - 1), pumped(t), pump, 0)
        on(t == READY, "take_half", take_half)
        with jax.named_scope("compute"):
            lax.fori_loop(jnp.maximum(t - READY, 0), jnp.maximum(t - READY + 1, 0), compute, 0)
        return 0

    lax.fori_loop(0, TICKS, tick, 0)

    mine = pl.ds(pl.multiple_of(256 * c, 256), 256)
    give = acc.at[pl.ds(pl.multiple_of(256 * (1 - c), 256), 256)]
    send(give, rb, m_ss.at[3], m_rs.at[3], sib)
    with jax.named_scope('w_rb'):
        got(rb, m_rs.at[3])
    for n in range(10):
        a = pl.ds(128 * n, 128)
        m = (acc[mine, a] + rb[:, a]).T.astype(BF)
        if n < 4:
            for j in range(4):
                bs[4 * n + j, pl.ds(0, 32), :] = m[32 * j : 32 * j + 32]
        elif n < 8:
            for j in range(4):
                bs[4 * j + n - 4, pl.ds(32, 32), :] = m[32 * j : 32 * j + 32]
        else:
            for j in range(8):
                bs[8 * (n - 8) + j, pl.ds(64, 16), :] = m[16 * j : 16 * j + 16]

    pieces = ((0, 32), (32, 48))
    for h, (lo, n) in enumerate(pieces):

        for i, j in FAR:
            i, j = (x + i) % 4, (y + j) % 4
            w = 4 * i + j
            send(bs.at[w, pl.ds(lo, n)], br.at[v, pl.ds(lo, n)], p_ss.at[h], p_rs.at[h], {"x": i, "y": j})
        pltpu.make_async_copy(bs.at[v, pl.ds(lo, n)], br.at[v, pl.ds(lo, n)], p_rs.at[h]).start()

    for h, (lo, n) in enumerate(pieces):
        with jax.named_scope("w_br"):
            got(br.at[:, pl.ds(lo, n)], p_rs.at[h])
        with jax.named_scope("unpack"):
            lanes = lax.broadcasted_iota(jnp.int32, (n, 128), 1) // 32
            for g in range(2):
                for a in range(4):
                    part = [br[4 * a + s, pl.ds(lo, n), pl.ds(128 * g, 128)].astype(F32) for s in range(4)]
                    for k in range(4):
                        m = roll(part[0], (0 - k) * 32)
                        for s in range(1, 4):
                            m = jnp.where(lanes == s, roll(part[s], (s - k) * 32), m)
                        ls[4 * g + k, pl.ds(lo, n), pl.ds(128 * a, 128)] = m.astype(BF)
        for d in (4, 3, 5, 2, 6, 1, 7):
            w = (z + d) % 8
            send(ls.at[w, pl.ds(lo, n)], lb.at[z, pl.ds(lo, n)], q_ss.at[h, d], q_rs.at[h, d], {"z": w})
        if h == 0:
            lt[...] = jnp.zeros_like(lt)

    def lad(b, src):
        for a in range(5):
            a = pl.ds(256 * a, 256)
            lt[a, pl.ds(0, 80)] += lax.dot_general(xb[b, a, :], src[b], NT, preferred_element_type=F32)

    lad(z, ls)

    def lad_step(j, _):
        d = 4 + ((j + 1) // 2) * (1 - 2 * (j % 2))
        b = (z + 8 - d) % 8
        with jax.named_scope("w_lb"):
            for h, (lo, n) in enumerate(pieces):
                got(lb.at[b, pl.ds(lo, n)], q_rs.at[h, d])
        with jax.named_scope("w_lad"):
            lad(b, lb)
        return 0

    lax.fori_loop(0, 7, lad_step, 0)
    send(lt, ltr, m_ss.at[6], m_rs.at[6], sib)
    ea = pltpu.roll(er[...], (1280 - 75 * v) % 1280, 1)[:, :128].T[:75, 0:1]
    with jax.named_scope("w_ltr"):
        got(ltr, m_rs.at[6])
    lc[pl.ds(1200, 80), :] = jnp.zeros((80, 128), F32)
    for i in range(4):
        for j in range(4):
            o = 75 * (4 * i + j)
            for n, off, cnt in ((0, a_off(i, j), 32), (32, b_off(i, j), 32), (64, c_off(i, j), 11)):
                lc[pl.ds(o + n, cnt), :] = lt[pl.ds(off, cnt), :] + ltr[pl.ds(off, cnt), :]
    for n in range(10):
        b = pl.ds(128 * n, 128)
        la[z, :, b] = lc[b, :].T[:80].astype(BF)

    chunks = ((0, 48), (48, 32))

    def la_part(i, h, ch):
        lo, n = chunks[ch]
        return la.at[i, pl.ds(lo, n), pl.ds(pl.multiple_of(640 * h, 128), 640)]

    def la_send(s, blk, d, ch):
        p = la_part(blk, c, ch)
        send(p, p, g_ss.at[2 * s + d, ch], g_rs.at[2 * s + d, ch], {"z": (zp, zm)[d]})

    def la_push(n, blk, ch):
        p = la_part(blk, c, ch)
        send(p, p, g_ss.at[8 + n, ch], g_rs.at[8 + n, ch], sib)

    for ch in range(2):
        for d in range(2):
            la_send(0, z, d, ch)

    total = jnp.zeros((75, 128), F32)
    ep = ep_ref[z]
    for n in range(10):
        w = 128 if n < 9 else 48
        b = pl.ds(128 * n, w)
        den = ea + er[0:1, b] - ep
        u = (res[n, pl.ds(z, 75, stride=8), :] + lc[pl.ds(128 * n, 128), :].T[:75])[:, :w] / den
        u = u * u
        if w < 128:
            u = jnp.concatenate([u, jnp.zeros((75, 128 - w), F32)], 1)
        total = total + u
    sc[...] = jnp.full((8, 128), jnp.sum(total), F32)

    def give_sum(j, _):
        send(sc, sp.at[v], m_ss.at[7], m_rs.at[7], plane_dev(j, c))
        return 0

    lax.fori_loop(1, 16, give_sum, 0)
    pltpu.make_async_copy(sc, sp.at[v], m_rs.at[7]).start()

    def finish(i):
        o = pl.ds(i, 75, stride=8)
        for n in range(10):
            b = pl.ds(128 * n, 128)
            res[n, o, :] = res[n, o, :] + la[i, :, b].astype(F32)[:75]

    for s in range(4):
        lo, hi = (z + 7 - s) % 8, (z + 1 + s) % 8
        with jax.named_scope(f"w_la{s}"):
            if s < 3:
                for ch in range(2):
                    got(la_part(lo, c, ch), g_rs.at[2 * s, ch])
                    if s < 2 or ch == 0:
                        la_send(s + 1, lo, 0, ch)
                    la_push(2 * s + 1, lo, ch)
                    got(la_part(hi, c, ch), g_rs.at[2 * s + 1, ch])
                    if s < 2 or ch == 1:
                        la_send(s + 1, hi, 1, ch)
                    la_push(2 * s, hi, ch)
            else:
                for ch in range(2):
                    got(la_part(lo, c, ch), g_rs.at[6 + ch, ch])
                    la_push(6, lo, ch)
        if s == 0:
            finish(z)
        if s == 1:
            with jax.named_scope("w_sp"):
                got(sp, m_rs.at[7])
            s_all = sp[0]
            for n in range(1, 16):
                s_all = s_all + sp[n]
            sz[z] = s_all

            def give_sz(j, _):
                send(sz.at[z], sz.at[z], m_ss.at[8], m_rs.at[8], {"z": (z + j) % 8})
                return 0

            lax.fori_loop(1, 8, give_sz, 0)
        if s >= 1:
            for n in (2 * s - 2, 2 * s - 1):
                with jax.named_scope("w_las"):
                    for ch in range(2):
                        got(la_part(zblk(n + 1), 1 - c, ch), g_rs.at[8 + n, ch])
                with jax.named_scope("finish"):
                    finish(zblk(n + 1))
    with jax.named_scope("w_las"):
        for ch in range(2):
            got(la_part(zblk(7), 1 - c, ch), g_rs.at[14, ch])
    with jax.named_scope("finish"):
        finish(zblk(7))
    outs = []
    for lo in range(0, 600, 200):
        for n in range(10):
            w = 128 if n < 9 else 48
            stage[pl.ds(lo, 200), pl.ds(128 * n, w)] = res[n, pl.ds(lo, 200), pl.ds(0, w)]
        p = pl.ds(lo, 200)
        outs.append(pltpu.make_async_copy(stage.at[p], out_ref.at[p], loc.at[3 + lo // 200]))
        outs[-1].start()
    with jax.named_scope("w_sz"):
        got(sz.at[pl.ds(0, 7)], m_rs.at[8])
    s_all = sz[0]
    for n in range(1, 8):
        s_all = s_all + sz[n]
    s_all = jnp.sqrt(s_all / (8 * 1200 * 1200) + EPS)
    rms_ref[0, 0] = s_all[0, 0]
    with jax.named_scope('w_out'):
        for o in outs:
            o.wait()

    for s in range(4):
        for d in range(2):
            i = 2 * s + d
            if s < 3:
                left(rows(0, 0, 32, 512 if d else 384), r_ss.at[i])
                left(rows(0, 0, 32, 384 if d else 512), r_ss.at[8 + i])
                left(tt.at[0], t_ss.at[i])
                for ch in range(2):
                    left(la_part(0, 0, ch), g_ss.at[i, ch])
            else:
                left(rows(0, 0, 32), r_ss.at[i])
                left(tt.at[0, pl.ds(0, 48 - 16 * d)], t_ss.at[i])
                left(la_part(0, 0, d), g_ss.at[i, d])
    for n in range(8):
        left(tt.at[0], u_ss.at[n])
    for n in range(7):
        for ch in range(2):
            left(la_part(0, 0, ch), g_ss.at[8 + n, ch])
    for n in (0, 1):
        left(rows(0, 0, 16), c_ss.at[n])
        left(xb.at[0, pl.ds(0, 16), pl.ds(0, 256)], c_ss.at[2 + n])
        left(rows(0, 0, 64), c_ss.at[4 + n])
        left(rows(0, 0, 32), c_ss.at[6 + n])
        for g in range(4):
            for q in range(4):
                left(rows(0, 0, 96 if g < 3 else 32), e_ss.at[g, q, n])

    def drain(k, wa, wb):
        for o, w in ((0, wa), (8, wb)):
            for n, cnt in ((0, 32), (2, 16), (4, 128), (6, 64)):
                left(rows(0, 0, cnt, w), x_ss.at[k, o + n])
                left(rows(0, 0, cnt, w), x_ss.at[k, o + n + 1])

    def drain_two(n, _):
        drain(2 * n + 1, 512, 384)
        drain(2 * n + 2, 384, 512)
        return 0

    drain(0, 512, 512)
    lax.fori_loop(0, 3, drain_two, 0)
    drain(7, 512, 512)

    @pl.when(c == y % 2)
    def _():
        left(zt_ref.at[pl.ds(0, 480)], m_ss.at[0])

    @pl.when(c != y % 2)
    def _():
        left(zt_ref, m_ss.at[0])

    left(hs.at[pl.ds(0, 15)], m_ss.at[1])
    left(hb.at[0], m_ss.at[2])
    left(rb, m_ss.at[3])
    for h, (lo, n) in enumerate(pieces):
        left(bs.at[pl.ds(0, 15), pl.ds(lo, n)], p_ss.at[h])
        for d in range(1, 8):
            left(ls.at[0, pl.ds(lo, n)], q_ss.at[h, d])
    left(lt, m_ss.at[6])
    left(sp.at[pl.ds(0, 15)], m_ss.at[7])
    left(sz.at[pl.ds(0, 7)], m_ss.at[8])


def shards(amplitudes, factors, kernel, other_terms, virt_energy, pair_energy):
    t = jnp.transpose(amplitudes, (1, 0, 2)).reshape(600, 75)
    other = jnp.transpose(other_terms, (1, 0, 2)).reshape(600, 1200)
    vm = pl.BlockSpec(memory_space=pltpu.VMEM)
    sm = pl.BlockSpec(memory_space=pltpu.SMEM)
    V = pltpu.VMEM
    dma = pltpu.SemaphoreType.DMA
    out, rms = pl.pallas_call(
        ladder_kernel,
        out_shape=(
            jax.ShapeDtypeStruct((600, 1200), F32),
            jax.ShapeDtypeStruct((1, 1), F32),
        ),
        in_specs=[vm, vm, vm, pl.BlockSpec(memory_space=pl.ANY), vm, sm],
        out_specs=(pl.BlockSpec(memory_space=pl.ANY), sm),
        scratch_shapes=[
            V((600, 1200), F32),
            V((10, 600, 128), F32),
            V((512, 512), BF),
            V((8, 1280), F32),
            V((8, 1280, 512), BF),
            V((16, 80, 640), BF),
            V((1280, 640), BF),
            V((2, 640, 128), F32),
            V((16, 80, 256), BF),
            V((2, 16, 80, 256), BF),
            V((512, 1280), BF),
            V((8, 2, 32, 512), BF),
            V((512, 512), BF),
            V((512, 1280), F32),
            V((256, 1280), F32),
            V((16, 80, 256), BF),
            V((16, 80, 256), BF),
            V((8, 80, 512), BF),
            V((8, 80, 512), BF),
            V((1280, 128), F32),
            V((1280, 128), F32),
            V((1280, 128), F32),
            V((8, 80, 1280), BF),
            V((8, 128), F32),
            V((16, 8, 128), F32),
            V((8, 8, 128), F32),
            dma((8, 16)), dma((8, 16)),
            dma((4, 4, 2)), dma((4, 4, 2)),
            dma((8,)), dma((8,)),
            dma((16,)), dma((16,)),
            dma((8,)), dma((8,)),
            dma((8,)), dma((8,)),
            dma((16, 2)), dma((16, 2)),
            dma((16,)), dma((16,)),
            dma((2,)), dma((2,)),
            dma((2, 8)), dma((2, 8)),
            dma((12,)),
        ],
        compiler_params=pltpu.CompilerParams(
            collective_id=0, has_side_effects=True, vmem_limit_bytes=60 * 1024 * 1024
        ),
        name="ladder",
    )(factors, t, kernel, other, virt_energy[None, :], pair_energy)
    return jnp.transpose(out.reshape(75, 8, 1200), (1, 0, 2)), rms.reshape(())


def solution(mesh):
    torus = Mesh(mesh.devices.reshape(4, 4, 8, 2), ("x", "y", "z", "core"))
    plane, rank = ("x", "y"), ("z", "core")
    return jax.shard_map(
        shards,
        mesh=torus,
        in_specs=(P(None, plane, rank), P(plane, rank), P(plane, rank), P(None, plane, None), P(), P()),
        out_specs=(P(None, plane, None), P()),
        check_vma=False,
    )
```

```python
import functools

import jax
import jax.numpy as jnp
from jax import lax
from jax.experimental import pallas as pl
from jax.experimental.pallas import tpu as pltpu
from jax.sharding import Mesh
from jax.sharding import PartitionSpec as P

MESH = pl.DeviceIdType.MESH
BF = jnp.bfloat16
F32 = jnp.float32
EPS = 1e-06
NT = (((1,), (1,)), ((), ()))
TN = (((0,), (0,)), ((), ()))
TICKS = 14
READY = 6
REGION = (pl.ds(1024, 256), pl.ds(0, 512), pl.ds(512, 512))
PIECES = ((64, 16), (0, 32), (32, 32))
FAR = sorted(((i, j) for i in range(4) for j in range(4) if i or j), key=lambda p: -min(p[0], 4 - p[0]) - min(p[1], 4 - p[1]))


def roll(a, shift):
    shift %= 128
    return a if shift == 0 else pltpu.roll(a, shift, 1)


def ladder_kernel(
    f_hbm, t_hbm, k_hbm, other_hbm, e_hbm, ep_hbm, out_ref, rms_ref,
    f_ref, t_ref, k_ref, e_ref, ep_ref,
    stage, res, packed, zt_ref, er,
    xb, tt, ttp, half, hs, hb, ht, zb_ref, wt, acc, rb, bs, br, ls, lb, lt, ltr, lc, la, sc, sp, sz,
    x_ss, x_rs, e_ss, e_rs, c_ss, c_rs, r_ss, r_rs, t_ss, t_rs, u_ss, u_rs, g_ss, g_rs, h_ss, h_rs, m_ss, m_rs, d_ss, d_rs, p_ss, p_rs, q_ss, q_rs, loc,
):
    x, y, z, c = (lax.axis_index(n) for n in ("x", "y", "z", "core"))
    v = 4 * x + y
    xp, xm = (x + 1) % 4, (x + 3) % 4
    yp, ym = (y + 1) % 4, (y + 3) % 4
    zp, zm = (z + 1) % 8, (z + 7) % 8
    sib = {"core": 1 - c}

    def rows(i, off, n, w=512, lo=0):
        return xb.at[i, pl.ds(pl.multiple_of(off, 16), n), pl.ds(lo, w)]

    def send(src, dst, ss, rs, dev):
        pltpu.make_async_remote_copy(
            src_ref=src, dst_ref=dst, send_sem=ss, recv_sem=rs, device_id=dev, device_id_type=MESH
        ).start()

    def got(dst, rs):
        pltpu.make_async_remote_copy(
            src_ref=dst, dst_ref=dst, send_sem=rs, recv_sem=rs, device_id=sib, device_id_type=MESH
        ).wait_recv()

    def left(src, ss):
        pltpu.make_async_remote_copy(
            src_ref=src, dst_ref=src, send_sem=ss, recv_sem=ss, device_id=sib, device_id_type=MESH
        ).wait_send()

    def a_off(i, j):
        return i * 128 + j * 32

    def b_off(i, j):
        return 512 + j * 128 + i * 32

    def c_off(i, j):
        return 1024 + i * 64 + j * 16

    loads = [
        pltpu.make_async_copy(a, b, loc.at[n])
        for n, (a, b) in enumerate(
            ((f_hbm, f_ref), (t_hbm, t_ref), (k_hbm, k_ref), (e_hbm, e_ref), (ep_hbm, ep_ref), (other_hbm, stage))
        )
    ]
    for o in loads:
        o.start()

    bar = pltpu.get_barrier_semaphore()

    def plane_dev(j, core):
        w = (v + j) % 16
        return {"x": w // 4, "y": w % 4, "core": core}

    def greet(j, _):
        pl.semaphore_signal(bar, inc=1, device_id=plane_dev(j, c), device_id_type=MESH)
        pl.semaphore_signal(bar, inc=1, device_id=plane_dev(j, 1 - c), device_id_type=MESH)
        return 0

    lax.fori_loop(1, 16, greet, 0)
    pl.semaphore_signal(bar, inc=1, device_id=sib, device_id_type=MESH)

    def greet_z(j, _):
        pl.semaphore_signal(bar, inc=1, device_id={"z": (z + j) % 8}, device_id_type=MESH)
        return 0

    lax.fori_loop(1, 8, greet_z, 0)
    with jax.named_scope("local"):
        loads[0].wait()
        xb[z, pl.ds(pl.multiple_of(a_off(x, y), 16), 32), :] = f_ref[pl.ds(0, 32), :]
        xb[z, pl.ds(pl.multiple_of(b_off(x, y), 16), 32), :] = f_ref[pl.ds(32, 32), :]
        last = jnp.concatenate([f_ref[pl.ds(64, 11), :].astype(F32), jnp.zeros((5, 512), F32)], 0)
        xb[z, pl.ds(pl.multiple_of(c_off(x, y), 16), 16), :] = last.astype(BF)
        loads[1].wait()
        for n in range(5):
            cnt = 128 if n < 4 else 88
            m = t_ref[pl.ds(128 * n, cnt), :].astype(F32)
            if cnt < 128:
                m = jnp.concatenate([m, jnp.zeros((128 - cnt, 75), F32)], 0)
            m = jnp.concatenate([m.T, jnp.zeros((5, 128), F32)], 0)
            tt[2 * z + c, :, pl.ds(128 * n, 128)] = m.astype(BF)
        loads[2].wait()
        for n in range(4):
            zt_ref[:, pl.ds(128 * n, 128)] = k_ref[pl.ds(128 * n, 128), :].astype(F32).T.astype(BF)
        for o in loads[3:]:
            o.wait()
        er[:, pl.ds(0, 1200)] = jnp.broadcast_to(e_ref[...].reshape(1, 1200), (8, 1200))
        er[:, pl.ds(1200, 80)] = jnp.zeros((8, 80), F32)
        for n in range(10):
            w = 128 if n < 9 else 48
            res[n, :, pl.ds(0, w)] = stage[:, pl.ds(128 * n, w)]
    with jax.named_scope('barrier'):
        pl.semaphore_wait(bar, 38)

    def zblk(k):
        return (z + ((k + 1) // 2) * (2 * (k % 2) - 1) + 8) % 8

    def ring_pieces(s, d, blk):
        a = rows(blk, a_off(x, y), 32, 512 if d or s == 3 else 384)
        b = rows(blk, b_off(x, y), 32, 384 if d and s < 3 else 512)
        return ((a, 2 * s + d), (b, 8 + 2 * s + d)) if s < 3 else (((b, a)[d], 6 + d),)

    def t_piece(s, d, blk):
        r = 2 * blk + c
        return tt.at[r] if s < 3 else tt.at[r, pl.ds(48 * d, 48 - 16 * d)]

    def ring_step(s, zl, zr):
        for d, blk in enumerate((zl, zr)):
            for p, i in ring_pieces(s, d, blk):
                send(p, p, r_ss.at[i], r_rs.at[i], {"z": (zp, zm)[d]})

    def t_step(s, zl, zr):
        for d, blk in enumerate((zl, zr)):
            p = t_piece(s, d, blk)
            send(p, p, t_ss.at[2 * s + d], t_rs.at[2 * s + d], {"z": (zp, zm)[d]})

    def push_t(n, blk):
        r = 2 * blk + c
        send(tt.at[r], tt.at[r], u_ss.at[n], u_rs.at[n], sib)

    def ring_got(s):
        lo, hi = (z + 7 - s) % 8, (z + 1 + s) % 8
        for d, blk in enumerate((lo, hi)):
            for p, i in ring_pieces(s, d, blk):
                got(p, r_rs.at[i])
        return lo, hi

    def t_got(s):
        lo, hi = (z + 7 - s) % 8, (z + 1 + s) % 8
        for d, blk in enumerate((lo, hi)):
            got(t_piece(s, d, blk), t_rs.at[2 * s + d])
        return lo, hi

    ring_step(0, z, z)
    t_step(0, z, z)
    push_t(0, z)

    def c_piece(i, j, h):
        return xb.at[z, pl.ds(pl.multiple_of(c_off(i, j), 16), 16), pl.ds(256 * h, 256)]

    def c_step(s):
        if s == 0:
            p = rows(z, c_off(x, y), 16)
            send(p, p, c_ss.at[0], c_rs.at[0], {"y": yp})
            send(p, p, c_ss.at[1], c_rs.at[1], {"y": ym})
        elif s == 1:
            got(rows(z, c_off(x, ym), 16), c_rs.at[0])
            got(rows(z, c_off(x, yp), 16), c_rs.at[1])
            p, q = c_piece(x, ym, 0), c_piece(x, yp, 1)
            send(p, p, c_ss.at[2], c_rs.at[2], {"y": yp})
            send(q, q, c_ss.at[3], c_rs.at[3], {"y": ym})
        elif s == 2:
            got(c_piece(x, (y + 2) % 4, 0), c_rs.at[2])
            got(c_piece(x, (y + 2) % 4, 1), c_rs.at[3])
            p = rows(z, c_off(x, 0), 64)
            send(p, p, c_ss.at[4], c_rs.at[4], {"x": xp})
            send(p, p, c_ss.at[5], c_rs.at[5], {"x": xm})
        elif s == 3:
            got(rows(z, c_off(xm, 0), 64), c_rs.at[4])
            got(rows(z, c_off(xp, 0), 64), c_rs.at[5])
            p, q = rows(z, c_off(xm, 0), 32), rows(z, c_off(xp, 2), 32)
            send(p, p, c_ss.at[6], c_rs.at[6], {"x": xp})
            send(q, q, c_ss.at[7], c_rs.at[7], {"x": xm})
        else:
            got(rows(z, c_off((x + 2) % 4, 0), 32), c_rs.at[6])
            got(rows(z, c_off((x + 2) % 4, 2), 32), c_rs.at[7])

    def quarter(blk, q, d, half_only):
        xq, yq = (x + q) % 4, (y + q) % 4
        a, b = rows(blk, xq * 128, 128, 128, 384), rows(blk, 512 + yq * 128, 128, 128, 384)
        if half_only:
            return (rows(blk, 1024 + xq * 64 + 32 * d, 32),)
        return (a, b)[d], rows(blk, 1024 + xq * 64, 64)

    def quarter_send(g, q, blks, half_only=False):
        for d, blk in enumerate(blks):
            for p in quarter(blk, q, d, half_only):
                send(p, p, e_ss.at[g, q, d], e_rs.at[g, q, d], {"z": (zp, zm)[d]})

    def pump(e, _):
        g, i = e // 4, e % 4
        q = i + (i == 2).astype(jnp.int32) - (i == 3).astype(jnp.int32)
        blks = (z + 7 - g) % 8, (z + 1 + g) % 8

        def take(n):
            for d in range(2):
                got(rows(blks[d], 0, n), e_rs.at[g, q, d])

        @pl.when(g < 3)
        def _():
            take(96)

        @pl.when(g == 3)
        def _():
            take(32)

        @pl.when(g < 2)
        def _():
            quarter_send(g + 1, q, blks)

        @pl.when(g == 2)
        def _():
            quarter_send(g + 1, q, blks, True)

        return 0

    def s1(k, wa, wb):
        b = zblk(k)
        p, q = rows(b, a_off(x, y), 32, wa), rows(b, b_off(x, y), 32, wb)
        send(p, p, x_ss.at[k, 0], x_rs.at[k, 0], {"y": yp})
        send(p, p, x_ss.at[k, 1], x_rs.at[k, 1], {"y": ym})
        send(q, q, x_ss.at[k, 8], x_rs.at[k, 8], {"x": xp})
        send(q, q, x_ss.at[k, 9], x_rs.at[k, 9], {"x": xm})

    def s2(k, wa, wb):
        b = zblk(k)
        got(rows(b, a_off(x, ym), 32, wa), x_rs.at[k, 0])
        got(rows(b, a_off(x, yp), 32, wa), x_rs.at[k, 1])
        p, q = rows(b, a_off(x, ym), 16, wa), rows(b, a_off(x, yp) + 16, 16, wa)
        send(p, p, x_ss.at[k, 2], x_rs.at[k, 2], {"y": yp})
        send(q, q, x_ss.at[k, 3], x_rs.at[k, 3], {"y": ym})
        got(rows(b, b_off(xm, y), 32, wb), x_rs.at[k, 8])
        got(rows(b, b_off(xp, y), 32, wb), x_rs.at[k, 9])
        p, q = rows(b, b_off(xm, y), 16, wb), rows(b, b_off(xp, y) + 16, 16, wb)
        send(p, p, x_ss.at[k, 10], x_rs.at[k, 10], {"x": xp})
        send(q, q, x_ss.at[k, 11], x_rs.at[k, 11], {"x": xm})

    def s3(k, wa, wb):
        b = zblk(k)
        y2, x2 = (y + 2) % 4, (x + 2) % 4
        got(rows(b, a_off(x, y2), 16, wa), x_rs.at[k, 2])
        got(rows(b, a_off(x, y2) + 16, 16, wa), x_rs.at[k, 3])
        p = rows(b, a_off(x, 0), 128, wa)
        send(p, p, x_ss.at[k, 4], x_rs.at[k, 4], {"x": xp})
        send(p, p, x_ss.at[k, 5], x_rs.at[k, 5], {"x": xm})
        got(rows(b, b_off(x2, y), 16, wb), x_rs.at[k, 10])
        got(rows(b, b_off(x2, y) + 16, 16, wb), x_rs.at[k, 11])
        p = rows(b, b_off(0, y), 128, wb)
        send(p, p, x_ss.at[k, 12], x_rs.at[k, 12], {"y": yp})
        send(p, p, x_ss.at[k, 13], x_rs.at[k, 13], {"y": ym})

    def s4(k, wa, wb):
        b = zblk(k)
        got(rows(b, a_off(xm, 0), 128, wa), x_rs.at[k, 4])
        got(rows(b, a_off(xp, 0), 128, wa), x_rs.at[k, 5])
        p, q = rows(b, a_off(xm, 0), 64, wa), rows(b, a_off(xp, 2), 64, wa)
        send(p, p, x_ss.at[k, 6], x_rs.at[k, 6], {"x": xp})
        send(q, q, x_ss.at[k, 7], x_rs.at[k, 7], {"x": xm})
        got(rows(b, b_off(0, ym), 128, wb), x_rs.at[k, 12])
        got(rows(b, b_off(0, yp), 128, wb), x_rs.at[k, 13])
        p, q = rows(b, b_off(0, ym), 64, wb), rows(b, b_off(2, yp), 64, wb)
        send(p, p, x_ss.at[k, 14], x_rs.at[k, 14], {"y": yp})
        send(q, q, x_ss.at[k, 15], x_rs.at[k, 15], {"y": ym})

    def s5(k, wa, wb):
        b = zblk(k)
        y2, x2 = (y + 2) % 4, (x + 2) % 4
        got(rows(b, a_off(x2, 0), 64, wa), x_rs.at[k, 6])
        got(rows(b, a_off(x2, 2), 64, wa), x_rs.at[k, 7])
        got(rows(b, b_off(0, y2), 64, wb), x_rs.at[k, 14])
        got(rows(b, b_off(2, y2), 64, wb), x_rs.at[k, 15])

    def send_kernel():
        kc = y % 2

        def one(j, _):
            w = (v + j) % 16
            src = zt_ref.at[pl.ds(pl.multiple_of(32 * w, 32), 32)]
            send(src, zb_ref.at[v // 2, c], m_ss.at[0], m_rs.at[0], plane_dev(j, kc))
            return 0

        lax.fori_loop(1, 16, one, 0)
        src = zt_ref.at[pl.ds(pl.multiple_of(32 * v, 32), 32)]

        @pl.when(c == kc)
        def _():
            pltpu.make_async_copy(src, zb_ref.at[v // 2, c], m_rs.at[0]).start()

        @pl.when(c != kc)
        def _():
            send(src, zb_ref.at[v // 2, c], m_ss.at[0], m_rs.at[0], sib)

    def make_half():
        for n in range(1, 8):
            b = zblk(n)
            got(tt.at[2 * b + 1 - c], u_rs.at[n])
        got(tt.at[2 * z + 1 - c], u_rs.at[0])
        for i in range(4):
            for j in range(4):
                w = 4 * i + j
                ttp[pl.ds(a_off(i, j), 32), :] = tt[w, pl.ds(0, 32), :]
                ttp[pl.ds(b_off(i, j), 32), :] = tt[w, pl.ds(32, 32), :]
                ttp[pl.ds(c_off(i, j), 16), :] = tt[w, pl.ds(64, 16), :]
        lanes = lax.broadcasted_iota(jnp.int32, (80, 128), 1) // 32

        def chunk(a, _):
            q = pl.ds(pl.multiple_of(256 * a, 256), 256)
            m = lax.dot_general(ttp[...], xb[z, :, q], TN, preferred_element_type=F32)
            half[0] = m[:, :128]
            half[1] = m[:, 128:]
            for h in range(2):
                for g in range(2):
                    part = [half[h, pl.ds(4 * g + k, 80, stride=8), :] for k in range(4)]
                    for s in range(4):
                        m = roll(part[0], (0 - s) * 32)
                        for k in range(1, 4):
                            m = jnp.where(lanes == k, roll(part[k], (k - s) * 32), m)
                        hs[8 * a + 4 * h + s, :, pl.ds(128 * g, 128)] = m.astype(BF)
            for s in range(8):
                w = 8 * a + s

                @pl.when(w != v)
                def _(w=w):
                    dev = {"x": w // 4, "y": w % 4}
                    send(hs.at[w], hb.at[c, v], m_ss.at[1], m_rs.at[1], dev)

            return 0

        lax.fori_loop(0, 2, chunk, 0)
        pltpu.make_async_copy(hs.at[v], hb.at[c, v], m_rs.at[1]).start()

    def take_half():
        with jax.named_scope('w_hb'):
            got(hb.at[c], m_rs.at[1])
        send(hb.at[c], hb.at[c], m_ss.at[2], m_rs.at[2], sib)
        acc[...] = jnp.zeros_like(acc)
        with jax.named_scope('w_hbs'):
            got(hb.at[1 - c], m_rs.at[2])
        for s in range(2):
            to = pl.ds(256 * s, 256)
            for i in range(4):
                m = jnp.concatenate([hb[s, 4 * i + j, pl.ds(0, 32), :] for j in range(4)], 0)
                ht[to, pl.ds(128 * i, 128)] = m.astype(F32).T.astype(BF)
                m = jnp.concatenate([hb[s, 4 * j + i, pl.ds(32, 32), :] for j in range(4)], 0)
                ht[to, pl.ds(512 + 128 * i, 128)] = m.astype(F32).T.astype(BF)
            for i in range(2):
                m = jnp.concatenate([hb[s, 8 * i + j, pl.ds(64, 16), :] for j in range(8)], 0)
                ht[to, pl.ds(1024 + 128 * i, 128)] = m.astype(F32).T.astype(BF)
        with jax.named_scope('w_zb'):
            got(zb_ref, m_rs.at[0])

    mine = pl.ds(pl.multiple_of(256 * c, 256), 256)
    yours = pl.ds(pl.multiple_of(256 * (1 - c), 256), 256)

    def compute(k, last):
        b = zblk(k)
        for q in range(2):
            q = pl.ds(256 * q, 256)
            cp = jnp.dot(ht[...], xb[b, :, q], preferred_element_type=F32)
            zz = zb_ref[b, :, :, q].astype(F32)
            for s in range(2):
                for i in range(8):
                    o = 256 * s + 32 * i
                    wt[pl.ds(o, 32), q] = (cp[o : o + 32] * zz[s]).astype(BF)
        for n in (4, 0, 1, 2, 3):
            a = pl.ds(256 * n, 256)
            acc[:, a] += lax.dot_general(wt[...], xb[b, a, :], NT, preferred_element_type=F32)
            if last is True and (n % 2 or n == 4):
                h = (n // 2 + 1) % 3
                send(acc.at[yours, REGION[h]], rb.at[:, REGION[h]], d_ss.at[h], d_rs.at[h], sib)
        return 0

    def on(cond, name, f, *args):
        @pl.when(cond)
        def _():
            with jax.named_scope(name):
                f(*args)

    def forward(s):
        lo, hi = ring_got(s - 1)
        if s < 4:
            ring_step(s, lo, hi)

    def forward_t(s):
        lo, hi = t_got(s - 1)
        if s < 4:
            t_step(s, lo, hi)
            push_t(2 * s - 1, hi)
            push_t(2 * s, lo)
        else:
            push_t(7, lo)

    def pumped(t):
        return jnp.clip(2 * (t - 4), 0, 16)

    def pair(f, n):
        @pl.when(n < 4)
        def _():
            f(2 * n - 1, 512, 384)
            f(2 * n, 384, 512)

        @pl.when(n == 4)
        def _():
            f(7, 512, 512)

    def single(f, k):
        @pl.when((k % 2 == 1) & (k < 7))
        def _():
            f(k, 512, 384)

        @pl.when(k % 2 == 0)
        def _():
            f(k, 384, 512)

        @pl.when(k == 7)
        def _():
            f(k, 512, 512)

    def tick(t, _):
        for s in range(1, 5):
            on(t == s, "forward", forward, s)
        on(t == 4, "s5", s5, 0, 512, 512)
        on(t >= 7, "s5", single, s5, t - 6)
        for s in range(5):
            on(t == s, "c_step", c_step, s)
        on(t == READY, "take_half", take_half)
        on(t == 3, "s4", s4, 0, 512, 512)
        on((t >= 5) & (t < 12), "s4", single, s4, t - 4)
        on(t == 2, "s3", s3, 0, 512, 512)
        on((t >= 3) & (t < 10) & (t != 4), "s3", single, s3, t - 2)
        on(t == 0, "s1", s1, 0, 512, 512)
        on((t >= 1) & (t < 5), "s1", pair, s1, t)
        on(t == 0, "send_kernel", send_kernel)
        for s in range(1, 5):
            on(t == s, "forward_t", forward_t, s)
        on(t == 3, "quarter", quarter_send, 0, 0, (z, z))
        on(t == 4, "quarter", quarter_send, 0, 1, (z, z))
        on(t == 4, "quarter", quarter_send, 0, 3, (z, z))
        on(t == 4, "quarter", quarter_send, 0, 2, (z, z))
        on(t == 4, "make_half", make_half)
        on(t == 4, "s3", s3, 2, 384, 512)
        on(t == 1, "s2", s2, 0, 512, 512)
        on((t >= 2) & (t < 4), "s2", pair, s2, t - 1)
        on(t == 5, "s2", pair, s2, t - 2)
        on(t == 7, "s2", s2, 7, 512, 512)
        with jax.named_scope("pump"):
            lax.fori_loop(pumped(t - 1), pumped(t), pump, 0)
        with jax.named_scope("compute"):
            lax.fori_loop(jnp.maximum(t - READY, 0), jnp.where(t < TICKS - 1, jnp.maximum(t - READY + 1, 0), 7), compute, 0)
        return 0

    lax.fori_loop(0, TICKS, tick, 0)
    with jax.named_scope('compute'):
        compute(7, True)

    for h, (lo, cnt) in enumerate(PIECES):
        with jax.named_scope("w_rb"):
            got(rb.at[:, REGION[h]], d_rs.at[h])
        for n in (range(8, 10), range(4), range(4, 8))[h]:
            a = pl.ds(128 * n, 128)
            m = (acc[mine, a] + rb[:, a]).T.astype(BF)
            for j in range(128 // cnt):
                w = (8 * (n - 8) + j, 4 * n + j, 4 * j + n - 4)[h]
                bs[w, pl.ds(lo, cnt), :] = m[cnt * j : cnt * j + cnt]
        for i, j in FAR:
            i, j = (x + i) % 4, (y + j) % 4
            w = 4 * i + j
            send(bs.at[w, pl.ds(lo, cnt)], br.at[v, pl.ds(lo, cnt)], p_ss.at[h], p_rs.at[h], {"x": i, "y": j})
        pltpu.make_async_copy(bs.at[v, pl.ds(lo, cnt)], br.at[v, pl.ds(lo, cnt)], p_rs.at[h]).start()

    for h, (lo, n) in enumerate(PIECES):
        with jax.named_scope("w_br"):
            got(br.at[:, pl.ds(lo, n)], p_rs.at[h])
        with jax.named_scope("unpack"):
            lanes = lax.broadcasted_iota(jnp.int32, (n, 128), 1) // 32
            for g in range(2):
                for a in range(4):
                    part = [br[4 * a + s, pl.ds(lo, n), pl.ds(128 * g, 128)].astype(F32) for s in range(4)]
                    for k in range(4):
                        m = roll(part[0], (0 - k) * 32)
                        for s in range(1, 4):
                            m = jnp.where(lanes == s, roll(part[s], (s - k) * 32), m)
                        ls[4 * g + k, pl.ds(lo, n), pl.ds(128 * a, 128)] = m.astype(BF)
        for d in (7, 1, 6, 2, 5, 3, 4):
            w = (z + d) % 8
            send(ls.at[w, pl.ds(lo, n)], lb.at[z, pl.ds(lo, n)], q_ss.at[h, d], q_rs.at[h, d], {"z": w})
        if h == 0:
            lt[...] = jnp.zeros_like(lt)

    def lad(b, src):
        for a in range(5):
            a = pl.ds(256 * a, 256)
            lt[a, pl.ds(0, 80)] += lax.dot_general(xb[b, a, :], src[b], NT, preferred_element_type=F32)

    lad(z, ls)

    def lad_step(j, _):
        d = 4 + ((7 - j) // 2) * (1 - 2 * (j % 2))
        b = (z + 8 - d) % 8
        with jax.named_scope("w_lb"):
            for h, (lo, n) in enumerate(PIECES):
                got(lb.at[b, pl.ds(lo, n)], q_rs.at[h, d])
        with jax.named_scope("w_lad"):
            lad(b, lb)
        return 0

    lax.fori_loop(0, 7, lad_step, 0)
    send(lt, ltr, m_ss.at[6], m_rs.at[6], sib)
    ea = pltpu.roll(er[...], (1280 - 75 * v) % 1280, 1)[:, :128].T[:75, 0:1]
    with jax.named_scope("w_ltr"):
        got(ltr, m_rs.at[6])
    lc[pl.ds(1200, 80), :] = jnp.zeros((80, 128), F32)
    for i in range(4):
        for j in range(4):
            o = 75 * (4 * i + j)
            for n, off, cnt in ((0, a_off(i, j), 32), (32, b_off(i, j), 32), (64, c_off(i, j), 11)):
                lc[pl.ds(o + n, cnt), :] = lt[pl.ds(off, cnt), :] + ltr[pl.ds(off, cnt), :]
    for n in range(10):
        b = pl.ds(128 * n, 128)
        la[z, :, b] = lc[b, :].T[:80].astype(BF)


    def la_part(i, h, lo, n=16):
        return la.at[i, pl.ds(lo, n), pl.ds(pl.multiple_of(640 * h, 128), 640)]

    def la_send(s, blk, d, ch):
        p = la_part(blk, c, 16 * ch)
        dev = {"z": ((zp, zm)[d] if s < 3 else (z + (2, 6)[d]) % 8)}
        send(p, p, g_ss.at[2 * s + d, ch], g_rs.at[2 * s + d, ch], dev)

    HALF = ((0, 48), (48, 32))

    def la_push(n, blk, h):
        p = la_part(blk, c, *HALF[h])
        send(p, p, h_ss.at[n, h], h_rs.at[n, h], sib)

    for ch in range(5):
        for d in range(2):
            la_send(0, z, d, ch)

    total = jnp.zeros((75, 128), F32)
    ep = ep_ref[z]
    for n in range(10):
        w = 128 if n < 9 else 48
        b = pl.ds(128 * n, w)
        den = ea + er[0:1, b] - ep
        u = (res[n, pl.ds(z, 75, stride=8), :] + lc[pl.ds(128 * n, 128), :].T[:75])[:, :w] / den
        u = u * u
        if w < 128:
            u = jnp.concatenate([u, jnp.zeros((75, 128 - w), F32)], 1)
        total = total + u
    sc[...] = jnp.full((8, 128), jnp.sum(total), F32)

    def give_sum(j, _):
        send(sc, sp.at[v], m_ss.at[7], m_rs.at[7], plane_dev(j, c))
        return 0

    lax.fori_loop(1, 16, give_sum, 0)
    pltpu.make_async_copy(sc, sp.at[v], m_rs.at[7]).start()

    def finish(i):
        o = pl.ds(i, 75, stride=8)
        for n in range(10):
            b = pl.ds(128 * n, 128)
            res[n, o, :] = la[i, :, b].astype(F32)[:75]

    for s in range(4):
        lo, hi = (z + 7 - s) % 8, (z + 1 + s) % 8
        with jax.named_scope(f"w_la{s}"):
            for ch in range(5):
                if s < 3:
                    got(la_part(lo, c, 16 * ch), g_rs.at[2 * s, ch])
                    if s < 2:
                        la_send(s + 1, lo, 0, ch)
                    if s == 1 and ch < 3:
                        la_send(3, lo, 0, ch)
                    got(la_part(hi, c, 16 * ch), g_rs.at[2 * s + 1, ch])
                    if s < 2:
                        la_send(s + 1, hi, 1, ch)
                    if s == 1 and ch >= 3:
                        la_send(3, hi, 1, ch)
                else:
                    got(la_part(lo, c, 16 * ch), g_rs.at[6 + (ch >= 3), ch])
                if ch in (2, 4):
                    h = ch // 2 - 1
                    la_push(2 * s + (s < 3), lo, h)
                    if s < 3:
                        la_push(2 * s, hi, h)
        if s == 0:
            finish(z)
            with jax.named_scope("w_sp"):
                got(sp, m_rs.at[7])
            s_all = sp[0]
            for n in range(1, 16):
                s_all = s_all + sp[n]
            sz[z] = s_all

            def give_sz(j, _):
                send(sz.at[z], sz.at[z], m_ss.at[8], m_rs.at[8], {"z": (z + j) % 8})
                return 0

            lax.fori_loop(1, 8, give_sz, 0)
        if s >= 1:
            for n in (2 * s - 2, 2 * s - 1):
                with jax.named_scope("w_las"):
                    for ch in range(2):
                        got(la_part(zblk(n + 1), 1 - c, *HALF[ch]), h_rs.at[n, ch])
                with jax.named_scope("finish"):
                    finish(zblk(n + 1))
    with jax.named_scope("w_las"):
        for ch in range(2):
            got(la_part(zblk(7), 1 - c, *HALF[ch]), h_rs.at[6, ch])
    with jax.named_scope("finish"):
        finish(zblk(7))
    outs = []
    for h, (lo, cnt) in enumerate(((0, 208), (208, 208), (416, 184))):
        p = pl.ds(lo, cnt)
        for n in range(10):
            w = 128 if n < 9 else 48
            packed[p, pl.ds(128 * n, w)] = res[n, p, pl.ds(0, w)].astype(BF)
        outs.append(pltpu.make_async_copy(packed.at[p], out_ref.at[p], loc.at[3 + h]))
        outs[-1].start()
    with jax.named_scope("w_sz"):
        got(sz.at[pl.ds(0, 7)], m_rs.at[8])
    s_all = sz[0]
    for n in range(1, 8):
        s_all = s_all + sz[n]
    s_all = jnp.sqrt(s_all / (8 * 1200 * 1200) + EPS)
    rms_ref[0, 0] = s_all[0, 0]
    with jax.named_scope('w_out'):
        for o in outs:
            o.wait()

    for s in range(4):
        for d in range(2):
            i = 2 * s + d
            if s < 3:
                left(rows(0, 0, 32, 512 if d else 384), r_ss.at[i])
                left(rows(0, 0, 32, 384 if d else 512), r_ss.at[8 + i])
                left(tt.at[0], t_ss.at[i])
                for ch in range(5):
                    left(la_part(0, 0, 0), g_ss.at[i, ch])
            else:
                left(rows(0, 0, 32), r_ss.at[i])
                left(tt.at[0, pl.ds(0, 48 - 16 * d)], t_ss.at[i])
                for ch in ((0, 1, 2), (3, 4))[d]:
                    left(la_part(0, 0, 0), g_ss.at[i, ch])
    for n in range(8):
        left(tt.at[0], u_ss.at[n])
    for n in range(7):
        for ch in range(2):
            left(la_part(0, 0, *HALF[ch]), h_ss.at[n, ch])
    for n in (0, 1):
        left(rows(0, 0, 16), c_ss.at[n])
        left(xb.at[0, pl.ds(0, 16), pl.ds(0, 256)], c_ss.at[2 + n])
        left(rows(0, 0, 64), c_ss.at[4 + n])
        left(rows(0, 0, 32), c_ss.at[6 + n])
        for g in range(4):
            for q in range(4):
                left(rows(0, 0, 96 if g < 3 else 32), e_ss.at[g, q, n])

    def drain(k, wa, wb):
        for o, w in ((0, wa), (8, wb)):
            for n, cnt in ((0, 32), (2, 16), (4, 128), (6, 64)):
                left(rows(0, 0, cnt, w), x_ss.at[k, o + n])
                left(rows(0, 0, cnt, w), x_ss.at[k, o + n + 1])

    def drain_two(n, _):
        drain(2 * n + 1, 512, 384)
        drain(2 * n + 2, 384, 512)
        return 0

    drain(0, 512, 512)
    lax.fori_loop(0, 3, drain_two, 0)
    drain(7, 512, 512)

    @pl.when(c == y % 2)
    def _():
        left(zt_ref.at[pl.ds(0, 480)], m_ss.at[0])

    @pl.when(c != y % 2)
    def _():
        left(zt_ref, m_ss.at[0])

    left(hs.at[pl.ds(0, 15)], m_ss.at[1])
    left(hb.at[0], m_ss.at[2])
    for h in range(3):
        left(rb.at[:, REGION[h]], d_ss.at[h])
    for h, (lo, n) in enumerate(PIECES):
        left(bs.at[pl.ds(0, 15), pl.ds(lo, n)], p_ss.at[h])
        for d in range(1, 8):
            left(ls.at[0, pl.ds(lo, n)], q_ss.at[h, d])
    left(lt, m_ss.at[6])
    left(sp.at[pl.ds(0, 15)], m_ss.at[7])
    left(sz.at[pl.ds(0, 7)], m_ss.at[8])


def shards(amplitudes, factors, kernel, other_terms, virt_energy, pair_energy):
    t = jnp.transpose(amplitudes, (1, 0, 2)).reshape(600, 75)
    other = jnp.transpose(other_terms, (1, 0, 2)).reshape(600, 1200)
    sm = pl.BlockSpec(memory_space=pltpu.SMEM)
    V = pltpu.VMEM
    dma = pltpu.SemaphoreType.DMA
    out, rms = pl.pallas_call(
        ladder_kernel,
        out_shape=(
            jax.ShapeDtypeStruct((600, 1200), BF),
            jax.ShapeDtypeStruct((1, 1), F32),
        ),
        in_specs=[pl.BlockSpec(memory_space=pltpu.HBM)] * 6,
        out_specs=(pl.BlockSpec(memory_space=pl.ANY), sm),
        scratch_shapes=[
            V((75, 512), BF),
            V((600, 75), BF),
            V((512, 512), BF),
            V((1200,), F32),
            pltpu.SMEM((8,), F32),
            V((600, 1200), F32),
            V((10, 600, 128), F32),
            V((600, 1200), BF),
            V((512, 512), BF),
            V((8, 1280), F32),
            V((8, 1280, 512), BF),
            V((16, 80, 640), BF),
            V((1280, 640), BF),
            V((2, 640, 128), F32),
            V((16, 80, 256), BF),
            V((2, 16, 80, 256), BF),
            V((512, 1280), BF),
            V((8, 2, 32, 512), BF),
            V((512, 512), BF),
            V((512, 1280), F32),
            V((256, 1280), F32),
            V((16, 80, 256), BF),
            V((16, 80, 256), BF),
            V((8, 80, 512), BF),
            V((8, 80, 512), BF),
            V((1280, 128), F32),
            V((1280, 128), F32),
            V((1280, 128), F32),
            V((8, 80, 1280), BF),
            V((8, 128), F32),
            V((16, 8, 128), F32),
            V((8, 8, 128), F32),
            dma((8, 16)), dma((8, 16)),
            dma((4, 4, 2)), dma((4, 4, 2)),
            dma((8,)), dma((8,)),
            dma((16,)), dma((16,)),
            dma((8,)), dma((8,)),
            dma((8,)), dma((8,)),
            dma((8, 5)), dma((8, 5)),
            dma((8, 2)), dma((8, 2)),
            dma((16,)), dma((16,)),
            dma((3,)), dma((3,)),
            dma((3,)), dma((3,)),
            dma((3, 8)), dma((3, 8)),
            dma((12,)),
        ],
        compiler_params=pltpu.CompilerParams(
            collective_id=0, has_side_effects=True, vmem_limit_bytes=56 * 1024 * 1024
        ),
        name="ladder",
    )(factors, t, kernel, other, virt_energy, pair_energy)
    residual = other + out.astype(F32)
    return jnp.transpose(residual.reshape(75, 8, 1200), (1, 0, 2)), rms.reshape(())


def solution(mesh):
    torus = Mesh(mesh.devices.reshape(4, 4, 8, 2), ("x", "y", "z", "core"))
    plane, rank = ("x", "y"), ("z", "core")
    return jax.shard_map(
        shards,
        mesh=torus,
        in_specs=(P(None, plane, rank), P(plane, rank), P(plane, rank), P(None, plane, None), P(), P()),
        out_specs=(P(None, plane, None), P()),
        check_vma=False,
    )
```

```python
import functools

import jax
import jax.numpy as jnp
from jax import lax
from jax.experimental import pallas as pl
from jax.experimental.pallas import tpu as pltpu
from jax.sharding import Mesh
from jax.sharding import PartitionSpec as P

MESH = pl.DeviceIdType.MESH
BF = jnp.bfloat16
F32 = jnp.float32
EPS = 1e-06
NT = (((1,), (1,)), ((), ()))
TN = (((0,), (0,)), ((), ()))
TICKS = 14
READY = 6
REGION = (pl.ds(1024, 256), pl.ds(0, 512), pl.ds(512, 512))
PIECES = ((64, 16), (0, 32), (32, 32))
FAR = sorted(((i, j) for i in range(4) for j in range(4) if i or j), key=lambda p: -min(p[0], 4 - p[0]) - min(p[1], 4 - p[1]))


def roll(a, shift):
    shift %= 128
    return a if shift == 0 else pltpu.roll(a, shift, 1)


def ladder_kernel(
    f_hbm, t_hbm, k_hbm, other_hbm, e_hbm, ep_hbm, out_ref, rms_ref,
    f_ref, t_ref, k_ref, e_ref, ep_ref,
    stage, res, packed, zt_ref, er,
    xb, tt, ttp, half, hs, hb, ht, zb_ref, wt, acc, rb, bs, br, ls, lb, lt, ltr, lc, la, sc, sp, sz,
    x_ss, x_rs, fin, e_rs, c_rs, r_rs, t_rs, u_rs, g_rs, h_rs, m_rs, d_rs, p_rs, q_rs, loc,
):
    x, y, z, c = (lax.axis_index(n) for n in ("x", "y", "z", "core"))
    v = 4 * x + y
    xp, xm = (x + 1) % 4, (x + 3) % 4
    yp, ym = (y + 1) % 4, (y + 3) % 4
    zp, zm = (z + 1) % 8, (z + 7) % 8
    sib = {"core": 1 - c}

    def rows(i, off, n, w=512, lo=0):
        return xb.at[i, pl.ds(pl.multiple_of(off, 16), n), pl.ds(lo, w)]

    def send(src, dst, ss, rs, dev):
        pltpu.make_async_remote_copy(
            src_ref=src, dst_ref=dst, send_sem=ss, recv_sem=rs, device_id=dev, device_id_type=MESH
        ).start()

    def got(dst, rs):
        pltpu.make_async_remote_copy(
            src_ref=dst, dst_ref=dst, send_sem=rs, recv_sem=rs, device_id=sib, device_id_type=MESH
        ).wait_recv()

    def left(src, ss):
        pltpu.make_async_remote_copy(
            src_ref=src, dst_ref=src, send_sem=ss, recv_sem=ss, device_id=sib, device_id_type=MESH
        ).wait_send()

    def a_off(i, j):
        return i * 128 + j * 32

    def b_off(i, j):
        return 512 + j * 128 + i * 32

    def c_off(i, j):
        return 1024 + i * 64 + j * 16

    loads = [
        pltpu.make_async_copy(a, b, loc.at[n])
        for n, (a, b) in enumerate(
            ((f_hbm, f_ref), (t_hbm, t_ref), (k_hbm, k_ref), (e_hbm, e_ref), (ep_hbm, ep_ref), (other_hbm, stage))
        )
    ]
    for o in loads:
        o.start()

    bar = pltpu.get_barrier_semaphore()

    def plane_dev(j, core):
        w = (v + j) % 16
        return {"x": w // 4, "y": w % 4, "core": core}

    def greet(j, _):
        pl.semaphore_signal(bar, inc=1, device_id=plane_dev(j, c), device_id_type=MESH)
        pl.semaphore_signal(bar, inc=1, device_id=plane_dev(j, 1 - c), device_id_type=MESH)
        return 0

    lax.fori_loop(1, 16, greet, 0)
    pl.semaphore_signal(bar, inc=1, device_id=sib, device_id_type=MESH)

    def greet_z(j, _):
        pl.semaphore_signal(bar, inc=1, device_id={"z": (z + j) % 8}, device_id_type=MESH)
        return 0

    lax.fori_loop(1, 8, greet_z, 0)
    with jax.named_scope("local"):
        loads[0].wait()
        xb[z, pl.ds(pl.multiple_of(a_off(x, y), 16), 32), :] = f_ref[pl.ds(0, 32), :]
        xb[z, pl.ds(pl.multiple_of(b_off(x, y), 16), 32), :] = f_ref[pl.ds(32, 32), :]
        last = jnp.concatenate([f_ref[pl.ds(64, 11), :].astype(F32), jnp.zeros((5, 512), F32)], 0)
        xb[z, pl.ds(pl.multiple_of(c_off(x, y), 16), 16), :] = last.astype(BF)
        loads[1].wait()
        for n in range(5):
            cnt = 128 if n < 4 else 88
            m = t_ref[pl.ds(128 * n, cnt), :].astype(F32)
            if cnt < 128:
                m = jnp.concatenate([m, jnp.zeros((128 - cnt, 75), F32)], 0)
            m = jnp.concatenate([m.T, jnp.zeros((5, 128), F32)], 0)
            tt[2 * z + c, :, pl.ds(128 * n, 128)] = m.astype(BF)
        loads[2].wait()
        for n in range(4):
            zt_ref[:, pl.ds(128 * n, 128)] = k_ref[pl.ds(128 * n, 128), :].astype(F32).T.astype(BF)
        for o in loads[3:]:
            o.wait()
        er[:, pl.ds(0, 1200)] = jnp.broadcast_to(e_ref[...].reshape(1, 1200), (8, 1200))
        er[:, pl.ds(1200, 80)] = jnp.zeros((8, 80), F32)
        for n in range(10):
            w = 128 if n < 9 else 48
            res[n, :, pl.ds(0, w)] = stage[:, pl.ds(128 * n, w)]
    with jax.named_scope('barrier'):
        pl.semaphore_wait(bar, 38)

    def zblk(k):
        return (z + ((k + 1) // 2) * (2 * (k % 2) - 1) + 8) % 8

    def ring_pieces(s, d, blk):
        a = rows(blk, a_off(x, y), 32, 512 if d or s == 3 else 384)
        b = rows(blk, b_off(x, y), 32, 384 if d and s < 3 else 512)
        return ((a, 2 * s + d), (b, 8 + 2 * s + d)) if s < 3 else (((b, a)[d], 6 + d),)

    def t_piece(s, d, blk):
        r = 2 * blk + c
        return tt.at[r] if s < 3 else tt.at[r, pl.ds(48 * d, 48 - 16 * d)]

    def ring_step(s, zl, zr):
        for d, blk in enumerate((zl, zr)):
            for p, i in ring_pieces(s, d, blk):
                send(p, p, fin.at[0], r_rs.at[i], {"z": (zp, zm)[d]})

    def t_step(s, zl, zr):
        for d, blk in enumerate((zl, zr)):
            p = t_piece(s, d, blk)
            send(p, p, fin.at[1], t_rs.at[2 * s + d], {"z": (zp, zm)[d]})

    def push_t(n, blk):
        r = 2 * blk + c
        send(tt.at[r], tt.at[r], fin.at[2], u_rs.at[n], sib)

    def ring_got(s):
        lo, hi = (z + 7 - s) % 8, (z + 1 + s) % 8
        for d, blk in enumerate((lo, hi)):
            for p, i in ring_pieces(s, d, blk):
                got(p, r_rs.at[i])
        return lo, hi

    def t_got(s):
        lo, hi = (z + 7 - s) % 8, (z + 1 + s) % 8
        for d, blk in enumerate((lo, hi)):
            got(t_piece(s, d, blk), t_rs.at[2 * s + d])
        return lo, hi

    ring_step(0, z, z)
    t_step(0, z, z)
    push_t(0, z)

    def c_piece(i, j, h):
        return xb.at[z, pl.ds(pl.multiple_of(c_off(i, j), 16), 16), pl.ds(256 * h, 256)]

    def c_step(s):
        if s == 0:
            p = rows(z, c_off(x, y), 16)
            send(p, p, fin.at[3], c_rs.at[0], {"y": yp})
            send(p, p, fin.at[3], c_rs.at[1], {"y": ym})
        elif s == 1:
            got(rows(z, c_off(x, ym), 16), c_rs.at[0])
            got(rows(z, c_off(x, yp), 16), c_rs.at[1])
            p, q = c_piece(x, ym, 0), c_piece(x, yp, 1)
            send(p, p, fin.at[3], c_rs.at[2], {"y": yp})
            send(q, q, fin.at[3], c_rs.at[3], {"y": ym})
        elif s == 2:
            got(c_piece(x, (y + 2) % 4, 0), c_rs.at[2])
            got(c_piece(x, (y + 2) % 4, 1), c_rs.at[3])
            p = rows(z, c_off(x, 0), 64)
            send(p, p, fin.at[3], c_rs.at[4], {"x": xp})
            send(p, p, fin.at[3], c_rs.at[5], {"x": xm})
        elif s == 3:
            got(rows(z, c_off(xm, 0), 64), c_rs.at[4])
            got(rows(z, c_off(xp, 0), 64), c_rs.at[5])
            p, q = rows(z, c_off(xm, 0), 32), rows(z, c_off(xp, 2), 32)
            send(p, p, fin.at[3], c_rs.at[6], {"x": xp})
            send(q, q, fin.at[3], c_rs.at[7], {"x": xm})
        else:
            got(rows(z, c_off((x + 2) % 4, 0), 32), c_rs.at[6])
            got(rows(z, c_off((x + 2) % 4, 2), 32), c_rs.at[7])

    def quarter(blk, q, d, half_only):
        xq, yq = (x + q) % 4, (y + q) % 4
        a, b = rows(blk, xq * 128, 128, 128, 384), rows(blk, 512 + yq * 128, 128, 128, 384)
        if half_only:
            return (rows(blk, 1024 + xq * 64 + 32 * d, 32),)
        return (a, b)[d], rows(blk, 1024 + xq * 64, 64)

    def quarter_send(g, q, blks, half_only=False):
        for d, blk in enumerate(blks):
            for p in quarter(blk, q, d, half_only):
                send(p, p, fin.at[4], e_rs.at[g, q, d], {"z": (zp, zm)[d]})

    def pump(e, _):
        g, i = e // 4, e % 4
        q = i + (i == 2).astype(jnp.int32) - (i == 3).astype(jnp.int32)
        blks = (z + 7 - g) % 8, (z + 1 + g) % 8

        def take(n):
            for d in range(2):
                got(rows(blks[d], 0, n), e_rs.at[g, q, d])

        @pl.when(g < 3)
        def _():
            take(96)

        @pl.when(g == 3)
        def _():
            take(32)

        @pl.when(g < 2)
        def _():
            quarter_send(g + 1, q, blks)

        @pl.when(g == 2)
        def _():
            quarter_send(g + 1, q, blks, True)

        return 0

    def s1(k, wa, wb):
        b = zblk(k)
        p, q = rows(b, a_off(x, y), 32, wa), rows(b, b_off(x, y), 32, wb)
        send(p, p, x_ss.at[k, 0], x_rs.at[k, 0], {"y": yp})
        send(p, p, x_ss.at[k, 0], x_rs.at[k, 0], {"y": ym})
        send(q, q, x_ss.at[k, 1], x_rs.at[k, 4], {"x": xp})
        send(q, q, x_ss.at[k, 1], x_rs.at[k, 4], {"x": xm})

    def s2(k, wa, wb):
        b = zblk(k)
        got(rows(b, 0, 64, wa), x_rs.at[k, 0])
        p, q = rows(b, a_off(x, ym), 16, wa), rows(b, a_off(x, yp) + 16, 16, wa)
        send(p, p, x_ss.at[k, 0], x_rs.at[k, 1], {"y": yp})
        send(q, q, x_ss.at[k, 0], x_rs.at[k, 1], {"y": ym})
        got(rows(b, 0, 64, wb), x_rs.at[k, 4])
        p, q = rows(b, b_off(xm, y), 16, wb), rows(b, b_off(xp, y) + 16, 16, wb)
        send(p, p, x_ss.at[k, 1], x_rs.at[k, 5], {"x": xp})
        send(q, q, x_ss.at[k, 1], x_rs.at[k, 5], {"x": xm})

    def s3(k, wa, wb):
        b = zblk(k)
        y2, x2 = (y + 2) % 4, (x + 2) % 4
        got(rows(b, 0, 32, wa), x_rs.at[k, 1])
        p = rows(b, a_off(x, 0), 128, wa)
        send(p, p, x_ss.at[k, 0], x_rs.at[k, 2], {"x": xp})
        send(p, p, x_ss.at[k, 0], x_rs.at[k, 2], {"x": xm})
        got(rows(b, 0, 32, wb), x_rs.at[k, 5])
        p = rows(b, b_off(0, y), 128, wb)
        send(p, p, x_ss.at[k, 1], x_rs.at[k, 6], {"y": yp})
        send(p, p, x_ss.at[k, 1], x_rs.at[k, 6], {"y": ym})

    def s4(k, wa, wb):
        b = zblk(k)
        got(rows(b, 0, 256, wa), x_rs.at[k, 2])
        p, q = rows(b, a_off(xm, 0), 64, wa), rows(b, a_off(xp, 2), 64, wa)
        send(p, p, x_ss.at[k, 0], x_rs.at[k, 3], {"x": xp})
        send(q, q, x_ss.at[k, 0], x_rs.at[k, 3], {"x": xm})
        got(rows(b, 0, 256, wb), x_rs.at[k, 6])
        p, q = rows(b, b_off(0, ym), 64, wb), rows(b, b_off(2, yp), 64, wb)
        send(p, p, x_ss.at[k, 1], x_rs.at[k, 7], {"y": yp})
        send(q, q, x_ss.at[k, 1], x_rs.at[k, 7], {"y": ym})

    def s5(k, wa, wb):
        b = zblk(k)
        y2, x2 = (y + 2) % 4, (x + 2) % 4
        got(rows(b, 0, 128, wa), x_rs.at[k, 3])
        got(rows(b, 0, 128, wb), x_rs.at[k, 7])

    def send_kernel():
        kc = y % 2

        def one(j, _):
            w = (v + j) % 16
            src = zt_ref.at[pl.ds(pl.multiple_of(32 * w, 32), 32)]
            send(src, zb_ref.at[v // 2, c], fin.at[15], m_rs.at[0], plane_dev(j, kc))
            return 0

        lax.fori_loop(1, 16, one, 0)
        src = zt_ref.at[pl.ds(pl.multiple_of(32 * v, 32), 32)]

        @pl.when(c == kc)
        def _():
            pltpu.make_async_copy(src, zb_ref.at[v // 2, c], m_rs.at[0]).start()

        @pl.when(c != kc)
        def _():
            send(src, zb_ref.at[v // 2, c], fin.at[15], m_rs.at[0], sib)

    def make_half():
        for n in range(1, 8):
            b = zblk(n)
            got(tt.at[2 * b + 1 - c], u_rs.at[n])
        got(tt.at[2 * z + 1 - c], u_rs.at[0])
        for i in range(4):
            for j in range(4):
                w = 4 * i + j
                ttp[pl.ds(a_off(i, j), 32), :] = tt[w, pl.ds(0, 32), :]
                ttp[pl.ds(b_off(i, j), 32), :] = tt[w, pl.ds(32, 32), :]
                ttp[pl.ds(c_off(i, j), 16), :] = tt[w, pl.ds(64, 16), :]
        lanes = lax.broadcasted_iota(jnp.int32, (80, 128), 1) // 32

        def chunk(a, _):
            q = pl.ds(pl.multiple_of(256 * a, 256), 256)
            m = lax.dot_general(ttp[...], xb[z, :, q], TN, preferred_element_type=F32)
            half[0] = m[:, :128]
            half[1] = m[:, 128:]
            for h in range(2):
                for g in range(2):
                    part = [half[h, pl.ds(4 * g + k, 80, stride=8), :] for k in range(4)]
                    for s in range(4):
                        m = roll(part[0], (0 - s) * 32)
                        for k in range(1, 4):
                            m = jnp.where(lanes == k, roll(part[k], (k - s) * 32), m)
                        hs[8 * a + 4 * h + s, :, pl.ds(128 * g, 128)] = m.astype(BF)
            for s in range(8):
                w = 8 * a + s

                @pl.when(w != v)
                def _(w=w):
                    dev = {"x": w // 4, "y": w % 4}
                    send(hs.at[w], hb.at[c, v], fin.at[5], m_rs.at[1], dev)

            return 0

        lax.fori_loop(0, 2, chunk, 0)
        pltpu.make_async_copy(hs.at[v], hb.at[c, v], m_rs.at[1]).start()

    def take_half():
        with jax.named_scope('w_hb'):
            got(hb.at[c], m_rs.at[1])
        send(hb.at[c], hb.at[c], fin.at[6], m_rs.at[2], sib)
        acc[...] = jnp.zeros_like(acc)
        with jax.named_scope('w_hbs'):
            got(hb.at[1 - c], m_rs.at[2])
        for s in range(2):
            to = pl.ds(256 * s, 256)
            for i in range(4):
                m = jnp.concatenate([hb[s, 4 * i + j, pl.ds(0, 32), :] for j in range(4)], 0)
                ht[to, pl.ds(128 * i, 128)] = m.astype(F32).T.astype(BF)
                m = jnp.concatenate([hb[s, 4 * j + i, pl.ds(32, 32), :] for j in range(4)], 0)
                ht[to, pl.ds(512 + 128 * i, 128)] = m.astype(F32).T.astype(BF)
            for i in range(2):
                m = jnp.concatenate([hb[s, 8 * i + j, pl.ds(64, 16), :] for j in range(8)], 0)
                ht[to, pl.ds(1024 + 128 * i, 128)] = m.astype(F32).T.astype(BF)
        with jax.named_scope('w_zb'):
            got(zb_ref, m_rs.at[0])

    mine = pl.ds(pl.multiple_of(256 * c, 256), 256)
    yours = pl.ds(pl.multiple_of(256 * (1 - c), 256), 256)

    def compute(k, last):
        b = zblk(k)
        for q in range(2):
            q = pl.ds(256 * q, 256)
            cp = jnp.dot(ht[...], xb[b, :, q], preferred_element_type=F32)
            zz = zb_ref[b, :, :, q].astype(F32)
            for s in range(2):
                for i in range(8):
                    o = 256 * s + 32 * i
                    wt[pl.ds(o, 32), q] = (cp[o : o + 32] * zz[s]).astype(BF)
        for n in (4, 0, 1, 2, 3):
            a = pl.ds(256 * n, 256)
            acc[:, a] += lax.dot_general(wt[...], xb[b, a, :], NT, preferred_element_type=F32)
            if last is True and (n % 2 or n == 4):
                h = (n // 2 + 1) % 3
                send(acc.at[yours, REGION[h]], rb.at[:, REGION[h]], fin.at[7], d_rs.at[h], sib)
        return 0

    def on(cond, name, f, *args):
        @pl.when(cond)
        def _():
            with jax.named_scope(name):
                f(*args)

    def forward(s):
        lo, hi = ring_got(s - 1)
        if s < 4:
            ring_step(s, lo, hi)

    def forward_t(s):
        lo, hi = t_got(s - 1)
        if s < 4:
            t_step(s, lo, hi)
            push_t(2 * s - 1, hi)
            push_t(2 * s, lo)
        else:
            push_t(7, lo)

    def pumped(t):
        return jnp.clip(2 * (t - 4), 0, 16)

    def pair(f, n):
        @pl.when(n < 4)
        def _():
            f(2 * n - 1, 512, 384)
            f(2 * n, 384, 512)

        @pl.when(n == 4)
        def _():
            f(7, 512, 512)

    def single(f, k):
        @pl.when((k % 2 == 1) & (k < 7))
        def _():
            f(k, 512, 384)

        @pl.when(k % 2 == 0)
        def _():
            f(k, 384, 512)

        @pl.when(k == 7)
        def _():
            f(k, 512, 512)

    def tick(t, _):
        for s in range(1, 5):
            on(t == s, "forward", forward, s)
        on(t == 4, "s5", s5, 0, 512, 512)
        on(t >= 7, "s5", single, s5, t - 6)
        for s in range(5):
            on(t == s, "c_step", c_step, s)
        on(t == READY, "take_half", take_half)
        on(t == 3, "s4", s4, 0, 512, 512)
        on((t >= 5) & (t < 12), "s4", single, s4, t - 4)
        on(t == 2, "s3", s3, 0, 512, 512)
        on((t >= 3) & (t < 10) & (t != 4), "s3", single, s3, t - 2)
        on(t == 0, "s1", s1, 0, 512, 512)
        on((t >= 1) & (t < 5), "s1", pair, s1, t)
        on(t == 0, "send_kernel", send_kernel)
        for s in range(1, 5):
            on(t == s, "forward_t", forward_t, s)
        on(t == 3, "quarter", quarter_send, 0, 0, (z, z))
        on(t == 4, "quarter", quarter_send, 0, 1, (z, z))
        on(t == 4, "quarter", quarter_send, 0, 3, (z, z))
        on(t == 4, "quarter", quarter_send, 0, 2, (z, z))
        on(t == 4, "make_half", make_half)
        on(t == 4, "s3", s3, 2, 384, 512)
        on(t == 1, "s2", s2, 0, 512, 512)
        on((t >= 2) & (t < 4), "s2", pair, s2, t - 1)
        on(t == 5, "s2", pair, s2, t - 2)
        on(t == 7, "s2", s2, 7, 512, 512)
        with jax.named_scope("pump"):
            lax.fori_loop(pumped(t - 1), pumped(t), pump, 0)
        with jax.named_scope("compute"):
            lax.fori_loop(jnp.maximum(t - READY, 0), jnp.where(t < TICKS - 1, jnp.maximum(t - READY + 1, 0), 7), compute, 0)
        return 0

    lax.fori_loop(0, TICKS, tick, 0)
    with jax.named_scope('compute'):
        compute(7, True)

    for h, (lo, cnt) in enumerate(PIECES):
        with jax.named_scope("w_rb"):
            got(rb.at[:, REGION[h]], d_rs.at[h])
        for n in (range(8, 10), range(4), range(4, 8))[h]:
            a = pl.ds(128 * n, 128)
            m = (acc[mine, a] + rb[:, a]).T.astype(BF)
            for j in range(128 // cnt):
                w = (8 * (n - 8) + j, 4 * n + j, 4 * j + n - 4)[h]
                bs[w, pl.ds(lo, cnt), :] = m[cnt * j : cnt * j + cnt]
        for i, j in FAR:
            i, j = (x + i) % 4, (y + j) % 4
            w = 4 * i + j
            send(bs.at[w, pl.ds(lo, cnt)], br.at[v, pl.ds(lo, cnt)], fin.at[8], p_rs.at[h], {"x": i, "y": j})
        pltpu.make_async_copy(bs.at[v, pl.ds(lo, cnt)], br.at[v, pl.ds(lo, cnt)], p_rs.at[h]).start()

    for k in range(8):
        wa, wb = (512, 512) if k in (0, 7) else (512, 384) if k % 2 else (384, 512)
        left(rows(0, 0, 480, wa), x_ss.at[k, 0])
        left(rows(0, 0, 480, wb), x_ss.at[k, 1])
    left(rows(0, 0, 400), fin.at[0])
    left(tt.at[pl.ds(0, 7)], fin.at[1])
    left(tt.at[pl.ds(0, 8)], fin.at[2])
    left(rows(0, 0, 240), fin.at[3])
    left(xb.at[pl.ds(0, 2)], fin.at[4])
    left(hs.at[pl.ds(0, 15)], fin.at[5])
    left(hb.at[0], fin.at[6])
    left(rb, fin.at[7])

    @pl.when(c == y % 2)
    def _():
        left(zt_ref.at[pl.ds(0, 480)], fin.at[15])

    @pl.when(c != y % 2)
    def _():
        left(zt_ref, fin.at[15])

    for h, (lo, n) in enumerate(PIECES):
        with jax.named_scope("w_br"):
            got(br.at[:, pl.ds(lo, n)], p_rs.at[h])
        with jax.named_scope("unpack"):
            lanes = lax.broadcasted_iota(jnp.int32, (n, 128), 1) // 32
            for g in range(2):
                for a in range(4):
                    part = [br[4 * a + s, pl.ds(lo, n), pl.ds(128 * g, 128)].astype(F32) for s in range(4)]
                    for k in range(4):
                        m = roll(part[0], (0 - k) * 32)
                        for s in range(1, 4):
                            m = jnp.where(lanes == s, roll(part[s], (s - k) * 32), m)
                        ls[4 * g + k, pl.ds(lo, n), pl.ds(128 * a, 128)] = m.astype(BF)
        for d in (7, 1, 6, 2, 5, 3, 4):
            w = (z + d) % 8
            send(ls.at[w, pl.ds(lo, n)], lb.at[z, pl.ds(lo, n)], fin.at[9], q_rs.at[h, d], {"z": w})
        if h == 0:
            lt[...] = jnp.zeros_like(lt)

    def lad(b, src):
        for a in range(5):
            a = pl.ds(256 * a, 256)
            lt[a, pl.ds(0, 80)] += lax.dot_general(xb[b, a, :], src[b], NT, preferred_element_type=F32)

    lad(z, ls)

    def lad_step(j, _):
        d = 4 + ((7 - j) // 2) * (1 - 2 * (j % 2))
        b = (z + 8 - d) % 8
        with jax.named_scope("w_lb"):
            for h, (lo, n) in enumerate(PIECES):
                got(lb.at[b, pl.ds(lo, n)], q_rs.at[h, d])
        with jax.named_scope("w_lad"):
            lad(b, lb)
        return 0

    lax.fori_loop(0, 7, lad_step, 0)
    send(lt, ltr, fin.at[10], m_rs.at[6], sib)
    ea = pltpu.roll(er[...], (1280 - 75 * v) % 1280, 1)[:, :128].T[:75, 0:1]
    with jax.named_scope("w_ltr"):
        got(ltr, m_rs.at[6])
    lc[pl.ds(1200, 80), :] = jnp.zeros((80, 128), F32)
    for i in range(4):
        for j in range(4):
            o = 75 * (4 * i + j)
            for n, off, cnt in ((0, a_off(i, j), 32), (32, b_off(i, j), 32), (64, c_off(i, j), 11)):
                lc[pl.ds(o + n, cnt), :] = lt[pl.ds(off, cnt), :] + ltr[pl.ds(off, cnt), :]
    for n in range(10):
        b = pl.ds(128 * n, 128)
        la[z, :, b] = lc[b, :].T[:80].astype(BF)


    def la_part(i, h, lo, n=16):
        return la.at[i, pl.ds(lo, n), pl.ds(pl.multiple_of(640 * h, 128), 640)]

    def la_send(s, blk, d, ch):
        p = la_part(blk, c, 16 * ch)
        dev = {"z": ((zp, zm)[d] if s < 3 else (z + (2, 6)[d]) % 8)}
        send(p, p, fin.at[13], g_rs.at[2 * s + d, ch], dev)

    HALF = ((0, 48), (48, 32))

    def la_push(n, blk, h):
        p = la_part(blk, c, *HALF[h])
        send(p, p, fin.at[14], h_rs.at[n, h], sib)

    for ch in range(5):
        for d in range(2):
            la_send(0, z, d, ch)

    total = jnp.zeros((75, 128), F32)
    ep = ep_ref[z]
    for n in range(10):
        w = 128 if n < 9 else 48
        b = pl.ds(128 * n, w)
        den = ea + er[0:1, b] - ep
        u = (res[n, pl.ds(z, 75, stride=8), :] + lc[pl.ds(128 * n, 128), :].T[:75])[:, :w] / den
        u = u * u
        if w < 128:
            u = jnp.concatenate([u, jnp.zeros((75, 128 - w), F32)], 1)
        total = total + u
    sc[...] = jnp.full((8, 128), jnp.sum(total), F32)

    def give_sum(j, _):
        send(sc, sp.at[v], fin.at[11], m_rs.at[7], plane_dev(j, c))
        return 0

    lax.fori_loop(1, 16, give_sum, 0)
    pltpu.make_async_copy(sc, sp.at[v], m_rs.at[7]).start()

    def finish(i):
        o = pl.ds(i, 75, stride=8)
        for n in range(10):
            b = pl.ds(128 * n, 128)
            res[n, o, :] = la[i, :, b].astype(F32)[:75]

    for s in range(4):
        lo, hi = (z + 7 - s) % 8, (z + 1 + s) % 8
        with jax.named_scope(f"w_la{s}"):
            for ch in range(5):
                if s < 3:
                    got(la_part(lo, c, 16 * ch), g_rs.at[2 * s, ch])
                    if s < 2:
                        la_send(s + 1, lo, 0, ch)
                    if s == 1 and ch < 3:
                        la_send(3, lo, 0, ch)
                    got(la_part(hi, c, 16 * ch), g_rs.at[2 * s + 1, ch])
                    if s < 2:
                        la_send(s + 1, hi, 1, ch)
                    if s == 1 and ch >= 3:
                        la_send(3, hi, 1, ch)
                else:
                    got(la_part(lo, c, 16 * ch), g_rs.at[6 + (ch >= 3), ch])
                if ch in (2, 4):
                    h = ch // 2 - 1
                    la_push(2 * s + (s < 3), lo, h)
                    if s < 3:
                        la_push(2 * s, hi, h)
        if s == 0:
            finish(z)
            with jax.named_scope("w_sp"):
                got(sp, m_rs.at[7])
            s_all = sp[0]
            for n in range(1, 16):
                s_all = s_all + sp[n]
            sz[z] = s_all

            def give_sz(j, _):
                send(sz.at[z], sz.at[z], fin.at[12], m_rs.at[8], {"z": (z + j) % 8})
                return 0

            lax.fori_loop(1, 8, give_sz, 0)
        if s >= 1:
            for n in (2 * s - 2, 2 * s - 1):
                with jax.named_scope("w_las"):
                    for ch in range(2):
                        got(la_part(zblk(n + 1), 1 - c, *HALF[ch]), h_rs.at[n, ch])
                with jax.named_scope("finish"):
                    finish(zblk(n + 1))
    with jax.named_scope("w_las"):
        for ch in range(2):
            got(la_part(zblk(7), 1 - c, *HALF[ch]), h_rs.at[6, ch])
    with jax.named_scope("finish"):
        finish(zblk(7))
    outs = []
    for h, (lo, cnt) in enumerate(((0, 208), (208, 208), (416, 184))):
        p = pl.ds(lo, cnt)
        for n in range(10):
            w = 128 if n < 9 else 48
            packed[p, pl.ds(128 * n, w)] = res[n, p, pl.ds(0, w)].astype(BF)
        outs.append(pltpu.make_async_copy(packed.at[p], out_ref.at[p], loc.at[3 + h]))
        outs[-1].start()
    with jax.named_scope("w_sz"):
        got(sz.at[pl.ds(0, 7)], m_rs.at[8])
    s_all = sz[0]
    for n in range(1, 8):
        s_all = s_all + sz[n]
    s_all = jnp.sqrt(s_all / (8 * 1200 * 1200) + EPS)
    rms_ref[0, 0] = s_all[0, 0]
    with jax.named_scope('w_out'):
        for o in outs:
            o.wait()

    left(bs.at[pl.ds(0, 15)], fin.at[8])
    left(ls.at[pl.ds(0, 7)], fin.at[9])
    left(lt, fin.at[10])
    left(sp.at[pl.ds(0, 15)], fin.at[11])
    left(sz.at[pl.ds(0, 7)], fin.at[12])
    left(la.at[pl.ds(0, 7), :, pl.ds(0, 640)], fin.at[13])
    left(la.at[pl.ds(0, 7), :, pl.ds(0, 640)], fin.at[14])


def shards(amplitudes, factors, kernel, other_terms, virt_energy, pair_energy):
    t = jnp.transpose(amplitudes, (1, 0, 2)).reshape(600, 75)
    other = jnp.transpose(other_terms, (1, 0, 2)).reshape(600, 1200)
    sm = pl.BlockSpec(memory_space=pltpu.SMEM)
    V = pltpu.VMEM
    dma = pltpu.SemaphoreType.DMA
    out, rms = pl.pallas_call(
        ladder_kernel,
        out_shape=(
            jax.ShapeDtypeStruct((600, 1200), BF),
            jax.ShapeDtypeStruct((1, 1), F32),
        ),
        in_specs=[pl.BlockSpec(memory_space=pltpu.HBM)] * 6,
        out_specs=(pl.BlockSpec(memory_space=pl.ANY), sm),
        scratch_shapes=[
            V((75, 512), BF),
            V((600, 75), BF),
            V((512, 512), BF),
            V((1200,), F32),
            pltpu.SMEM((8,), F32),
            V((600, 1200), F32),
            V((10, 600, 128), F32),
            V((600, 1200), BF),
            V((512, 512), BF),
            V((8, 1280), F32),
            V((8, 1280, 512), BF),
            V((16, 80, 640), BF),
            V((1280, 640), BF),
            V((2, 640, 128), F32),
            V((16, 80, 256), BF),
            V((2, 16, 80, 256), BF),
            V((512, 1280), BF),
            V((8, 2, 32, 512), BF),
            V((512, 512), BF),
            V((512, 1280), F32),
            V((256, 1280), F32),
            V((16, 80, 256), BF),
            V((16, 80, 256), BF),
            V((8, 80, 512), BF),
            V((8, 80, 512), BF),
            V((1280, 128), F32),
            V((1280, 128), F32),
            V((1280, 128), F32),
            V((8, 80, 1280), BF),
            V((8, 128), F32),
            V((16, 8, 128), F32),
            V((8, 8, 128), F32),
            dma((8, 2)), dma((8, 8)), dma((16,)),
            dma((4, 4, 2)),
            dma((8,)),
            dma((16,)),
            dma((8,)),
            dma((8,)),
            dma((8, 5)),
            dma((8, 2)),
            dma((16,)),
            dma((3,)),
            dma((3,)),
            dma((3, 8)),
            dma((12,)),
        ],
        compiler_params=pltpu.CompilerParams(
            collective_id=0, has_side_effects=True, vmem_limit_bytes=56 * 1024 * 1024
        ),
        name="ladder",
    )(factors, t, kernel, other, virt_energy, pair_energy)
    residual = other + out.astype(F32)
    return jnp.transpose(residual.reshape(75, 8, 1200), (1, 0, 2)), rms.reshape(())


def solution(mesh):
    torus = Mesh(mesh.devices.reshape(4, 4, 8, 2), ("x", "y", "z", "core"))
    plane, rank = ("x", "y"), ("z", "core")
    return jax.shard_map(
        shards,
        mesh=torus,
        in_specs=(P(None, plane, rank), P(plane, rank), P(plane, rank), P(None, plane, None), P(), P()),
        out_specs=(P(None, plane, None), P()),
        check_vma=False,
    )
```
